128 devices in a mesh: dp: 1, tp: 16 (over z, y), fsdp: 8 (over x, core).
Axes of the slice: x: 4, y: 4, z: 4, core: 2. Of those that a mesh axis runs over, the one named last changes fastest.
Arguments:
- hidden: bfloat16 [8, 2048, 4096], P(('dp', 'fsdp'))
- positions: int32 [2048], replicated
- norm_gain: float32 [4096], P('fsdp')
- w_query: bfloat16 [4096, 4096], P('fsdp', 'tp')
- w_key: bfloat16 [4096, 256], P('fsdp')
- w_value: bfloat16 [4096, 256], P('fsdp')
- w_gate: bfloat16 [4096, 16384], P('fsdp', 'tp')
- w_up: bfloat16 [4096, 16384], P('fsdp', 'tp')
- w_out: bfloat16 [4096, 4096], P('tp', 'fsdp')
- w_down: bfloat16 [16384, 4096], P('tp', 'fsdp')
Outputs:
- output: bfloat16 [8, 2048, 4096], P(('dp', 'fsdp'))
All inputs are finite; a program needn't handle non-finite values.
Results may differ from the reference program's by a relative error of at most 0.0110866.
Values are sent between devices in bfloat16 or wider.
A program may use at most 1 GiB of HBM per device.

```python
import jax
import jax.numpy as jnp
from jax import lax

BATCH_ROWS = 8
SEQ_LEN = 2048
D_MODEL = 4096
N_HEADS = 16
HEAD_DIM = 256
D_FF = 16384


def setup_inputs(seed: int = 0, part: int = 0) -> dict:
    key_list = jax.random.split(jax.random.key(seed), 11)
    row_key = jax.random.fold_in(key_list[0], part)
    d_scale = D_MODEL ** -0.5
    q_width = N_HEADS * HEAD_DIM
    hidden = jax.random.normal(row_key, (BATCH_ROWS, SEQ_LEN, D_MODEL), jnp.float32)
    pos_steps = jax.random.randint(key_list[1], (SEQ_LEN,), 1, 3, dtype=jnp.int32)
    offset = jax.random.randint(key_list[2], (), 0, 1024, dtype=jnp.int32)
    positions = (offset + jnp.cumsum(pos_steps) - pos_steps[0]).astype(jnp.int32)
    norm_gain = jax.random.uniform(key_list[3], (D_MODEL,), jnp.float32, 0.5, 1.5)
    w_query = 2.0 * d_scale * jax.random.normal(key_list[4], (D_MODEL, q_width), jnp.float32)
    w_key = d_scale * jax.random.normal(key_list[5], (D_MODEL, HEAD_DIM), jnp.float32)
    w_value = d_scale * jax.random.normal(key_list[6], (D_MODEL, HEAD_DIM), jnp.float32)
    w_gate = d_scale * jax.random.normal(key_list[7], (D_MODEL, D_FF), jnp.float32)
    w_up = d_scale * jax.random.normal(key_list[8], (D_MODEL, D_FF), jnp.float32)
    w_out = q_width ** -0.5 * jax.random.normal(key_list[9], (q_width, D_MODEL), jnp.float32)
    w_down = D_FF ** -0.5 * jax.random.normal(key_list[10], (D_FF, D_MODEL), jnp.float32)
    return {
        "hidden": hidden.astype(jnp.bfloat16),
        "positions": positions,
        "norm_gain": norm_gain,
        "w_query": w_query.astype(jnp.bfloat16),
        "w_key": w_key.astype(jnp.bfloat16),
        "w_value": w_value.astype(jnp.bfloat16),
        "w_gate": w_gate.astype(jnp.bfloat16),
        "w_up": w_up.astype(jnp.bfloat16),
        "w_out": w_out.astype(jnp.bfloat16),
        "w_down": w_down.astype(jnp.bfloat16),
    }


def rope_tables(positions, head_dim):
    inv_freq = 10000.0 ** (-jnp.arange(0, head_dim, 2, dtype=jnp.float32) / head_dim)
    angles = positions.astype(jnp.float32)[:, None] * inv_freq[None, :]
    angles = jnp.concatenate([angles, angles], axis=-1)
    return jnp.cos(angles), jnp.sin(angles)


def rope_rotate(vectors, cos_t, sin_t):
    half_dim = vectors.shape[-1] // 2
    rotated = jnp.concatenate([-vectors[..., half_dim:], vectors[..., :half_dim]], axis=-1)
    return vectors * cos_t + rotated * sin_t


def layer_norm(hidden, gain_vec):
    row_f32 = hidden.astype(jnp.float32)
    centered = row_f32 - jnp.mean(row_f32, axis=-1, keepdims=True)
    variance = jnp.mean(centered * centered, axis=-1, keepdims=True)
    return (centered * lax.rsqrt(variance + 1e-6) * gain_vec).astype(jnp.bfloat16)


def reference(hidden, positions, norm_gain, w_query, w_key, w_value, w_gate, w_up, w_out, w_down):
    cos_t, sin_t = rope_tables(positions, HEAD_DIM)
    q_block = min(256, SEQ_LEN)
    n_blocks = SEQ_LEN // q_block
    score_scale = HEAD_DIM ** -0.5
    key_index = jnp.arange(SEQ_LEN)

    def seq_layer(seq_rows):
        normed = layer_norm(seq_rows, norm_gain)
        query_raw = jnp.dot(normed, w_query, preferred_element_type=jnp.float32).astype(jnp.bfloat16)
        key_raw = jnp.dot(normed, w_key, preferred_element_type=jnp.float32).astype(jnp.bfloat16)
        values = jnp.dot(normed, w_value, preferred_element_type=jnp.float32).astype(jnp.bfloat16)
        gate_raw = jnp.dot(normed, w_gate, preferred_element_type=jnp.float32).astype(jnp.bfloat16)
        up_raw = jnp.dot(normed, w_up, preferred_element_type=jnp.float32).astype(jnp.bfloat16)
        query_rot = rope_rotate(query_raw.reshape(SEQ_LEN, N_HEADS, HEAD_DIM).astype(jnp.float32), cos_t[:, None, :], sin_t[:, None, :]).astype(jnp.bfloat16)
        key_f32 = rope_rotate(key_raw.astype(jnp.float32), cos_t, sin_t).astype(jnp.bfloat16).astype(jnp.float32)
        value_f32 = values.astype(jnp.float32)
        query_blocks = query_rot.reshape(n_blocks, q_block, N_HEADS, HEAD_DIM)

        def block_attn(block_args):
            query_rows, blk_start = block_args
            scores = jnp.einsum("qhe,te->qht", query_rows.astype(jnp.float32), key_f32) * score_scale
            query_index = blk_start + jnp.arange(q_block)
            causal_mask = key_index[None, None, :] <= query_index[:, None, None]
            scores = jnp.where(causal_mask, scores, -1e30)
            prob_rows = jax.nn.softmax(scores, axis=-1).astype(jnp.bfloat16)
            attn_rows = jnp.einsum("qht,te->qhe", prob_rows.astype(jnp.float32), value_f32)
            return attn_rows.astype(jnp.bfloat16)

        attn_out = lax.map(block_attn, (query_blocks, jnp.arange(n_blocks) * q_block))
        attn_out = attn_out.reshape(SEQ_LEN, N_HEADS * HEAD_DIM)
        gated_act = (jax.nn.silu(gate_raw.astype(jnp.float32)) * up_raw.astype(jnp.float32)).astype(jnp.bfloat16)
        branch = jnp.dot(attn_out, w_out, preferred_element_type=jnp.float32) + jnp.dot(gated_act, w_down, preferred_element_type=jnp.float32)
        return (seq_rows.astype(jnp.float32) + branch).astype(jnp.bfloat16)

    return lax.map(seq_layer, hidden)
```

```python
import jax
import jax.numpy as jnp
from jax import lax
from jax.experimental import pallas as pl
from jax.experimental.pallas import tpu as pltpu
from jax.sharding import PartitionSpec as P

Q_BLOCK = 512
NORM_EPS = 1e-6


def rope_tables(positions, head_dim):
    inv_freq = 10000.0 ** (-jnp.arange(0, head_dim, 2, dtype=jnp.float32) / head_dim)
    angles = positions.astype(jnp.float32)[:, None] * inv_freq[None, :]
    angles = jnp.concatenate([angles, angles], axis=-1)
    return jnp.cos(angles), jnp.sin(angles)


def rope_rotate(vectors, cos_t, sin_t):
    half_dim = vectors.shape[-1] // 2
    rotated = jnp.concatenate([-vectors[..., half_dim:], vectors[..., :half_dim]], axis=-1)
    return vectors * cos_t + rotated * sin_t


def layer_norm(hidden, gain_vec):
    row_f32 = hidden.astype(jnp.float32)
    centered = row_f32 - jnp.mean(row_f32, axis=-1, keepdims=True)
    variance = jnp.mean(centered * centered, axis=-1, keepdims=True)
    return (centered * lax.rsqrt(variance + NORM_EPS) * gain_vec).astype(jnp.bfloat16)


def project(operand, weight):
    return jnp.einsum("bsn,nm->bsm", operand, weight, preferred_element_type=jnp.float32)


def causal_attention(query_rot, key_rot, values):
    batch = query_rot.shape[0]
    seq_len = query_rot.shape[1]
    n_heads = query_rot.shape[2]
    head_dim = query_rot.shape[3]
    q_block = min(Q_BLOCK, seq_len)
    score_scale = head_dim ** -0.5
    pieces = []
    for blk_idx in range(seq_len // q_block):
        blk_lo = blk_idx * q_block
        blk_hi = blk_lo + q_block
        scores = jnp.einsum("bshe,bte->bsht", query_rot[:, blk_lo:blk_hi], key_rot[:, :blk_hi], preferred_element_type=jnp.float32) * score_scale
        causal_mask = jnp.arange(blk_hi)[None, :] <= (blk_lo + jnp.arange(q_block))[:, None]
        scores = jnp.where(causal_mask[None, :, None, :], scores, -1e30)
        prob_rows = jax.nn.softmax(scores, axis=-1).astype(jnp.bfloat16)
        pieces.append(jnp.einsum("bsht,bte->bshe", prob_rows, values[:, :blk_hi], preferred_element_type=jnp.float32).astype(jnp.bfloat16))
    attn_out = jnp.concatenate(pieces, axis=1)
    return attn_out.reshape(batch, seq_len, n_heads * head_dim)


MESH = pl.DeviceIdType.MESH
TPA = 4
COL = 8


def _ring_ids(t):
    z, y = t // TPA, t % TPA
    y_r, y_l = z * TPA + (y + 1) % TPA, z * TPA + (y + 3) % TPA
    z_r, z_l = ((z + 1) % TPA) * TPA + y, ((z + 3) % TPA) * TPA + y
    return (y, y_r, y_l), (z, z_r, z_l)


def _fsdp_ids(f):
    xc, core = f // 2, f % 2
    f_p = xc * 2 + (1 - core)
    f_r = ((xc + 1) % 4) * 2 + core
    f_l = ((xc + 3) % 4) * 2 + core
    return xc, core, f_p, f_r, f_l


def reduce_kernel(az, x_hbm, wo, wd, out, wbuf, part, r1, r2, r3, r4, ybuf, xbuf,
                  ssem, rsem, wss, wrs, lsem, osem):
    t = lax.axis_index("tp")
    f = lax.axis_index("fsdp")
    ring_y, ring_z = _ring_ids(t)
    xc, core, f_p, f_r, f_l = _fsdp_ids(f)
    seq = az.shape[0]
    cols = wbuf.shape[2]
    half = seq // 2
    big = half // TPA
    small = big // TPA
    hd = wo.shape[0]

    ld_o = pltpu.make_async_copy(wo, wbuf.at[0, pl.ds(0, hd)], lsem.at[0])
    ld_d = pltpu.make_async_copy(wd, wbuf.at[0, pl.ds(hd, wd.shape[0])], lsem.at[1])
    ld_o.start()
    ld_d.start()
    axes = ((ring_y, ring_z), (ring_z, ring_y))

    def own_rows(h):
        (i1, _, _), (i2, _, _) = axes[h]
        return pl.multiple_of(h * half + i1 * big + i2 * small, small)

    ld_x = [pltpu.make_async_copy(x_hbm.at[pl.ds(own_rows(h), small), :], xbuf.at[h], lsem.at[2 + h]) for h in range(2)]
    for c in ld_x:
        c.start()

    barrier = pltpu.get_barrier_semaphore()
    for other in (ring_y[1], ring_y[2], ring_z[1], ring_z[2]):
        pl.semaphore_signal(barrier, inc=1, device_id={"tp": other}, device_id_type=MESH)
    for other in (f_p, f_r, f_l):
        pl.semaphore_signal(barrier, inc=1, device_id={"fsdp": other}, device_id_type=MESH)
    pl.semaphore_wait(barrier, 7)

    def wcopy(k, src, dst, dev):
        return pltpu.make_async_remote_copy(src_ref=src, dst_ref=dst, send_sem=wss.at[k], recv_sem=wrs.at[k],
                                            device_id={"fsdp": dev}, device_id_type=MESH)

    kk = wbuf.shape[1]
    kh = kk // 2
    top, bot = pl.ds(0, kh), pl.ds(kh, kh)
    w_own_p = wcopy(0, wbuf.at[0], wbuf.at[1], f_p)
    w_own_r = wcopy(1, wbuf.at[0], wbuf.at[2], f_r)
    w_own_l = wcopy(2, wbuf.at[0], wbuf.at[4], f_l)
    w_2p = wcopy(3, wbuf.at[2], wbuf.at[3], f_p)
    w_4p = wcopy(4, wbuf.at[4], wbuf.at[5], f_p)
    w_2r = wcopy(5, wbuf.at[2, top], wbuf.at[6, top], f_r)
    w_4l = wcopy(6, wbuf.at[4, bot], wbuf.at[6, bot], f_l)
    w_6p = wcopy(7, wbuf.at[6], wbuf.at[7], f_p)
    ld_o.wait()
    ld_d.wait()
    w_own_r.start()
    w_own_l.start()
    w_own_p.start()
    for c in ld_x:
        c.wait()

    def block_of(k):
        q = k // 2
        dx = 3 * q - 5 * (q // 2) - 2 * (q // 3)
        return ((xc + dx) % 4) * 2 + (core + k % 2) % 2

    def ring_copy(cb, h, d, step, src, dst, dev):
        return pltpu.make_async_remote_copy(src_ref=src, dst_ref=dst, send_sem=ssem.at[cb, h, d, step],
                                            recv_sem=rsem.at[cb, h, d, step], device_id={"tp": dev}, device_id_type=MESH)

    def rs_first(cb, h, step, ring, base, n, land):
        i, r, l = ring
        o = (i + 2) % TPA
        m = n // 2
        s = pl.multiple_of(base + o * n, m)
        return (ring_copy(cb, h, 0, step, part.at[cb, pl.ds(s, m)], land.at[cb, h, 0], r),
                ring_copy(cb, h, 1, step, part.at[cb, pl.ds(s + m, m)], land.at[cb, h, 1], l))

    def rs_second(cb, h, step, ring, base, n, land):
        i, r, l = ring
        s_r = pl.multiple_of(base + ((i + 1) % TPA) * n, n)
        s_l = pl.multiple_of(base + ((i + 3) % TPA) * n, n)
        return (ring_copy(cb, h, 0, step, part.at[cb, pl.ds(s_r, n)], land.at[cb, h, 0], r),
                ring_copy(cb, h, 1, step, part.at[cb, pl.ds(s_l, n)], land.at[cb, h, 1], l))

    def rs_update(cb, h, ring, base, n, land):
        i, _, _ = ring
        m = n // 2
        s_r = pl.multiple_of(base + ((i + 1) % TPA) * n, m)
        s_l = pl.multiple_of(base + ((i + 3) % TPA) * n + m, m)
        for s, d in ((s_r, 0), (s_l, 1)):
            rows = pl.ds(s, m)
            part[cb, rows] = (part[cb, rows].astype(jnp.float32) + land[cb, h, d].astype(jnp.float32)).astype(jnp.bfloat16)

    def ag_first(cb, h, step, ring, src, base, n):
        i, r, l = ring
        g = block_of(cb)
        dst = out.at[g, pl.ds(pl.multiple_of(base + i * n, n), n)]
        if src is None:
            src = dst
        return (ring_copy(cb, h, 0, step, src, dst, r), ring_copy(cb, h, 1, step, src, dst, l))

    def ag_second(cb, h, step, ring, base, n):
        i, r, l = ring
        g = block_of(cb)
        m = n // 2
        from_l = out.at[g, pl.ds(pl.multiple_of(base + ((i + 3) % TPA) * n, m), m)]
        from_r = out.at[g, pl.ds(pl.multiple_of(base + ((i + 1) % TPA) * n + m, m), m)]
        return (ring_copy(cb, h, 0, step, from_l, from_l, r), ring_copy(cb, h, 1, step, from_r, from_r, l))

    def copies(cb, step):
        res = []
        for h in range(2):
            ring1, ring2 = axes[h]
            base1 = h * half
            base2 = pl.multiple_of(h * half + ring1[0] * big, big)
            if step == 0:
                res.extend(rs_first(cb, h, step, ring1, base1, big, r1))
            elif step == 1:
                res.extend(rs_second(cb, h, step, ring1, base1, big, r2))
            elif step == 2:
                res.extend(rs_first(cb, h, step, ring2, base2, small, r3))
            elif step == 3:
                res.extend(rs_second(cb, h, step, ring2, base2, small, r4))
            elif step == 4:
                res.extend(ag_first(cb, h, step, ring2, ybuf.at[cb, h], base2, small))
            elif step == 5:
                res.extend(ag_second(cb, h, step, ring2, base2, small))
            elif step == 6:
                res.extend(ag_first(cb, h, step, ring1, None, base1, big))
            else:
                res.extend(ag_second(cb, h, step, ring1, base1, big))
        return res

    def start(cb, step):
        for c in copies(cb, step):
            c.start()

    def finish(cb, step):
        for c in copies(cb, step):
            c.wait_recv()
            c.wait_send()

    def own_out(cb, h):
        return pltpu.make_async_copy(ybuf.at[cb, h], out.at[block_of(cb), pl.ds(own_rows(h), small)], osem.at[cb, h])

    def stage0(cb):
        @pl.when(cb == 1)
        def _():
            w_own_p.wait()

        @pl.when(cb == 2)
        def _():
            w_own_r.wait()
            w_own_l.wait()
            w_2r.start()
            w_4l.start()
            w_2p.start()
            w_4p.start()

        @pl.when(cb == 3)
        def _():
            w_2p.wait()

        @pl.when(cb == 5)
        def _():
            w_4p.wait()

        @pl.when(cb == 6)
        def _():
            w_2r.wait()
            w_4l.wait()
            w_6p.start()

        @pl.when(cb == 7)
        def _():
            w_6p.wait()

        @pl.loop(0, seq // MT)
        def _(i):
            rows = pl.ds(pl.multiple_of(i * MT, MT), MT)
            part[cb, rows] = jnp.dot(az[rows, :], wbuf[cb], preferred_element_type=jnp.float32).astype(jnp.bfloat16)

        start(cb, 0)

    def stage1(cb):
        finish(cb, 0)
        for h in range(2):
            rs_update(cb, h, axes[h][0], h * half, big, r1)
        start(cb, 1)

    def stage2(cb):
        finish(cb, 1)
        for h in range(2):
            rows = pl.ds(pl.multiple_of(h * half + axes[h][0][0] * big, big), big)
            part[cb, rows] = (part[cb, rows].astype(jnp.float32) + r2[cb, h, 0].astype(jnp.float32)
                              + r2[cb, h, 1].astype(jnp.float32)).astype(jnp.bfloat16)
        start(cb, 2)

    def stage3(cb):
        finish(cb, 2)
        for h in range(2):
            rs_update(cb, h, axes[h][1], pl.multiple_of(h * half + axes[h][0][0] * big, big), small, r3)
        start(cb, 3)

    def stage4(cb):
        finish(cb, 3)
        g = block_of(cb)
        for h in range(2):
            branch = (part[cb, pl.ds(own_rows(h), small)].astype(jnp.float32) + r4[cb, h, 0].astype(jnp.float32)
                      + r4[cb, h, 1].astype(jnp.float32))
            xs = xbuf[h, :, pl.ds(pl.multiple_of(g * cols, cols), cols)].astype(jnp.float32)
            ybuf[cb, h] = (xs + branch).astype(jnp.bfloat16)
            own_out(cb, h).start()
        start(cb, 4)

    def stage5(cb):
        finish(cb, 4)
        start(cb, 5)

    def stage6(cb):
        finish(cb, 5)
        for h in range(2):
            own_out(cb, h).wait()
        start(cb, 6)

    def stage7(cb):
        finish(cb, 6)
        start(cb, 7)

    def stage8(cb):
        finish(cb, 7)

    stages = (stage0, stage1, stage2, stage3, stage4, stage5, stage6, stage7, stage8)

    @pl.loop(0, COL + len(stages) - 1)
    def _(n):
        for s, fn in enumerate(stages):
            cb = n - s

            @pl.when(jnp.logical_and(cb >= 0, cb < COL))
            def _(fn=fn, cb=cb):
                fn(cb)


MT = 512


def reduce_call(az, x, wo, wd):
    seq, kk = az.shape
    d = x.shape[1]
    cols = d // COL
    half = seq // 2
    big, small = half // TPA, half // TPA // TPA
    bf = jnp.bfloat16
    hbm = pl.BlockSpec(memory_space=pl.ANY)
    vm = pl.BlockSpec(memory_space=pltpu.VMEM)
    res = pl.pallas_call(
        reduce_kernel,
        out_shape=jax.ShapeDtypeStruct((COL, seq, cols), bf),
        in_specs=[vm, hbm, hbm, hbm],
        out_specs=hbm,
        scratch_shapes=[
            pltpu.VMEM((COL, kk, cols), bf),
            pltpu.VMEM((COL, seq, cols), bf),
            pltpu.VMEM((COL, 2, 2, big // 2, cols), bf),
            pltpu.VMEM((COL, 2, 2, big, cols), bf),
            pltpu.VMEM((COL, 2, 2, small // 2, cols), bf),
            pltpu.VMEM((COL, 2, 2, small, cols), bf),
            pltpu.VMEM((COL, 2, small, cols), bf),
            pltpu.VMEM((2, small, d), bf),
            pltpu.SemaphoreType.DMA((COL, 2, 2, 8)),
            pltpu.SemaphoreType.DMA((COL, 2, 2, 8)),
            pltpu.SemaphoreType.DMA((8,)),
            pltpu.SemaphoreType.DMA((8,)),
            pltpu.SemaphoreType.DMA((4,)),
            pltpu.SemaphoreType.DMA((COL, 2)),
        ],
        compiler_params=pltpu.CompilerParams(collective_id=1, has_side_effects=True, vmem_limit_bytes=60 * 1024 * 1024),
        cost_estimate=pl.CostEstimate(flops=2 * seq * kk * d, bytes_accessed=4 * seq * d, transcendentals=0),
        name="down_reduce",
    )(az, x, wo, wd)
    return res.transpose(1, 0, 2).reshape(1, seq, d)


def solution(mesh):
    row_spec = P(("dp", "fsdp"), None, None)

    def local_layer(hidden, positions, norm_gain, w_query, w_key, w_value, w_gate, w_up, w_out, w_down):
        gain_full = lax.all_gather(norm_gain, "fsdp", axis=0, tiled=True)
        w_in = jnp.concatenate([w_query, w_key, w_value, w_gate, w_up], axis=1)
        w_in = lax.all_gather(w_in, "fsdp", axis=0, tiled=True)
        batch = hidden.shape[0]
        seq_len = hidden.shape[1]
        head_dim = w_key.shape[1]
        ff = w_gate.shape[1]
        normed = layer_norm(hidden, gain_full)
        raw = project(normed, w_in).astype(jnp.bfloat16)
        query_raw, key_raw, values = raw[..., :head_dim], raw[..., head_dim:2 * head_dim], raw[..., 2 * head_dim:3 * head_dim]
        gate_raw, up_raw = raw[..., 3 * head_dim:3 * head_dim + ff], raw[..., 3 * head_dim + ff:]
        cos_t, sin_t = rope_tables(positions, head_dim)
        query_rot = rope_rotate(query_raw.reshape(batch, seq_len, -1, head_dim).astype(jnp.float32), cos_t[:, None, :], sin_t[:, None, :]).astype(jnp.bfloat16)
        key_rot = rope_rotate(key_raw.astype(jnp.float32), cos_t, sin_t).astype(jnp.bfloat16)
        attn_out = causal_attention(query_rot, key_rot, values)
        gated_act = (jax.nn.silu(gate_raw.astype(jnp.float32)) * up_raw.astype(jnp.float32)).astype(jnp.bfloat16)
        az = jnp.concatenate([attn_out, gated_act], axis=-1)[0]
        return reduce_call(az, hidden[0], w_out, w_down)

    in_specs = (row_spec, P(None), P("fsdp"), P("fsdp", "tp"), P("fsdp", None), P("fsdp", None), P("fsdp", "tp"), P("fsdp", "tp"), P("tp", "fsdp"), P("tp", "fsdp"))
    return jax.shard_map(local_layer, mesh=mesh, in_specs=in_specs, out_specs=row_spec, check_vma=False)
```

```python
import jax
import jax.numpy as jnp
from jax import lax
from jax.experimental import pallas as pl
from jax.experimental.pallas import tpu as pltpu
from jax.sharding import PartitionSpec as P

NORM_EPS = 1e-6
MESH = pl.DeviceIdType.MESH
TPA = 4
COL = 8


def _ring_ids(t):
    z, y = t // TPA, t % TPA
    y_r, y_l = z * TPA + (y + 1) % TPA, z * TPA + (y + 3) % TPA
    z_r, z_l = ((z + 1) % TPA) * TPA + y, ((z + 3) % TPA) * TPA + y
    return (y, y_r, y_l), (z, z_r, z_l)


def _fsdp_ids(f):
    xc, core = f // 2, f % 2
    f_p = xc * 2 + (1 - core)
    f_r = ((xc + 1) % 4) * 2 + core
    f_l = ((xc + 3) % 4) * 2 + core
    return xc, core, f_p, f_r, f_l


QB = 256
LN_ROWS = 128
LN_SUB = 64
GU = 128
M1 = 512


def project_kernel(x_hbm, pos, inv_freq, gain, wq, wk, wv, wg, wu, az, wbuf, h, q, k, v, cos_t, sin_t, gbuf, xb, scores, acc,
                   ssem, rsem, gss, grs, lsem, gsem, xsem):
    f = lax.axis_index("fsdp")
    nf = lax.axis_size("fsdp")
    xc, core, f_p, f_r, f_l = _fsdp_ids(f)
    f_o = ((xc + 2) % 4) * 2 + core
    seq, d = h.shape
    depth = wq.shape[0]
    mid = depth // 2
    hd = wq.shape[1]
    n_chunk = wbuf.shape[0]
    n_ff = wg.shape[1] // GU

    def rows_of(dev):
        return pl.ds(pl.multiple_of(dev * depth, depth), depth)

    def half_of(dev, part):
        return pl.ds(pl.multiple_of(dev * depth + part * mid, mid), mid)

    def load(i, part, src, col):
        return pltpu.make_async_copy(src.at[:, pl.ds(col, GU)], wbuf.at[i, rows_of(f), pl.ds(part * GU, GU)], lsem.at[i, part])

    for i, w in enumerate((wq, wk, wv)):
        for part in range(2):
            load(i, part, w, part * GU).start()
    for j in range(n_ff):
        load(3 + j, 0, wg, j * GU).start()
        load(3 + j, 1, wu, j * GU).start()

    def load_x(blk):
        slot = blk % 2
        return pltpu.make_async_copy(x_hbm.at[pl.ds(pl.multiple_of(blk * LN_ROWS, LN_ROWS), LN_ROWS), :], xb.at[slot], xsem.at[slot])

    load_x(0).start()
    ld_g = pltpu.make_async_copy(gain, gbuf.at[:, pl.ds(pl.multiple_of(f * depth, depth), depth)], gsem)
    ld_g.start()

    barrier = pltpu.get_barrier_semaphore()
    for e in range(1, nf):
        pl.semaphore_signal(barrier, inc=1, device_id={"fsdp": (f + e) % nf}, device_id_type=MESH)
    pl.semaphore_wait(barrier, nf - 1)

    def rcopy(i, s, src, dev):
        return pltpu.make_async_remote_copy(src_ref=src, dst_ref=src, send_sem=ssem.at[i, s], recv_sem=rsem.at[i, s],
                                            device_id={"fsdp": dev}, device_id_type=MESH)

    def transfer(i, s):
        src, dev = (
            (lambda: wbuf.at[i, rows_of(f)], f_r),
            (lambda: wbuf.at[i, rows_of(f)], f_l),
            (lambda: wbuf.at[i, rows_of(f)], f_p),
            (lambda: wbuf.at[i, half_of(f_l, 0)], f_r),
            (lambda: wbuf.at[i, half_of(f_r, 1)], f_l),
            (lambda: wbuf.at[i, rows_of(f_l)], f_p),
            (lambda: wbuf.at[i, rows_of(f_r)], f_p),
            (lambda: wbuf.at[i, rows_of(f_o)], f_p),
        )[s]
        return rcopy(i, s, src(), dev)

    def send_own(i):
        for part in range(2):
            load(i, part, wq, part * GU).wait()
        for s in range(3):
            transfer(i, s).start()

    def net_a(i):
        transfer(i, 0).wait_recv()
        transfer(i, 3).start()
        transfer(i, 1).wait_recv()
        transfer(i, 4).start()

        @pl.when(i + 2 < n_chunk)
        def _():
            send_own(i + 2)

        transfer(i, 5).start()
        transfer(i, 6).start()

    def net_b(i):
        transfer(i, 3).wait_recv()
        transfer(i, 4).wait_recv()
        transfer(i, 7).start()

    def ready(i):
        for s in (2, 5, 6, 7):
            transfer(i, s).wait_recv()
        for s in range(8):
            transfer(i, s).wait_send()

    ld_g.wait()
    gcol = gbuf.at[:, pl.ds(pl.multiple_of(f * depth, depth), depth)]
    gcopies = [pltpu.make_async_remote_copy(src_ref=gcol, dst_ref=gcol, send_sem=gss.at[e], recv_sem=grs.at[e],
                                            device_id={"fsdp": (f + e) % nf}, device_id_type=MESH) for e in range(1, nf)]
    for c in gcopies:
        c.start()
    send_own(0)
    send_own(1)

    @pl.loop(0, seq // QB)
    def _(b):
        rows = pl.ds(pl.multiple_of(b * QB, QB), QB)
        angle = pos[rows, :].astype(jnp.float32) * inv_freq[...]
        cos_t[rows, :] = jnp.cos(angle)
        sin_t[rows, :] = jnp.sin(angle)

    for c in gcopies:
        c.wait()

    n_blk = seq // LN_ROWS

    def norm_blocks(lo, hi):
        @pl.loop(lo, hi)
        def _(blk):
            load_x(blk).wait()

            @pl.when(blk + 1 < n_blk)
            def _():
                load_x(blk + 1).start()

            @pl.loop(0, LN_ROWS // LN_SUB)
            def _(r):
                row = xb[blk % 2, pl.ds(pl.multiple_of(r * LN_SUB, LN_SUB), LN_SUB), :].astype(jnp.float32)
                centered = row - jnp.sum(row, axis=-1, keepdims=True) * (1.0 / d)
                var = jnp.sum(centered * centered, axis=-1, keepdims=True) * (1.0 / d)
                out = centered * lax.rsqrt(var + NORM_EPS) * gbuf[...]
                h[pl.ds(pl.multiple_of(blk * LN_ROWS + r * LN_SUB, LN_SUB), LN_SUB), :] = out.astype(jnp.bfloat16)

    norm_blocks(0, n_blk // 2)
    net_a(0)
    norm_blocks(n_blk // 2, n_blk)

    def rope(rows):
        y = acc[...].astype(jnp.bfloat16).astype(jnp.float32)
        a, b = y[:, :hd // 2], y[:, hd // 2:]
        c, s = cos_t[rows, :], sin_t[rows, :]
        return jnp.concatenate([a * c - b * s, b * c + a * s], axis=1).astype(jnp.bfloat16)

    def compute(i):
        @pl.loop(0, seq // M1)
        def _(m):
            rows = pl.ds(pl.multiple_of(m * M1, M1), M1)
            acc[...] = jnp.dot(h[rows, :], wbuf[i], preferred_element_type=jnp.float32)

            @pl.when(i == 0)
            def _():
                q[rows, :] = rope(rows)

            @pl.when(i == 1)
            def _():
                k[rows, :] = rope(rows)

            @pl.when(i == 2)
            def _():
                v[rows, :] = acc[...].astype(jnp.bfloat16)

            @pl.when(i >= 3)
            def _():
                g = acc[:, :GU].astype(jnp.bfloat16).astype(jnp.float32)
                u = acc[:, GU:].astype(jnp.bfloat16).astype(jnp.float32)
                z = (g * (1.0 / (1.0 + jnp.exp(-g)))) * u
                az[rows, pl.ds(pl.multiple_of(hd + (i - 3) * GU, GU), GU)] = z.astype(jnp.bfloat16)

    scale = hd ** -0.5

    def tile(b):
        return pl.ds(pl.multiple_of(b * QB, QB), QB)

    def attend(b):
        qb = q[tile(b), :]

        def score(t):
            return lax.dot_general(qb, k[tile(t), :], (((1,), (1,)), ((), ())), preferred_element_type=jnp.float32) * scale

        def first(t, m):
            s = score(t)
            scores[t] = s
            return jnp.maximum(m, jnp.max(s, axis=-1, keepdims=True))

        s = score(b)
        keep = lax.broadcasted_iota(jnp.int32, (QB, QB), 1) <= lax.broadcasted_iota(jnp.int32, (QB, QB), 0)
        s = jnp.where(keep, s, -1e30)
        scores[b] = s
        m = lax.fori_loop(0, b, first, jnp.max(s, axis=-1, keepdims=True))

        def second(t, total):
            e = jnp.exp(scores[t] - m)
            scores[t] = e
            return total + jnp.sum(e, axis=-1, keepdims=True)

        total = lax.fori_loop(0, b + 1, second, jnp.zeros((QB, 1), jnp.float32))
        inv = 1.0 / total
        acc[0:QB, :] = jnp.zeros((QB, hd), jnp.float32)

        @pl.loop(0, b + 1)
        def _(t):
            p = (scores[t] * inv).astype(jnp.bfloat16)
            acc[0:QB, :] += jnp.dot(p, v[tile(t), :], preferred_element_type=jnp.float32)

        az[tile(b), 0:hd] = acc[0:QB, :].astype(jnp.bfloat16)

    n_q = seq // QB

    @pl.loop(1, n_chunk + 1)
    def _(i):
        @pl.when(i < n_chunk)
        def _():
            net_a(i)

        net_b(i - 1)

        @pl.when(i == 4)
        def _():
            attend(0)

        @pl.when(jnp.logical_and(i >= 4, i < 4 + n_q - 1))
        def _():
            attend(i - 3)

        ready(i - 1)
        compute(i - 1)


def project_call(x, positions, norm_gain, w_query, w_key, w_value, w_gate, w_up):
    seq, d = x.shape
    depth, hd = w_query.shape
    ff = w_gate.shape[1]
    n_chunk = 3 + ff // GU
    inv_freq = 10000.0 ** (-jnp.arange(0, hd, 2, dtype=jnp.float32) / hd)
    bf, f32 = jnp.bfloat16, jnp.float32
    hbm = pl.BlockSpec(memory_space=pl.ANY)
    vm = pl.BlockSpec(memory_space=pltpu.VMEM)
    flops = 2 * seq * d * (3 * hd + 2 * ff) + 2 * seq * seq * hd
    return pl.pallas_call(
        project_kernel,
        out_shape=jax.ShapeDtypeStruct((seq, hd + ff), bf),
        in_specs=[hbm, vm, vm] + [hbm] * 6,
        out_specs=vm,
        scratch_shapes=[
            pltpu.VMEM((n_chunk, d, hd), bf),
            pltpu.VMEM((seq, d), bf),
            pltpu.VMEM((seq, hd), bf),
            pltpu.VMEM((seq, hd), bf),
            pltpu.VMEM((seq, hd), bf),
            pltpu.VMEM((seq, hd // 2), f32),
            pltpu.VMEM((seq, hd // 2), f32),
            pltpu.VMEM((1, d), f32),
            pltpu.VMEM((2, LN_ROWS, d), bf),
            pltpu.VMEM((seq // QB, QB, QB), f32),
            pltpu.VMEM((M1, hd), f32),
            pltpu.SemaphoreType.DMA((n_chunk, 8)),
            pltpu.SemaphoreType.DMA((n_chunk, 8)),
            pltpu.SemaphoreType.DMA((8,)),
            pltpu.SemaphoreType.DMA((8,)),
            pltpu.SemaphoreType.DMA((n_chunk, 2)),
            pltpu.SemaphoreType.DMA,
            pltpu.SemaphoreType.DMA((2,)),
        ],
        compiler_params=pltpu.CompilerParams(collective_id=0, has_side_effects=True, vmem_limit_bytes=63 * 1024 * 1024),
        cost_estimate=pl.CostEstimate(flops=flops, bytes_accessed=2 * seq * d, transcendentals=0),
        name="gather_project",
    )(x, positions.reshape(seq, 1), inv_freq.reshape(1, hd // 2), norm_gain.reshape(1, depth), w_query, w_key, w_value, w_gate, w_up)


def reduce_kernel(az, x_hbm, wo, wd, out, wbuf, part, r1, r2, r3, r4, ybuf, xbuf,
                  ssem, rsem, wss, wrs, lsem, osem):
    t = lax.axis_index("tp")
    f = lax.axis_index("fsdp")
    ring_y, ring_z = _ring_ids(t)
    xc, core, f_p, f_r, f_l = _fsdp_ids(f)
    seq = az.shape[0]
    cols = wbuf.shape[2]
    half = seq // 2
    big = half // TPA
    small = big // TPA
    hd = wo.shape[0]

    ld_o = pltpu.make_async_copy(wo, wbuf.at[0, pl.ds(0, hd)], lsem.at[0])
    ld_d = pltpu.make_async_copy(wd, wbuf.at[0, pl.ds(hd, wd.shape[0])], lsem.at[1])
    ld_o.start()
    ld_d.start()
    axes = ((ring_y, ring_z), (ring_z, ring_y))

    def own_rows(h):
        (i1, _, _), (i2, _, _) = axes[h]
        return pl.multiple_of(h * half + i1 * big + i2 * small, small)

    ld_x = [pltpu.make_async_copy(x_hbm.at[pl.ds(own_rows(h), small), :], xbuf.at[h], lsem.at[2 + h]) for h in range(2)]
    for c in ld_x:
        c.start()

    barrier = pltpu.get_barrier_semaphore()
    for other in (ring_y[1], ring_y[2], ring_z[1], ring_z[2]):
        pl.semaphore_signal(barrier, inc=1, device_id={"tp": other}, device_id_type=MESH)
    for other in (f_p, f_r, f_l):
        pl.semaphore_signal(barrier, inc=1, device_id={"fsdp": other}, device_id_type=MESH)
    pl.semaphore_wait(barrier, 7)

    def wcopy(k, src, dst, dev):
        return pltpu.make_async_remote_copy(src_ref=src, dst_ref=dst, send_sem=wss.at[k], recv_sem=wrs.at[k],
                                            device_id={"fsdp": dev}, device_id_type=MESH)

    kk = wbuf.shape[1]
    kh = kk // 2
    top, bot = pl.ds(0, kh), pl.ds(kh, kh)
    w_own_p = wcopy(0, wbuf.at[0], wbuf.at[1], f_p)
    w_own_r = wcopy(1, wbuf.at[0], wbuf.at[2], f_r)
    w_own_l = wcopy(2, wbuf.at[0], wbuf.at[4], f_l)
    w_2p = wcopy(3, wbuf.at[2], wbuf.at[3], f_p)
    w_4p = wcopy(4, wbuf.at[4], wbuf.at[5], f_p)
    w_2r = wcopy(5, wbuf.at[2, top], wbuf.at[6, top], f_r)
    w_4l = wcopy(6, wbuf.at[4, bot], wbuf.at[6, bot], f_l)
    w_6p = wcopy(7, wbuf.at[6], wbuf.at[7], f_p)
    ld_o.wait()
    ld_d.wait()
    w_own_r.start()
    w_own_l.start()
    w_own_p.start()
    for c in ld_x:
        c.wait()

    def block_of(k):
        q = k // 2
        dx = 3 * q - 5 * (q // 2) - 2 * (q // 3)
        return ((xc + dx) % 4) * 2 + (core + k % 2) % 2

    def ring_copy(cb, h, d, step, src, dst, dev):
        return pltpu.make_async_remote_copy(src_ref=src, dst_ref=dst, send_sem=ssem.at[cb, h, d, step],
                                            recv_sem=rsem.at[cb, h, d, step], device_id={"tp": dev}, device_id_type=MESH)

    def rs_first(cb, h, step, ring, base, n, land):
        i, r, l = ring
        o = (i + 2) % TPA
        m = n // 2
        s = pl.multiple_of(base + o * n, m)
        return (ring_copy(cb, h, 0, step, part.at[cb, pl.ds(s, m)], land.at[cb, h, 0], r),
                ring_copy(cb, h, 1, step, part.at[cb, pl.ds(s + m, m)], land.at[cb, h, 1], l))

    def rs_second(cb, h, step, ring, base, n, land):
        i, r, l = ring
        s_r = pl.multiple_of(base + ((i + 1) % TPA) * n, n)
        s_l = pl.multiple_of(base + ((i + 3) % TPA) * n, n)
        return (ring_copy(cb, h, 0, step, part.at[cb, pl.ds(s_r, n)], land.at[cb, h, 0], r),
                ring_copy(cb, h, 1, step, part.at[cb, pl.ds(s_l, n)], land.at[cb, h, 1], l))

    def rs_update(cb, h, ring, base, n, land):
        i, _, _ = ring
        m = n // 2
        s_r = pl.multiple_of(base + ((i + 1) % TPA) * n, m)
        s_l = pl.multiple_of(base + ((i + 3) % TPA) * n + m, m)
        for s, d in ((s_r, 0), (s_l, 1)):
            rows = pl.ds(s, m)
            part[cb, rows] = (part[cb, rows].astype(jnp.float32) + land[cb, h, d].astype(jnp.float32)).astype(jnp.bfloat16)

    def ag_first(cb, h, step, ring, src, base, n):
        i, r, l = ring
        g = block_of(cb)
        dst = out.at[g, pl.ds(pl.multiple_of(base + i * n, n), n)]
        if src is None:
            src = dst
        return (ring_copy(cb, h, 0, step, src, dst, r), ring_copy(cb, h, 1, step, src, dst, l))

    def ag_second(cb, h, step, ring, base, n):
        i, r, l = ring
        g = block_of(cb)
        m = n // 2
        from_l = out.at[g, pl.ds(pl.multiple_of(base + ((i + 3) % TPA) * n, m), m)]
        from_r = out.at[g, pl.ds(pl.multiple_of(base + ((i + 1) % TPA) * n + m, m), m)]
        return (ring_copy(cb, h, 0, step, from_l, from_l, r), ring_copy(cb, h, 1, step, from_r, from_r, l))

    def copies(cb, step):
        res = []
        for h in range(2):
            ring1, ring2 = axes[h]
            base1 = h * half
            base2 = pl.multiple_of(h * half + ring1[0] * big, big)
            if step == 0:
                res.extend(rs_first(cb, h, step, ring1, base1, big, r1))
            elif step == 1:
                res.extend(rs_second(cb, h, step, ring1, base1, big, r2))
            elif step == 2:
                res.extend(rs_first(cb, h, step, ring2, base2, small, r3))
            elif step == 3:
                res.extend(rs_second(cb, h, step, ring2, base2, small, r4))
            elif step == 4:
                res.extend(ag_first(cb, h, step, ring2, ybuf.at[cb, h], base2, small))
            elif step == 5:
                res.extend(ag_second(cb, h, step, ring2, base2, small))
            elif step == 6:
                res.extend(ag_first(cb, h, step, ring1, None, base1, big))
            else:
                res.extend(ag_second(cb, h, step, ring1, base1, big))
        return res

    def start(cb, step):
        for c in copies(cb, step):
            c.start()

    def finish(cb, step):
        for c in copies(cb, step):
            c.wait_recv()
            c.wait_send()

    def own_out(cb, h):
        return pltpu.make_async_copy(ybuf.at[cb, h], out.at[block_of(cb), pl.ds(own_rows(h), small)], osem.at[cb, h])

    def stage0(cb):
        @pl.when(cb == 1)
        def _():
            w_own_p.wait()

        @pl.when(cb == 2)
        def _():
            w_own_r.wait()
            w_own_l.wait()
            w_2r.start()
            w_4l.start()
            w_2p.start()
            w_4p.start()

        @pl.when(cb == 3)
        def _():
            w_2p.wait()

        @pl.when(cb == 5)
        def _():
            w_4p.wait()

        @pl.when(cb == 6)
        def _():
            w_2r.wait()
            w_4l.wait()
            w_6p.start()

        @pl.when(cb == 7)
        def _():
            w_6p.wait()

        @pl.loop(0, seq // MT)
        def _(i):
            rows = pl.ds(pl.multiple_of(i * MT, MT), MT)
            part[cb, rows] = jnp.dot(az[rows, :], wbuf[cb], preferred_element_type=jnp.float32).astype(jnp.bfloat16)

        start(cb, 0)

    def stage1(cb):
        finish(cb, 0)
        for h in range(2):
            rs_update(cb, h, axes[h][0], h * half, big, r1)
        start(cb, 1)

    def stage2(cb):
        finish(cb, 1)
        for h in range(2):
            rows = pl.ds(pl.multiple_of(h * half + axes[h][0][0] * big, big), big)
            part[cb, rows] = (part[cb, rows].astype(jnp.float32) + r2[cb, h, 0].astype(jnp.float32)
                              + r2[cb, h, 1].astype(jnp.float32)).astype(jnp.bfloat16)
        start(cb, 2)

    def stage3(cb):
        finish(cb, 2)
        for h in range(2):
            rs_update(cb, h, axes[h][1], pl.multiple_of(h * half + axes[h][0][0] * big, big), small, r3)
        start(cb, 3)

    def stage4(cb):
        finish(cb, 3)
        g = block_of(cb)
        for h in range(2):
            branch = (part[cb, pl.ds(own_rows(h), small)].astype(jnp.float32) + r4[cb, h, 0].astype(jnp.float32)
                      + r4[cb, h, 1].astype(jnp.float32))
            xs = xbuf[h, :, pl.ds(pl.multiple_of(g * cols, cols), cols)].astype(jnp.float32)
            ybuf[cb, h] = (xs + branch).astype(jnp.bfloat16)
            own_out(cb, h).start()
        start(cb, 4)

    def stage5(cb):
        finish(cb, 4)
        start(cb, 5)

    def stage6(cb):
        finish(cb, 5)
        for h in range(2):
            own_out(cb, h).wait()
        start(cb, 6)

    def stage7(cb):
        finish(cb, 6)
        start(cb, 7)

    def stage8(cb):
        finish(cb, 7)

    stages = (stage0, stage1, stage2, stage3, stage4, stage5, stage6, stage7, stage8)

    @pl.loop(0, COL + len(stages) - 1)
    def _(n):
        for s, fn in enumerate(stages):
            cb = n - s

            @pl.when(jnp.logical_and(cb >= 0, cb < COL))
            def _(fn=fn, cb=cb):
                fn(cb)


MT = 512


def reduce_call(az, x, wo, wd):
    seq, kk = az.shape
    d = x.shape[1]
    cols = d // COL
    half = seq // 2
    big, small = half // TPA, half // TPA // TPA
    bf = jnp.bfloat16
    hbm = pl.BlockSpec(memory_space=pl.ANY)
    vm = pl.BlockSpec(memory_space=pltpu.VMEM)
    res = pl.pallas_call(
        reduce_kernel,
        out_shape=jax.ShapeDtypeStruct((COL, seq, cols), bf),
        in_specs=[vm, hbm, hbm, hbm],
        out_specs=hbm,
        scratch_shapes=[
            pltpu.VMEM((COL, kk, cols), bf),
            pltpu.VMEM((COL, seq, cols), bf),
            pltpu.VMEM((COL, 2, 2, big // 2, cols), bf),
            pltpu.VMEM((COL, 2, 2, big, cols), bf),
            pltpu.VMEM((COL, 2, 2, small // 2, cols), bf),
            pltpu.VMEM((COL, 2, 2, small, cols), bf),
            pltpu.VMEM((COL, 2, small, cols), bf),
            pltpu.VMEM((2, small, d), bf),
            pltpu.SemaphoreType.DMA((COL, 2, 2, 8)),
            pltpu.SemaphoreType.DMA((COL, 2, 2, 8)),
            pltpu.SemaphoreType.DMA((8,)),
            pltpu.SemaphoreType.DMA((8,)),
            pltpu.SemaphoreType.DMA((4,)),
            pltpu.SemaphoreType.DMA((COL, 2)),
        ],
        compiler_params=pltpu.CompilerParams(collective_id=1, has_side_effects=True, vmem_limit_bytes=60 * 1024 * 1024),
        cost_estimate=pl.CostEstimate(flops=2 * seq * kk * d, bytes_accessed=4 * seq * d, transcendentals=0),
        name="down_reduce",
    )(az, x, wo, wd)
    return repack(res)[None]


def repack_kernel(src, dst):
    cols = src.shape[2]
    for b in range(COL):
        dst[:, b * cols:(b + 1) * cols] = src[b]


def repack(blocks):
    n, seq, cols = blocks.shape
    rows = 128
    return pl.pallas_call(
        repack_kernel,
        grid=(seq // rows,),
        out_shape=jax.ShapeDtypeStruct((seq, n * cols), blocks.dtype),
        in_specs=[pl.BlockSpec((n, rows, cols), lambda i: (0, i, 0))],
        out_specs=pl.BlockSpec((rows, n * cols), lambda i: (i, 0)),
        name="repack",
    )(blocks)


def solution(mesh):
    row_spec = P(("dp", "fsdp"), None, None)

    def local_layer(hidden, positions, norm_gain, w_query, w_key, w_value, w_gate, w_up, w_out, w_down):
        az = project_call(hidden[0], positions, norm_gain, w_query, w_key, w_value, w_gate, w_up)
        return reduce_call(az, hidden[0], w_out, w_down)

    in_specs = (row_spec, P(None), P("fsdp"), P("fsdp", "tp"), P("fsdp", None), P("fsdp", None), P("fsdp", "tp"), P("fsdp", "tp"), P("tp", "fsdp"), P("tp", "fsdp"))
    return jax.shard_map(local_layer, mesh=mesh, in_specs=in_specs, out_specs=row_spec, check_vma=False)
```

```python
import jax
import jax.numpy as jnp
import numpy as np
from jax import lax
from jax.experimental import pallas as pl
from jax.experimental.pallas import tpu as pltpu
from jax.sharding import PartitionSpec as P

NORM_EPS = 1e-6
MESH = pl.DeviceIdType.MESH
TPA = 4
COL = 8


def _ring_ids(t):
    z, y = t // TPA, t % TPA
    y_r, y_l = z * TPA + (y + 1) % TPA, z * TPA + (y + 3) % TPA
    z_r, z_l = ((z + 1) % TPA) * TPA + y, ((z + 3) % TPA) * TPA + y
    return (y, y_r, y_l), (z, z_r, z_l)


def _fsdp_ids(f):
    xc, core = f // 2, f % 2
    f_p = xc * 2 + (1 - core)
    f_r = ((xc + 1) % 4) * 2 + core
    f_l = ((xc + 3) % 4) * 2 + core
    return xc, core, f_p, f_r, f_l


QB = 256
LN_ROWS = 128
X_SLOTS = 4
LN_SUB = 64
GU = 128
M1 = 1024


def project_kernel(x_hbm, pos, inv_freq, gain, wq, wk, wv, wg, wu, az, wbuf, h, q, k, v, cos_t, sin_t, gbuf, xb, scores, acc,
                   ssem, rsem, gss, grs, lsem, gsem, xsem):
    f = lax.axis_index("fsdp")
    nf = lax.axis_size("fsdp")
    xc, core, f_p, f_r, f_l = _fsdp_ids(f)
    f_o = ((xc + 2) % 4) * 2 + core
    seq, d = h.shape
    depth = wq.shape[0]
    mid = depth // 2
    hd = wq.shape[1]
    n_chunk = wbuf.shape[0]
    n_ff = wg.shape[1] // GU

    def rows_of(dev):
        return pl.ds(pl.multiple_of(dev * depth, depth), depth)

    def half_of(dev, part):
        return pl.ds(pl.multiple_of(dev * depth + part * mid, mid), mid)

    def load(i, part, src, col):
        return pltpu.make_async_copy(src.at[:, pl.ds(col, GU)], wbuf.at[i, rows_of(f), pl.ds(part * GU, GU)], lsem.at[i, part])

    for i, w in enumerate((wq, wk, wv)):
        for part in range(2):
            load(i, part, w, part * GU).start()
    for j in range(n_ff):
        load(3 + j, 0, wg, j * GU).start()
        load(3 + j, 1, wu, j * GU).start()

    def load_x(blk):
        slot = blk % X_SLOTS
        return pltpu.make_async_copy(x_hbm.at[pl.ds(pl.multiple_of(blk * LN_ROWS, LN_ROWS), LN_ROWS), :], xb.at[slot], xsem.at[slot])

    for blk in range(X_SLOTS - 1):
        load_x(blk).start()
    ld_g = pltpu.make_async_copy(gain, gbuf.at[:, pl.ds(pl.multiple_of(f * depth, depth), depth)], gsem)
    ld_g.start()

    barrier = pltpu.get_barrier_semaphore()
    for e in range(1, nf):
        pl.semaphore_signal(barrier, inc=1, device_id={"fsdp": (f + e) % nf}, device_id_type=MESH)
    pl.semaphore_wait(barrier, nf - 1)

    def rcopy(i, s, src, dev):
        return pltpu.make_async_remote_copy(src_ref=src, dst_ref=src, send_sem=ssem.at[i, s], recv_sem=rsem.at[i, s],
                                            device_id={"fsdp": dev}, device_id_type=MESH)

    def transfer(i, s):
        src, dev = (
            (lambda: wbuf.at[i, rows_of(f)], f_r),
            (lambda: wbuf.at[i, rows_of(f)], f_l),
            (lambda: wbuf.at[i, rows_of(f)], f_p),
            (lambda: wbuf.at[i, half_of(f_l, 0)], f_r),
            (lambda: wbuf.at[i, half_of(f_r, 1)], f_l),
            (lambda: wbuf.at[i, rows_of(f_l)], f_p),
            (lambda: wbuf.at[i, rows_of(f_r)], f_p),
            (lambda: wbuf.at[i, rows_of(f_o)], f_p),
        )[s]
        return rcopy(i, s, src(), dev)

    def send_own(i):
        for part in range(2):
            load(i, part, wq, part * GU).wait()
        for s in range(3):
            transfer(i, s).start()

    def net_a(i):
        transfer(i, 0).wait_recv()
        transfer(i, 3).start()
        transfer(i, 1).wait_recv()
        transfer(i, 4).start()

        @pl.when(i + 2 < n_chunk)
        def _():
            send_own(i + 2)

        transfer(i, 5).start()
        transfer(i, 6).start()

    def net_b(i):
        transfer(i, 3).wait_recv()
        transfer(i, 4).wait_recv()
        transfer(i, 7).start()

    def ready(i):
        for s in (2, 5, 6, 7):
            transfer(i, s).wait_recv()
        for s in range(8):
            transfer(i, s).wait_send()

    ld_g.wait()
    gcol = gbuf.at[:, pl.ds(pl.multiple_of(f * depth, depth), depth)]
    gcopies = [pltpu.make_async_remote_copy(src_ref=gcol, dst_ref=gcol, send_sem=gss.at[e], recv_sem=grs.at[e],
                                            device_id={"fsdp": (f + e) % nf}, device_id_type=MESH) for e in range(1, nf)]
    for c in gcopies:
        c.start()
    send_own(0)
    send_own(1)

    lanes = pos.shape[1]
    eye = lax.broadcasted_iota(jnp.int32, (lanes, lanes), 0) == lax.broadcasted_iota(jnp.int32, (lanes, lanes), 1)

    @pl.loop(0, seq // lanes)
    def _(b):
        rows = pl.ds(pl.multiple_of(b * lanes, lanes), lanes)
        line = pos[pl.ds(b, 1), :].astype(jnp.float32)
        column = jnp.sum(jnp.where(eye, line, 0.0), axis=-1, keepdims=True)
        angle = column * inv_freq[...]
        cos_t[rows, :] = jnp.cos(angle)
        sin_t[rows, :] = jnp.sin(angle)

    for c in gcopies:
        c.wait()

    n_blk = seq // LN_ROWS

    def norm_blocks(lo, hi):
        @pl.loop(lo, hi)
        def _(blk):
            load_x(blk).wait()

            @pl.when(blk + X_SLOTS - 1 < n_blk)
            def _():
                load_x(blk + X_SLOTS - 1).start()

            @pl.loop(0, LN_ROWS // LN_SUB)
            def _(r):
                row = xb[blk % X_SLOTS, pl.ds(pl.multiple_of(r * LN_SUB, LN_SUB), LN_SUB), :].astype(jnp.float32)
                centered = row - jnp.sum(row, axis=-1, keepdims=True) * (1.0 / d)
                var = jnp.sum(centered * centered, axis=-1, keepdims=True) * (1.0 / d)
                out = centered * lax.rsqrt(var + NORM_EPS) * gbuf[...]
                h[pl.ds(pl.multiple_of(blk * LN_ROWS + r * LN_SUB, LN_SUB), LN_SUB), :] = out.astype(jnp.bfloat16)

    norm_blocks(0, n_blk // 2)
    net_a(0)
    norm_blocks(n_blk // 2, n_blk)

    def rope(rows):
        y = acc[...].astype(jnp.bfloat16).astype(jnp.float32)
        a, b = y[:, :hd // 2], y[:, hd // 2:]
        c, s = cos_t[rows, :], sin_t[rows, :]
        return jnp.concatenate([a * c - b * s, b * c + a * s], axis=1).astype(jnp.bfloat16)

    def compute(i):
        @pl.loop(0, seq // M1)
        def _(m):
            rows = pl.ds(pl.multiple_of(m * M1, M1), M1)
            acc[...] = jnp.dot(h[rows, :], wbuf[i], preferred_element_type=jnp.float32)

            @pl.when(i == 0)
            def _():
                q[rows, :] = rope(rows)

            @pl.when(i == 1)
            def _():
                k[rows, :] = rope(rows)

            @pl.when(i == 2)
            def _():
                v[rows, :] = acc[...].astype(jnp.bfloat16)

            @pl.when(i >= 3)
            def _():
                g = acc[:, :GU].astype(jnp.bfloat16).astype(jnp.float32)
                u = acc[:, GU:].astype(jnp.bfloat16).astype(jnp.float32)
                z = (g * (1.0 / (1.0 + jnp.exp(-g)))) * u
                az[rows, pl.ds(pl.multiple_of(hd + (i - 3) * GU, GU), GU)] = z.astype(jnp.bfloat16)

    scale = hd ** -0.5
    n_q = seq // QB

    def attend(b):
        rows = pl.ds(b * QB, QB)
        qb = q[rows, :]
        peak = None
        for t in range(b + 1):
            s = lax.dot_general(qb, k[pl.ds(t * QB, QB), :], (((1,), (1,)), ((), ())), preferred_element_type=jnp.float32) * scale
            if t == b:
                keep = lax.broadcasted_iota(jnp.int32, (QB, QB), 1) <= lax.broadcasted_iota(jnp.int32, (QB, QB), 0)
                s = jnp.where(keep, s, -1e30)
            scores[:, t * QB:(t + 1) * QB] = s
            s = jnp.maximum(s[:, :128], s[:, 128:])
            peak = s if peak is None else jnp.maximum(peak, s)
        peak = jnp.max(peak, axis=-1, keepdims=True)
        total = None
        for t in range(b + 1):
            e = jnp.exp(scores[:, t * QB:(t + 1) * QB] - peak)
            scores[:, t * QB:(t + 1) * QB] = e
            e = e[:, :128] + e[:, 128:]
            total = e if total is None else total + e
        inv = 1.0 / jnp.sum(total, axis=-1, keepdims=True)
        p = (scores[:, :(b + 1) * QB] * inv).astype(jnp.bfloat16)
        out = jnp.dot(p, v[pl.ds(0, (b + 1) * QB), :], preferred_element_type=jnp.float32)
        az[rows, 0:hd] = out.astype(jnp.bfloat16)

    @pl.loop(1, n_chunk + 1)
    def _(i):
        @pl.when(i < n_chunk)
        def _():
            net_a(i)

        net_b(i - 1)

        for b in range(n_q):
            @pl.when(i == (3 + b if b else 4))
            def _(b=b):
                attend(b)

        ready(i - 1)
        compute(i - 1)


def project_call(x, positions, norm_gain, w_query, w_key, w_value, w_gate, w_up):
    seq, d = x.shape
    depth, hd = w_query.shape
    ff = w_gate.shape[1]
    n_chunk = 3 + ff // GU
    inv_freq = jnp.asarray((10000.0 ** (-np.arange(0, hd, 2) / hd)).astype(np.float32))
    bf, f32 = jnp.bfloat16, jnp.float32
    hbm = pl.BlockSpec(memory_space=pl.ANY)
    vm = pl.BlockSpec(memory_space=pltpu.VMEM)
    flops = 2 * seq * d * (3 * hd + 2 * ff) + 2 * seq * seq * hd
    return pl.pallas_call(
        project_kernel,
        out_shape=jax.ShapeDtypeStruct((seq, hd + ff), bf),
        in_specs=[hbm, vm, vm] + [hbm] * 6,
        out_specs=vm,
        scratch_shapes=[
            pltpu.VMEM((n_chunk, d, hd), bf),
            pltpu.VMEM((seq, d), bf),
            pltpu.VMEM((seq, hd), bf),
            pltpu.VMEM((seq, hd), bf),
            pltpu.VMEM((seq, hd), bf),
            pltpu.VMEM((seq, hd // 2), f32),
            pltpu.VMEM((seq, hd // 2), f32),
            pltpu.VMEM((1, d), f32),
            pltpu.VMEM((X_SLOTS, LN_ROWS, d), bf),
            pltpu.VMEM((QB, seq), f32),
            pltpu.VMEM((M1, hd), f32),
            pltpu.SemaphoreType.DMA((n_chunk, 8)),
            pltpu.SemaphoreType.DMA((n_chunk, 8)),
            pltpu.SemaphoreType.DMA((8,)),
            pltpu.SemaphoreType.DMA((8,)),
            pltpu.SemaphoreType.DMA((n_chunk, 2)),
            pltpu.SemaphoreType.DMA,
            pltpu.SemaphoreType.DMA((X_SLOTS,)),
        ],
        compiler_params=pltpu.CompilerParams(collective_id=0, has_side_effects=True, vmem_limit_bytes=63 * 1024 * 1024),
        cost_estimate=pl.CostEstimate(flops=flops, bytes_accessed=2 * seq * d, transcendentals=0),
        name="gather_project",
    )(x, positions.reshape(seq // 128, 128), inv_freq.reshape(1, hd // 2), norm_gain.reshape(1, depth), w_query, w_key, w_value, w_gate, w_up)


def reduce_kernel(az, x_hbm, wo, wd, out, wbuf, part, r1, r2, r3, r4, xbuf,
                  ssem, rsem, wss, wrs, lsem):
    t = lax.axis_index("tp")
    f = lax.axis_index("fsdp")
    ring_y, ring_z = _ring_ids(t)
    xc, core, f_p, f_r, f_l = _fsdp_ids(f)
    seq = az.shape[0]
    cols = wbuf.shape[2]
    half = seq // 2
    big = half // TPA
    small = big // TPA
    hd = wo.shape[0]

    ld_o = pltpu.make_async_copy(wo, wbuf.at[0, pl.ds(0, hd)], lsem.at[0])
    ld_d = pltpu.make_async_copy(wd, wbuf.at[0, pl.ds(hd, wd.shape[0])], lsem.at[1])
    ld_o.start()
    ld_d.start()
    axes = ((ring_y, ring_z), (ring_z, ring_y))

    def own_rows(h):
        (i1, _, _), (i2, _, _) = axes[h]
        return pl.multiple_of(h * half + i1 * big + i2 * small, small)

    ld_x = [pltpu.make_async_copy(x_hbm.at[pl.ds(own_rows(h), small), :], xbuf.at[h], lsem.at[2 + h]) for h in range(2)]
    for c in ld_x:
        c.start()

    barrier = pltpu.get_barrier_semaphore()
    for other in (ring_y[1], ring_y[2], ring_z[1], ring_z[2]):
        pl.semaphore_signal(barrier, inc=1, device_id={"tp": other}, device_id_type=MESH)
    for other in (f_p, f_r, f_l):
        pl.semaphore_signal(barrier, inc=1, device_id={"fsdp": other}, device_id_type=MESH)
    pl.semaphore_wait(barrier, 7)

    def wcopy(k, src, dst, dev):
        return pltpu.make_async_remote_copy(src_ref=src, dst_ref=dst, send_sem=wss.at[k], recv_sem=wrs.at[k],
                                            device_id={"fsdp": dev}, device_id_type=MESH)

    kk = wbuf.shape[1]
    kh = kk // 2
    top, bot = pl.ds(0, kh), pl.ds(kh, kh)
    w_own_p = wcopy(0, wbuf.at[0], wbuf.at[1], f_p)
    w_own_r = wcopy(1, wbuf.at[0], wbuf.at[2], f_r)
    w_own_l = wcopy(2, wbuf.at[0], wbuf.at[4], f_l)
    w_2p = wcopy(3, wbuf.at[2], wbuf.at[3], f_p)
    w_4p = wcopy(4, wbuf.at[4], wbuf.at[5], f_p)
    w_2r = wcopy(5, wbuf.at[2, top], wbuf.at[6, top], f_r)
    w_4l = wcopy(6, wbuf.at[4, bot], wbuf.at[6, bot], f_l)
    w_6p = wcopy(7, wbuf.at[6], wbuf.at[7], f_p)
    ld_o.wait()
    ld_d.wait()
    w_own_r.start()
    w_own_l.start()
    w_own_p.start()
    for c in ld_x:
        c.wait()

    def block_of(k):
        q = k // 2
        dx = 3 * q - 5 * (q // 2) - 2 * (q // 3)
        return ((xc + dx) % 4) * 2 + (core + k % 2) % 2

    def ring_copy(cb, h, d, step, src, dst, dev):
        return pltpu.make_async_remote_copy(src_ref=src, dst_ref=dst, send_sem=ssem.at[cb, h, d, step],
                                            recv_sem=rsem.at[cb, h, d, step], device_id={"tp": dev}, device_id_type=MESH)

    def rs_first(cb, h, step, ring, base, n, land):
        i, r, l = ring
        o = (i + 2) % TPA
        m = n // 2
        s = pl.multiple_of(base + o * n, m)
        return (ring_copy(cb, h, 0, step, part.at[cb % PART_SLOTS, pl.ds(s, m)], land.at[cb % land.shape[0], h, 0], r),
                ring_copy(cb, h, 1, step, part.at[cb % PART_SLOTS, pl.ds(s + m, m)], land.at[cb % land.shape[0], h, 1], l))

    def rs_second(cb, h, step, ring, base, n, land):
        i, r, l = ring
        s_r = pl.multiple_of(base + ((i + 1) % TPA) * n, n)
        s_l = pl.multiple_of(base + ((i + 3) % TPA) * n, n)
        return (ring_copy(cb, h, 0, step, part.at[cb % PART_SLOTS, pl.ds(s_r, n)], land.at[cb % land.shape[0], h, 0], r),
                ring_copy(cb, h, 1, step, part.at[cb % PART_SLOTS, pl.ds(s_l, n)], land.at[cb % land.shape[0], h, 1], l))

    def rs_update(cb, h, ring, base, n, land):
        i, _, _ = ring
        m = n // 2
        s_r = pl.multiple_of(base + ((i + 1) % TPA) * n, m)
        s_l = pl.multiple_of(base + ((i + 3) % TPA) * n + m, m)
        for s, d in ((s_r, 0), (s_l, 1)):
            rows = pl.ds(s, m)
            part[cb % PART_SLOTS, rows] = (part[cb % PART_SLOTS, rows].astype(jnp.float32) + land[cb % land.shape[0], h, d].astype(jnp.float32)).astype(jnp.bfloat16)

    def ag_first(cb, h, step, ring, src, base, n):
        i, r, l = ring
        g = block_of(cb)
        dst = out.at[g, pl.ds(pl.multiple_of(base + i * n, n), n)]
        if src is None:
            src = dst
        return (ring_copy(cb, h, 0, step, src, dst, r), ring_copy(cb, h, 1, step, src, dst, l))

    def ag_second(cb, h, step, ring, base, n):
        i, r, l = ring
        g = block_of(cb)
        m = n // 2
        from_l = out.at[g, pl.ds(pl.multiple_of(base + ((i + 3) % TPA) * n, m), m)]
        from_r = out.at[g, pl.ds(pl.multiple_of(base + ((i + 1) % TPA) * n + m, m), m)]
        return (ring_copy(cb, h, 0, step, from_l, from_l, r), ring_copy(cb, h, 1, step, from_r, from_r, l))

    def copies(cb, step):
        res = []
        for h in range(2):
            ring1, ring2 = axes[h]
            base1 = h * half
            base2 = pl.multiple_of(h * half + ring1[0] * big, big)
            if step == 0:
                res.extend(rs_first(cb, h, step, ring1, base1, big, r1))
            elif step == 1:
                res.extend(rs_second(cb, h, step, ring1, base1, big, r2))
            elif step == 2:
                res.extend(rs_first(cb, h, step, ring2, base2, small, r3))
            elif step == 3:
                res.extend(rs_second(cb, h, step, ring2, base2, small, r4))
            elif step == 4:
                res.extend(ag_first(cb, h, step, ring2, None, base2, small))
            elif step == 5:
                res.extend(ag_second(cb, h, step, ring2, base2, small))
            elif step == 6:
                res.extend(ag_first(cb, h, step, ring1, None, base1, big))
            else:
                res.extend(ag_second(cb, h, step, ring1, base1, big))
        return res

    def start(cb, step):
        for c in copies(cb, step):
            c.start()

    def finish(cb, step):
        for c in copies(cb, step):
            c.wait_recv()
            c.wait_send()

    def stage0(cb):
        @pl.when(cb == 1)
        def _():
            w_own_p.wait()

        @pl.when(cb == 2)
        def _():
            w_own_r.wait()
            w_own_l.wait()
            w_2r.start()
            w_4l.start()
            w_2p.start()
            w_4p.start()

        @pl.when(cb == 3)
        def _():
            w_2p.wait()

        @pl.when(cb == 5)
        def _():
            w_4p.wait()

        @pl.when(cb == 6)
        def _():
            w_2r.wait()
            w_4l.wait()
            w_6p.start()

        @pl.when(cb == 7)
        def _():
            w_6p.wait()

        @pl.loop(0, seq // MT)
        def _(i):
            rows = pl.ds(pl.multiple_of(i * MT, MT), MT)
            part[cb % PART_SLOTS, rows] = jnp.dot(az[rows, :], wbuf[cb], preferred_element_type=jnp.float32).astype(jnp.bfloat16)

        start(cb, 0)

    def stage1(cb):
        finish(cb, 0)
        for h in range(2):
            rs_update(cb, h, axes[h][0], h * half, big, r1)
        start(cb, 1)

    def stage2(cb):
        finish(cb, 1)
        for h in range(2):
            rows = pl.ds(pl.multiple_of(h * half + axes[h][0][0] * big, big), big)
            part[cb % PART_SLOTS, rows] = (part[cb % PART_SLOTS, rows].astype(jnp.float32) + r2[cb % r2.shape[0], h, 0].astype(jnp.float32)
                              + r2[cb % r2.shape[0], h, 1].astype(jnp.float32)).astype(jnp.bfloat16)
        start(cb, 2)

    def stage3(cb):
        finish(cb, 2)
        for h in range(2):
            rs_update(cb, h, axes[h][1], pl.multiple_of(h * half + axes[h][0][0] * big, big), small, r3)
        start(cb, 3)

    def stage4(cb):
        finish(cb, 3)
        g = block_of(cb)
        for h in range(2):
            branch = (part[cb % PART_SLOTS, pl.ds(own_rows(h), small)].astype(jnp.float32) + r4[cb % r4.shape[0], h, 0].astype(jnp.float32)
                      + r4[cb % r4.shape[0], h, 1].astype(jnp.float32))
            xs = xbuf[h, :, pl.ds(pl.multiple_of(g * cols, cols), cols)].astype(jnp.float32)
            out[g, pl.ds(own_rows(h), small), :] = (xs + branch).astype(jnp.bfloat16)
        start(cb, 4)

    def stage5(cb):
        finish(cb, 4)
        start(cb, 5)

    def stage6(cb):
        finish(cb, 5)
        start(cb, 6)

    def stage7(cb):
        finish(cb, 6)
        start(cb, 7)

    def stage8(cb):
        finish(cb, 7)

    stages = (stage0, stage1, stage2, stage3, stage4, stage5, stage6, stage7, stage8)

    @pl.loop(0, COL + GAP + len(stages) - 1)
    def _(n):
        for s, fn in enumerate(stages):
            turn = n - s

            @pl.when(jnp.logical_or(jnp.logical_and(turn >= 0, turn < 2), jnp.logical_and(turn >= 2 + GAP, turn < COL + GAP)))
            def _(fn=fn, turn=turn):
                fn(jnp.where(turn >= 2, turn - GAP, turn))


MT = 512
PART_SLOTS = 5
LAND_SLOTS = 4
GAP = 3


def reduce_call(az, x, wo, wd):
    seq, kk = az.shape
    d = x.shape[1]
    cols = d // COL
    half = seq // 2
    big, small = half // TPA, half // TPA // TPA
    bf = jnp.bfloat16
    hbm = pl.BlockSpec(memory_space=pl.ANY)
    vm = pl.BlockSpec(memory_space=pltpu.VMEM)
    res = pl.pallas_call(
        reduce_kernel,
        out_shape=pltpu.VMEM((COL, seq, cols), bf),
        in_specs=[vm, hbm, hbm, hbm],
        out_specs=vm,
        scratch_shapes=[
            pltpu.VMEM((COL, kk, cols), bf),
            pltpu.VMEM((PART_SLOTS, seq, cols), bf),
            pltpu.VMEM((COL, 2, 2, big // 2, cols), bf),
            pltpu.VMEM((LAND_SLOTS, 2, 2, big, cols), bf),
            pltpu.VMEM((COL, 2, 2, small // 2, cols), bf),
            pltpu.VMEM((COL, 2, 2, small, cols), bf),
            pltpu.VMEM((2, small, d), bf),
            pltpu.SemaphoreType.DMA((COL, 2, 2, 8)),
            pltpu.SemaphoreType.DMA((COL, 2, 2, 8)),
            pltpu.SemaphoreType.DMA((8,)),
            pltpu.SemaphoreType.DMA((8,)),
            pltpu.SemaphoreType.DMA((4,)),
        ],
        compiler_params=pltpu.CompilerParams(collective_id=1, has_side_effects=True, vmem_limit_bytes=40 * 1024 * 1024),
        cost_estimate=pl.CostEstimate(flops=2 * seq * kk * d, bytes_accessed=4 * seq * d, transcendentals=0),
        name="down_reduce",
    )(az, x, wo, wd)
    return write_out(res)[None]


def write_kernel(src, dst, sem):
    n, seq, cols = src.shape
    copies = [pltpu.make_async_copy(src.at[b], dst.at[:, pl.ds(b * cols, cols)], sem.at[b]) for b in range(n)]
    for c in copies:
        c.start()
    for c in copies:
        c.wait()


def write_out(blocks):
    n, seq, cols = blocks.shape
    return pl.pallas_call(
        write_kernel,
        out_shape=jax.ShapeDtypeStruct((seq, n * cols), blocks.dtype),
        in_specs=[pl.BlockSpec(memory_space=pltpu.VMEM)],
        out_specs=pl.BlockSpec(memory_space=pl.ANY),
        scratch_shapes=[pltpu.SemaphoreType.DMA((n,))],
        compiler_params=pltpu.CompilerParams(vmem_limit_bytes=24 * 1024 * 1024),
        name="write_out",
    )(blocks)


def solution(mesh):
    row_spec = P(("dp", "fsdp"), None, None)

    def local_layer(hidden, positions, norm_gain, w_query, w_key, w_value, w_gate, w_up, w_out, w_down):
        az = project_call(hidden[0], positions, norm_gain, w_query, w_key, w_value, w_gate, w_up)
        return reduce_call(az, hidden[0], w_out, w_down)

    in_specs = (row_spec, P(None), P("fsdp"), P("fsdp", "tp"), P("fsdp", None), P("fsdp", None), P("fsdp", "tp"), P("fsdp", "tp"), P("tp", "fsdp"), P("tp", "fsdp"))
    return jax.shard_map(local_layer, mesh=mesh, in_specs=in_specs, out_specs=row_spec, check_vma=False)
```

```python
import jax
import jax.numpy as jnp
import numpy as np
from jax import lax
from jax.experimental import pallas as pl
from jax.experimental.pallas import tpu as pltpu
from jax.sharding import PartitionSpec as P

NORM_EPS = 1e-6
MESH = pl.DeviceIdType.MESH
TPA = 4
COL = 8


def _ring_ids(t):
    z, y = t // TPA, t % TPA
    y_r, y_l = z * TPA + (y + 1) % TPA, z * TPA + (y + 3) % TPA
    z_r, z_l = ((z + 1) % TPA) * TPA + y, ((z + 3) % TPA) * TPA + y
    return (y, y_r, y_l), (z, z_r, z_l)


def _fsdp_ids(f):
    xc, core = f // 2, f % 2
    f_p = xc * 2 + (1 - core)
    f_r = ((xc + 1) % 4) * 2 + core
    f_l = ((xc + 3) % 4) * 2 + core
    return xc, core, f_p, f_r, f_l


QB = 256
LN_ROWS = 128
X_SLOTS = 4
LN_SUB = 64
GU = 128
M1 = 1024
PRE_DOWN = 512


def project_kernel(x_hbm, pos, inv_freq, gain, wq, wk, wv, wg, wu, wo, wd, az, pre, wbuf, h, q, k, v, cos_t, sin_t, gbuf, xb, scores, acc,
                   ssem, rsem, gss, grs, lsem, gsem, xsem, kss, krs, pss, prs):
    f = lax.axis_index("fsdp")
    nf = lax.axis_size("fsdp")
    t = lax.axis_index("tp")
    nt = lax.axis_size("tp")
    ring_y, ring_z = _ring_ids(t)
    z_id, y_id = ring_z[0], ring_y[0]
    xc, core, f_p, f_r, f_l = _fsdp_ids(f)
    f_o = ((xc + 2) % 4) * 2 + core
    seq, d = h.shape
    depth = gain.shape[1]
    hd = wq.shape[3]
    n_chunk = wbuf.shape[0]
    n_ff = wg.shape[3] // GU
    n_x = n_ff + 1

    def half_of(i, dev, part):
        return wbuf.at[i, dev, pl.ds(part * (TPA // 2), TPA // 2)]

    def load(i, part, src, col):
        return pltpu.make_async_copy(src.at[:, :, :, pl.ds(col, GU)], wbuf.at[i, f, :, :, :, pl.ds(part * GU, GU)], lsem.at[i, part])

    ld_kv = [pltpu.make_async_copy(w.at[z_id, y_id], wbuf.at[1 + i, f, z_id, y_id], lsem.at[1 + i, 0]) for i, w in enumerate((wk, wv))]
    for c in ld_kv:
        c.start()
    for part in range(2):
        load(0, part, wq, part * GU).start()
    for j in range(n_ff):
        load(3 + j, 0, wg, j * GU).start()
        load(3 + j, 1, wu, j * GU).start()

    def load_x(blk):
        slot = blk % X_SLOTS
        return pltpu.make_async_copy(x_hbm.at[pl.ds(pl.multiple_of(blk * LN_ROWS, LN_ROWS), LN_ROWS), :], xb.at[slot], xsem.at[slot])

    for blk in range(X_SLOTS - 1):
        load_x(blk).start()
    ld_g = pltpu.make_async_copy(gain, gbuf.at[:, pl.ds(pl.multiple_of(f * depth, depth), depth)], gsem)
    ld_g.start()

    barrier = pltpu.get_barrier_semaphore()
    for e in range(1, nf):
        pl.semaphore_signal(barrier, inc=1, device_id={"fsdp": (f + e) % nf}, device_id_type=MESH)
    for other in (ring_y[1], ring_y[2], ring_z[1], ring_z[2]):
        pl.semaphore_signal(barrier, inc=1, device_id={"tp": other}, device_id_type=MESH)
    pl.semaphore_wait(barrier, nf - 1 + 4)

    def rcopy(i, s, src, dev):
        return pltpu.make_async_remote_copy(src_ref=src, dst_ref=src, send_sem=ssem.at[i, s], recv_sem=rsem.at[i, s],
                                            device_id={"fsdp": dev}, device_id_type=MESH)

    def transfer(i, s):
        src, dev = (
            (lambda: wbuf.at[i, f], f_r),
            (lambda: wbuf.at[i, f], f_l),
            (lambda: wbuf.at[i, f], f_p),
            (lambda: half_of(i, f_l, 0), f_r),
            (lambda: half_of(i, f_r, 1), f_l),
            (lambda: wbuf.at[i, f_l], f_p),
            (lambda: wbuf.at[i, f_r], f_p),
            (lambda: wbuf.at[i, f_o], f_p),
        )[s]
        return rcopy(i, s, src(), dev)

    def chunk_of(xi):
        return xi + 2 * ((xi + n_x - 1) // n_x)

    kv_rings = ((ring_y, ring_z), (ring_z, ring_y))

    def kv_unit(i, dev, lo, n):
        z, y = (z_id, dev) if i == 0 else (dev, y_id)
        return wbuf.at[1 + i, pl.ds(lo, n), z, y]

    def kv_line(i, dev, lo, n):
        return wbuf.at[1 + i, pl.ds(lo, n), dev] if i == 0 else wbuf.at[1 + i, pl.ds(lo, n), :, dev]

    def kv_copies(step):
        res = []
        for i in range(2):
            ids = kv_rings[i][step // 2]
            me, r, l = ids
            view = kv_line if step >= 2 else kv_unit
            if step % 2 == 0:
                src = (view(i, me, 0, nf), view(i, me, 0, nf))
            else:
                src = (view(i, (me + TPA - 1) % TPA, 0, nf // 2), view(i, (me + 1) % TPA, nf // 2, nf // 2))
            for d_, (part, dev) in enumerate(zip(src, (r, l))):
                res.append(pltpu.make_async_remote_copy(src_ref=part, dst_ref=part, send_sem=kss.at[nf + step, 2 * i + d_], recv_sem=krs.at[nf + step, 2 * i + d_],
                                                        device_id={"tp": dev}, device_id_type=MESH))
        return res

    def kv_start(step):
        for c in kv_copies(step):
            c.start()

    def kv_finish(step):
        for c in kv_copies(step):
            c.wait_recv()
            c.wait_send()

    n_o = wo.shape[0]
    n_d = pre.shape[1] - n_o

    def pre_copies():
        res = []
        for d_, dev in ((0, f_r), (1, f_l)):
            for e, (src, lo, n) in enumerate(((wo, 0, n_o), (wd, n_o, n_d))):
                res.append(pltpu.make_async_remote_copy(src_ref=src.at[pl.ds(0, n)], dst_ref=pre.at[d_, pl.ds(lo, n)], send_sem=pss.at[d_, e], recv_sem=prs.at[d_, e],
                                                        device_id={"fsdp": dev}, device_id_type=MESH))
        return res

    def send_own(i):
        for part in range(2):
            load(i, part, wq, part * GU).wait()
        for s in range(3):
            transfer(i, s).start()

    def net_a(xi):
        i = chunk_of(xi)
        transfer(i, 0).wait_recv()
        transfer(i, 3).start()
        transfer(i, 1).wait_recv()
        transfer(i, 4).start()

        @pl.when(xi + 2 < n_x)
        def _():
            send_own(chunk_of(xi + 2))

        @pl.when(xi + 1 == n_x)
        def _():
            for c in pre_copies():
                c.start()

        transfer(i, 5).start()
        transfer(i, 6).start()

    def net_b(xi):
        i = chunk_of(xi)
        transfer(i, 3).wait_recv()
        transfer(i, 4).wait_recv()
        transfer(i, 7).start()

    def ready(i):
        for s in (2, 5, 6, 7):
            transfer(i, s).wait_recv()
        for s in range(8):
            transfer(i, s).wait_send()

    ld_g.wait()
    gcol = gbuf.at[:, pl.ds(pl.multiple_of(f * depth, depth), depth)]
    gcopies = [pltpu.make_async_remote_copy(src_ref=gcol, dst_ref=gcol, send_sem=gss.at[e], recv_sem=grs.at[e],
                                            device_id={"fsdp": (f + e) % nf}, device_id_type=MESH) for e in range(1, nf)]
    for c in gcopies:
        c.start()
    kv_x = []
    for i in range(2):
        ld_kv[i].wait()
        for e in range(1, nf):
            part = wbuf.at[1 + i, f, z_id, y_id]
            kv_x.append(pltpu.make_async_remote_copy(src_ref=part, dst_ref=part, send_sem=kss.at[e, i], recv_sem=krs.at[e, i],
                                                     device_id={"fsdp": (f + e) % nf}, device_id_type=MESH))
    for c in kv_x:
        c.start()
    send_own(0)
    send_own(3)

    lanes = pos.shape[1]
    eye = lax.broadcasted_iota(jnp.int32, (lanes, lanes), 0) == lax.broadcasted_iota(jnp.int32, (lanes, lanes), 1)

    @pl.loop(0, seq // lanes)
    def _(b):
        rows = pl.ds(pl.multiple_of(b * lanes, lanes), lanes)
        line = pos[pl.ds(b, 1), :].astype(jnp.float32)
        column = jnp.sum(jnp.where(eye, line, 0.0), axis=-1, keepdims=True)
        angle = column * inv_freq[...]
        cos_t[rows, :] = jnp.cos(angle)
        sin_t[rows, :] = jnp.sin(angle)

    for c in gcopies:
        c.wait()
    for c in kv_x:
        c.wait()
    kv_start(0)

    n_blk = seq // LN_ROWS

    def norm_blocks(lo, hi):
        @pl.loop(lo, hi)
        def _(blk):
            load_x(blk).wait()

            @pl.when(blk + X_SLOTS - 1 < n_blk)
            def _():
                load_x(blk + X_SLOTS - 1).start()

            @pl.loop(0, LN_ROWS // LN_SUB)
            def _(r):
                row = xb[blk % X_SLOTS, pl.ds(pl.multiple_of(r * LN_SUB, LN_SUB), LN_SUB), :].astype(jnp.float32)
                centered = row - jnp.sum(row, axis=-1, keepdims=True) * (1.0 / d)
                var = jnp.sum(centered * centered, axis=-1, keepdims=True) * (1.0 / d)
                out = centered * lax.rsqrt(var + NORM_EPS) * gbuf[...]
                h[pl.ds(pl.multiple_of(blk * LN_ROWS + r * LN_SUB, LN_SUB), LN_SUB), :] = out.astype(jnp.bfloat16)

    norm_blocks(0, n_blk // 2)
    net_a(0)
    kv_finish(0)
    kv_start(1)
    norm_blocks(n_blk // 2, n_blk)
    kv_finish(1)
    kv_start(2)

    def rope(rows):
        y = acc[...].astype(jnp.bfloat16).astype(jnp.float32)
        a, b = y[:, :hd // 2], y[:, hd // 2:]
        c, s = cos_t[rows, :], sin_t[rows, :]
        return jnp.concatenate([a * c - b * s, b * c + a * s], axis=1).astype(jnp.bfloat16)

    def compute(i):
        @pl.loop(0, seq // M1)
        def _(m):
            rows = pl.ds(pl.multiple_of(m * M1, M1), M1)
            acc[...] = jnp.dot(h[rows, :], wbuf[i].reshape(d, hd), preferred_element_type=jnp.float32)

            @pl.when(i == 0)
            def _():
                q[rows, :] = rope(rows)

            @pl.when(i == 1)
            def _():
                k[rows, :] = rope(rows)

            @pl.when(i == 2)
            def _():
                v[rows, :] = acc[...].astype(jnp.bfloat16)

            @pl.when(i >= 3)
            def _():
                g = acc[:, :GU].astype(jnp.bfloat16).astype(jnp.float32)
                u = acc[:, GU:].astype(jnp.bfloat16).astype(jnp.float32)
                z = (g * (1.0 / (1.0 + jnp.exp(-g)))) * u
                az[rows, pl.ds(pl.multiple_of(hd + (i - 3) * GU, GU), GU)] = z.astype(jnp.bfloat16)

    scale = hd ** -0.5
    n_q = seq // QB

    def attend(b):
        rows = pl.ds(b * QB, QB)
        qb = q[rows, :]
        peak = None
        for t in range(b + 1):
            s = lax.dot_general(qb, k[pl.ds(t * QB, QB), :], (((1,), (1,)), ((), ())), preferred_element_type=jnp.float32) * scale
            if t == b:
                keep = lax.broadcasted_iota(jnp.int32, (QB, QB), 1) <= lax.broadcasted_iota(jnp.int32, (QB, QB), 0)
                s = jnp.where(keep, s, -1e30)
            scores[:, t * QB:(t + 1) * QB] = s
            s = jnp.maximum(s[:, :128], s[:, 128:])
            peak = s if peak is None else jnp.maximum(peak, s)
        peak = jnp.max(peak, axis=-1, keepdims=True)
        total = None
        for t in range(b + 1):
            e = jnp.exp(scores[:, t * QB:(t + 1) * QB] - peak)
            scores[:, t * QB:(t + 1) * QB] = e
            e = e[:, :128] + e[:, 128:]
            total = e if total is None else total + e
        inv = 1.0 / jnp.sum(total, axis=-1, keepdims=True)
        p = (scores[:, :(b + 1) * QB] * inv).astype(jnp.bfloat16)
        out = jnp.dot(p, v[pl.ds(0, (b + 1) * QB), :], preferred_element_type=jnp.float32)
        az[rows, 0:hd] = out.astype(jnp.bfloat16)

    n_first = 3

    @pl.loop(0, n_chunk)
    def _(j):
        on_k, on_v = j == n_first + 1, j == n_first + 3
        xi = j - (j + n_chunk - n_first - 1) // n_chunk - (j + n_chunk - n_first - 3) // n_chunk
        on_x = jnp.logical_not(jnp.logical_or(on_k, on_v))

        @pl.when(on_x)
        def _():
            @pl.when(xi + 1 < n_x)
            def _():
                net_a(xi + 1)

            net_b(xi)

        @pl.when(j == 2)
        def _():
            kv_finish(2)
            kv_start(3)

        @pl.when(on_k)
        def _():
            kv_finish(3)

        for lo, hi, step in ((0, 4, n_first + 4), (4, 6, n_first + 5), (6, 8, n_first + 6)):
            @pl.when(j == step)
            def _(lo=lo, hi=hi):
                for b in range(lo, hi):
                    attend(b)

        @pl.when(on_x)
        def _():
            ready(chunk_of(xi))

        compute(jnp.where(on_k, 1, jnp.where(on_v, 2, chunk_of(xi))))

    for c in pre_copies():
        c.wait()


def project_call(x, positions, norm_gain, w_query, w_key, w_value, w_gate, w_up, w_out, w_down):
    seq, d = x.shape
    depth, hd = w_query.shape
    ff = w_gate.shape[1]
    n_chunk = 3 + ff // GU
    inv_freq = jnp.asarray((10000.0 ** (-np.arange(0, hd, 2) / hd)).astype(np.float32))
    bf, f32 = jnp.bfloat16, jnp.float32
    hbm = pl.BlockSpec(memory_space=pl.ANY)
    vm = pl.BlockSpec(memory_space=pltpu.VMEM)
    flops = 2 * seq * d * (3 * hd + 2 * ff) + 2 * seq * seq * hd
    return pl.pallas_call(
        project_kernel,
        out_shape=(jax.ShapeDtypeStruct((seq, hd + ff), bf), jax.ShapeDtypeStruct((2, hd + PRE_DOWN, w_out.shape[1]), bf)),
        in_specs=[hbm, vm, vm] + [hbm] * 8,
        out_specs=(vm, hbm),
        scratch_shapes=[
            pltpu.VMEM((n_chunk, d // depth, TPA, TPA, depth // TPA // TPA, hd), bf),
            pltpu.VMEM((seq, d), bf),
            pltpu.VMEM((seq, hd), bf),
            pltpu.VMEM((seq, hd), bf),
            pltpu.VMEM((seq, hd), bf),
            pltpu.VMEM((seq, hd // 2), f32),
            pltpu.VMEM((seq, hd // 2), f32),
            pltpu.VMEM((1, d), f32),
            pltpu.VMEM((X_SLOTS, LN_ROWS, d), bf),
            pltpu.VMEM((QB, seq), f32),
            pltpu.VMEM((M1, hd), f32),
            pltpu.SemaphoreType.DMA((n_chunk, 8)),
            pltpu.SemaphoreType.DMA((n_chunk, 8)),
            pltpu.SemaphoreType.DMA((8,)),
            pltpu.SemaphoreType.DMA((8,)),
            pltpu.SemaphoreType.DMA((n_chunk, 2)),
            pltpu.SemaphoreType.DMA,
            pltpu.SemaphoreType.DMA((X_SLOTS,)),
            pltpu.SemaphoreType.DMA((12, 4)),
            pltpu.SemaphoreType.DMA((12, 4)),
            pltpu.SemaphoreType.DMA((2, 2)),
            pltpu.SemaphoreType.DMA((2, 2)),
        ],
        compiler_params=pltpu.CompilerParams(collective_id=0, has_side_effects=True, vmem_limit_bytes=63 * 1024 * 1024),
        cost_estimate=pl.CostEstimate(flops=flops, bytes_accessed=2 * seq * d, transcendentals=0),
        name="gather_project",
    )(x, positions.reshape(seq // 128, 128), inv_freq.reshape(1, hd // 2), norm_gain.reshape(1, depth),
      *(w.reshape(TPA, TPA, depth // TPA // TPA, w.shape[1]) for w in (w_query, w_key, w_value, w_gate, w_up)), w_out, w_down)


def reduce_kernel(az, pre, x_hbm, wo, wd, out, wbuf, part, r1, r2, r3, r4, xbuf,
                  ssem, rsem, wss, wrs, lsem):
    t = lax.axis_index("tp")
    f = lax.axis_index("fsdp")
    ring_y, ring_z = _ring_ids(t)
    xc, core, f_p, f_r, f_l = _fsdp_ids(f)
    seq = az.shape[0]
    cols = wbuf.shape[2]
    half = seq // 2
    big = half // TPA
    small = big // TPA
    hd = wo.shape[0]

    ld_o = pltpu.make_async_copy(wo, wbuf.at[0, pl.ds(0, hd)], lsem.at[0])
    ld_d = pltpu.make_async_copy(wd, wbuf.at[0, pl.ds(hd, wd.shape[0])], lsem.at[1])
    n_pre = pre.shape[1]
    n_rest = wbuf.shape[1] - n_pre
    ld_pre = [pltpu.make_async_copy(pre.at[e], wbuf.at[2 + 2 * e, pl.ds(0, n_pre)], lsem.at[4 + e]) for e in range(2)]
    ld_o.start()
    ld_d.start()
    for c in ld_pre:
        c.start()
    axes = ((ring_y, ring_z), (ring_z, ring_y))

    def own_rows(h):
        (i1, _, _), (i2, _, _) = axes[h]
        return pl.multiple_of(h * half + i1 * big + i2 * small, small)

    ld_x = [pltpu.make_async_copy(x_hbm.at[pl.ds(own_rows(h), small), :], xbuf.at[h], lsem.at[2 + h]) for h in range(2)]
    for c in ld_x:
        c.start()

    barrier = pltpu.get_barrier_semaphore()
    for other in (ring_y[1], ring_y[2], ring_z[1], ring_z[2]):
        pl.semaphore_signal(barrier, inc=1, device_id={"tp": other}, device_id_type=MESH)
    for other in (f_p, f_r, f_l):
        pl.semaphore_signal(barrier, inc=1, device_id={"fsdp": other}, device_id_type=MESH)
    pl.semaphore_wait(barrier, 7)

    def wcopy(k, src, dst, dev):
        return pltpu.make_async_remote_copy(src_ref=src, dst_ref=dst, send_sem=wss.at[k], recv_sem=wrs.at[k],
                                            device_id={"fsdp": dev}, device_id_type=MESH)

    kk = wbuf.shape[1]
    kh = kk // 2
    top, bot = pl.ds(0, kh), pl.ds(kh, kh)
    w_own_p = wcopy(0, wbuf.at[0], wbuf.at[1], f_p)
    rest = pl.ds(n_pre, n_rest)
    w_own_r = wcopy(1, wbuf.at[0, rest], wbuf.at[2, rest], f_r)
    w_own_l = wcopy(2, wbuf.at[0, rest], wbuf.at[4, rest], f_l)
    w_2p = wcopy(3, wbuf.at[2], wbuf.at[3], f_p)
    w_4p = wcopy(4, wbuf.at[4], wbuf.at[5], f_p)
    w_2r = wcopy(5, wbuf.at[2, top], wbuf.at[6, top], f_r)
    w_4l = wcopy(6, wbuf.at[4, bot], wbuf.at[6, bot], f_l)
    w_6p = wcopy(7, wbuf.at[6], wbuf.at[7], f_p)
    ld_o.wait()
    ld_d.wait()
    w_own_r.start()
    w_own_l.start()
    w_own_p.start()
    for c in ld_x + ld_pre:
        c.wait()

    def block_of(k):
        q = k // 2
        dx = 3 * q - 5 * (q // 2) - 2 * (q // 3)
        return ((xc + dx) % 4) * 2 + (core + k % 2) % 2

    def ring_copy(cb, h, d, step, src, dst, dev):
        return pltpu.make_async_remote_copy(src_ref=src, dst_ref=dst, send_sem=ssem.at[cb, h, d, step],
                                            recv_sem=rsem.at[cb, h, d, step], device_id={"tp": dev}, device_id_type=MESH)

    def rs_first(cb, h, step, ring, base, n, land):
        i, r, l = ring
        o = (i + 2) % TPA
        m = n // 2
        s = pl.multiple_of(base + o * n, m)
        return (ring_copy(cb, h, 0, step, part.at[cb % PART_SLOTS, pl.ds(s, m)], land.at[cb % land.shape[0], h, 0], r),
                ring_copy(cb, h, 1, step, part.at[cb % PART_SLOTS, pl.ds(s + m, m)], land.at[cb % land.shape[0], h, 1], l))

    def rs_second(cb, h, step, ring, base, n, land):
        i, r, l = ring
        s_r = pl.multiple_of(base + ((i + 1) % TPA) * n, n)
        s_l = pl.multiple_of(base + ((i + 3) % TPA) * n, n)
        return (ring_copy(cb, h, 0, step, part.at[cb % PART_SLOTS, pl.ds(s_r, n)], land.at[cb % land.shape[0], h, 0], r),
                ring_copy(cb, h, 1, step, part.at[cb % PART_SLOTS, pl.ds(s_l, n)], land.at[cb % land.shape[0], h, 1], l))

    def rs_update(cb, h, ring, base, n, land):
        i, _, _ = ring
        m = n // 2
        s_r = pl.multiple_of(base + ((i + 1) % TPA) * n, m)
        s_l = pl.multiple_of(base + ((i + 3) % TPA) * n + m, m)
        for s, d in ((s_r, 0), (s_l, 1)):
            rows = pl.ds(s, m)
            part[cb % PART_SLOTS, rows] = (part[cb % PART_SLOTS, rows].astype(jnp.float32) + land[cb % land.shape[0], h, d].astype(jnp.float32)).astype(jnp.bfloat16)

    def ag_first(cb, h, step, ring, src, base, n):
        i, r, l = ring
        g = block_of(cb)
        dst = out.at[g, pl.ds(pl.multiple_of(base + i * n, n), n)]
        if src is None:
            src = dst
        return (ring_copy(cb, h, 0, step, src, dst, r), ring_copy(cb, h, 1, step, src, dst, l))

    def ag_second(cb, h, step, ring, base, n):
        i, r, l = ring
        g = block_of(cb)
        m = n // 2
        from_l = out.at[g, pl.ds(pl.multiple_of(base + ((i + 3) % TPA) * n, m), m)]
        from_r = out.at[g, pl.ds(pl.multiple_of(base + ((i + 1) % TPA) * n + m, m), m)]
        return (ring_copy(cb, h, 0, step, from_l, from_l, r), ring_copy(cb, h, 1, step, from_r, from_r, l))

    def copies(cb, step):
        res = []
        for h in range(2):
            ring1, ring2 = axes[h]
            base1 = h * half
            base2 = pl.multiple_of(h * half + ring1[0] * big, big)
            if step == 0:
                res.extend(rs_first(cb, h, step, ring1, base1, big, r1))
            elif step == 1:
                res.extend(rs_second(cb, h, step, ring1, base1, big, r2))
            elif step == 2:
                res.extend(rs_first(cb, h, step, ring2, base2, small, r3))
            elif step == 3:
                res.extend(rs_second(cb, h, step, ring2, base2, small, r4))
            elif step == 4:
                res.extend(ag_first(cb, h, step, ring2, None, base2, small))
            elif step == 5:
                res.extend(ag_second(cb, h, step, ring2, base2, small))
            elif step == 6:
                res.extend(ag_first(cb, h, step, ring1, None, base1, big))
            else:
                res.extend(ag_second(cb, h, step, ring1, base1, big))
        return res

    def start(cb, step):
        for c in copies(cb, step):
            c.start()

    def finish(cb, step):
        for c in copies(cb, step):
            c.wait_recv()
            c.wait_send()

    def stage0(cb):
        @pl.when(cb == 1)
        def _():
            w_own_p.wait()

        @pl.when(cb == 2)
        def _():
            w_own_r.wait()
            w_own_l.wait()
            w_2r.start()
            w_4l.start()
            w_2p.start()
            w_4p.start()

        @pl.when(cb == 3)
        def _():
            w_2p.wait()

        @pl.when(cb == 5)
        def _():
            w_4p.wait()

        @pl.when(cb == 6)
        def _():
            w_2r.wait()
            w_4l.wait()
            w_6p.start()

        @pl.when(cb == 7)
        def _():
            w_6p.wait()

        @pl.loop(0, seq // MT)
        def _(i):
            rows = pl.ds(pl.multiple_of(i * MT, MT), MT)
            part[cb % PART_SLOTS, rows] = jnp.dot(az[rows, :], wbuf[cb], preferred_element_type=jnp.float32).astype(jnp.bfloat16)

        start(cb, 0)

    def stage1(cb):
        finish(cb, 0)
        for h in range(2):
            rs_update(cb, h, axes[h][0], h * half, big, r1)
        start(cb, 1)

    def stage2(cb):
        finish(cb, 1)
        for h in range(2):
            rows = pl.ds(pl.multiple_of(h * half + axes[h][0][0] * big, big), big)
            part[cb % PART_SLOTS, rows] = (part[cb % PART_SLOTS, rows].astype(jnp.float32) + r2[cb % r2.shape[0], h, 0].astype(jnp.float32)
                              + r2[cb % r2.shape[0], h, 1].astype(jnp.float32)).astype(jnp.bfloat16)
        start(cb, 2)

    def stage3(cb):
        finish(cb, 2)
        for h in range(2):
            rs_update(cb, h, axes[h][1], pl.multiple_of(h * half + axes[h][0][0] * big, big), small, r3)
        start(cb, 3)

    def stage4(cb):
        finish(cb, 3)
        g = block_of(cb)
        for h in range(2):
            branch = (part[cb % PART_SLOTS, pl.ds(own_rows(h), small)].astype(jnp.float32) + r4[cb % r4.shape[0], h, 0].astype(jnp.float32)
                      + r4[cb % r4.shape[0], h, 1].astype(jnp.float32))
            xs = xbuf[h, :, pl.ds(pl.multiple_of(g * cols, cols), cols)].astype(jnp.float32)
            out[g, pl.ds(own_rows(h), small), :] = (xs + branch).astype(jnp.bfloat16)
        start(cb, 4)

    def stage5(cb):
        finish(cb, 4)
        start(cb, 5)

    def stage6(cb):
        finish(cb, 5)
        start(cb, 6)

    def stage7(cb):
        finish(cb, 6)
        start(cb, 7)

    def stage8(cb):
        finish(cb, 7)

    stages = (stage0, stage1, stage2, stage3, stage4, stage5, stage6, stage7, stage8)

    @pl.loop(0, COL + GAP + len(stages) - 1)
    def _(n):
        for s, fn in enumerate(stages):
            turn = n - s

            @pl.when(jnp.logical_or(jnp.logical_and(turn >= 0, turn < 2), jnp.logical_and(turn >= 2 + GAP, turn < COL + GAP)))
            def _(fn=fn, turn=turn):
                fn(jnp.where(turn >= 2, turn - GAP, turn))


MT = 512
PART_SLOTS = 5
LAND_SLOTS = 4
GAP = 1


def reduce_call(az, pre, x, wo, wd):
    seq, kk = az.shape
    d = x.shape[1]
    cols = d // COL
    half = seq // 2
    big, small = half // TPA, half // TPA // TPA
    bf = jnp.bfloat16
    hbm = pl.BlockSpec(memory_space=pl.ANY)
    vm = pl.BlockSpec(memory_space=pltpu.VMEM)
    res = pl.pallas_call(
        reduce_kernel,
        out_shape=pltpu.VMEM((COL, seq, cols), bf),
        in_specs=[vm, hbm, hbm, hbm, hbm],
        out_specs=vm,
        scratch_shapes=[
            pltpu.VMEM((COL, kk, cols), bf),
            pltpu.VMEM((PART_SLOTS, seq, cols), bf),
            pltpu.VMEM((COL, 2, 2, big // 2, cols), bf),
            pltpu.VMEM((LAND_SLOTS, 2, 2, big, cols), bf),
            pltpu.VMEM((COL, 2, 2, small // 2, cols), bf),
            pltpu.VMEM((COL, 2, 2, small, cols), bf),
            pltpu.VMEM((2, small, d), bf),
            pltpu.SemaphoreType.DMA((COL, 2, 2, 8)),
            pltpu.SemaphoreType.DMA((COL, 2, 2, 8)),
            pltpu.SemaphoreType.DMA((8,)),
            pltpu.SemaphoreType.DMA((8,)),
            pltpu.SemaphoreType.DMA((6,)),
        ],
        compiler_params=pltpu.CompilerParams(collective_id=1, has_side_effects=True, vmem_limit_bytes=40 * 1024 * 1024),
        cost_estimate=pl.CostEstimate(flops=2 * seq * kk * d, bytes_accessed=4 * seq * d, transcendentals=0),
        name="down_reduce",
    )(az, pre, x, wo, wd)
    return write_out(res)[None]


def write_kernel(src, dst, sem):
    n, seq, cols = src.shape
    copies = [pltpu.make_async_copy(src.at[b], dst.at[:, pl.ds(b * cols, cols)], sem.at[b]) for b in range(n)]
    for c in copies:
        c.start()
    for c in copies:
        c.wait()


def write_out(blocks):
    n, seq, cols = blocks.shape
    return pl.pallas_call(
        write_kernel,
        out_shape=jax.ShapeDtypeStruct((seq, n * cols), blocks.dtype),
        in_specs=[pl.BlockSpec(memory_space=pltpu.VMEM)],
        out_specs=pl.BlockSpec(memory_space=pl.ANY),
        scratch_shapes=[pltpu.SemaphoreType.DMA((n,))],
        compiler_params=pltpu.CompilerParams(vmem_limit_bytes=24 * 1024 * 1024),
        name="write_out",
    )(blocks)


def solution(mesh):
    row_spec = P(("dp", "fsdp"), None, None)

    def local_layer(hidden, positions, norm_gain, w_query, w_key, w_value, w_gate, w_up, w_out, w_down):
        az, pre = project_call(hidden[0], positions, norm_gain, w_query, w_key, w_value, w_gate, w_up, w_out, w_down)
        return reduce_call(az, pre, hidden[0], w_out, w_down)

    in_specs = (row_spec, P(None), P("fsdp"), P("fsdp", "tp"), P("fsdp", None), P("fsdp", None), P("fsdp", "tp"), P("fsdp", "tp"), P("tp", "fsdp"), P("tp", "fsdp"))
    return jax.shard_map(local_layer, mesh=mesh, in_specs=in_specs, out_specs=row_spec, check_vma=False)
```

```python
import jax
import jax.numpy as jnp
import numpy as np
from jax import lax
from jax.experimental import pallas as pl
from jax.experimental.pallas import tpu as pltpu
from jax.sharding import PartitionSpec as P

NORM_EPS = 1e-6
MESH = pl.DeviceIdType.MESH
TPA = 4
COL = 8


def _ring_ids(t):
    z, y = t // TPA, t % TPA
    y_r, y_l = z * TPA + (y + 1) % TPA, z * TPA + (y + 3) % TPA
    z_r, z_l = ((z + 1) % TPA) * TPA + y, ((z + 3) % TPA) * TPA + y
    return (y, y_r, y_l), (z, z_r, z_l)


def _fsdp_ids(f):
    xc, core = f // 2, f % 2
    f_p = xc * 2 + (1 - core)
    f_r = ((xc + 1) % 4) * 2 + core
    f_l = ((xc + 3) % 4) * 2 + core
    return xc, core, f_p, f_r, f_l


QB = 256
LN_ROWS = 128
X_SLOTS = 4
LN_SUB = 64
GU = 128
M1 = 1024
M2 = 512
PRE_DOWN = 256


def project_kernel(x_hbm, pos, inv_freq, gain, wq, wk, wv, wg, wu, wo, wd, az, pre, wbuf, h, q, kv, cos_t, sin_t, gbuf, xb, scores,
                   ssem, rsem, gss, grs, lsem, gsem, xsem, kss, krs, pss, prs):
    f = lax.axis_index("fsdp")
    nf = lax.axis_size("fsdp")
    t = lax.axis_index("tp")
    nt = lax.axis_size("tp")
    ring_y, ring_z = _ring_ids(t)
    z_id, y_id = ring_z[0], ring_y[0]
    xc, core, f_p, f_r, f_l = _fsdp_ids(f)
    f_o = ((xc + 2) % 4) * 2 + core
    seq, d = h.shape
    depth = gain.shape[1]
    hd = wq.shape[3]
    n_chunk = wbuf.shape[0]
    n_ff = wg.shape[3] // GU
    n_x = n_ff + 1

    def half_of(i, dev, part):
        return wbuf.at[i, dev, pl.ds(part * (TPA // 2), TPA // 2)]

    def load(i, part, src, col):
        return pltpu.make_async_copy(src.at[:, :, :, pl.ds(col, GU)], wbuf.at[i, f, :, :, :, pl.ds(part * GU, GU)], lsem.at[i, part])

    ld_kv = [pltpu.make_async_copy(w.at[z_id, y_id], wbuf.at[1 + i, f, z_id, y_id], lsem.at[1 + i, 0]) for i, w in enumerate((wk, wv))]
    for c in ld_kv:
        c.start()
    for part in range(2):
        load(0, part, wq, part * GU).start()
    for j in range(n_ff):
        load(3 + j, 0, wg, j * GU).start()
        load(3 + j, 1, wu, j * GU).start()

    def load_x(blk):
        slot = blk % X_SLOTS
        return pltpu.make_async_copy(x_hbm.at[pl.ds(pl.multiple_of(blk * LN_ROWS, LN_ROWS), LN_ROWS), :], xb.at[slot], xsem.at[slot])

    for blk in range(X_SLOTS - 1):
        load_x(blk).start()
    ld_g = pltpu.make_async_copy(gain, gbuf.at[:, pl.ds(pl.multiple_of(f * depth, depth), depth)], gsem)
    ld_g.start()

    barrier = pltpu.get_barrier_semaphore()
    for e in range(1, nf):
        pl.semaphore_signal(barrier, inc=1, device_id={"fsdp": (f + e) % nf}, device_id_type=MESH)
    for other in (ring_y[1], ring_y[2], ring_z[1], ring_z[2]):
        pl.semaphore_signal(barrier, inc=1, device_id={"tp": other}, device_id_type=MESH)
    pl.semaphore_wait(barrier, nf - 1 + 4)

    def rcopy(i, s, src, dev):
        return pltpu.make_async_remote_copy(src_ref=src, dst_ref=src, send_sem=ssem.at[i, s], recv_sem=rsem.at[i, s],
                                            device_id={"fsdp": dev}, device_id_type=MESH)

    def transfer(i, s):
        src, dev = (
            (lambda: wbuf.at[i, f], f_r),
            (lambda: wbuf.at[i, f], f_l),
            (lambda: wbuf.at[i, f], f_p),
            (lambda: half_of(i, f_l, 0), f_r),
            (lambda: half_of(i, f_r, 1), f_l),
            (lambda: wbuf.at[i, f_l], f_p),
            (lambda: wbuf.at[i, f_r], f_p),
            (lambda: wbuf.at[i, f_o], f_p),
        )[s]
        return rcopy(i, s, src(), dev)

    def chunk_of(xi):
        return xi + 2 * ((xi + n_x - 1) // n_x)

    kv_rings = ((ring_y, ring_z), (ring_z, ring_y))

    def ids_of(i, dev):
        return (z_id, dev) if i == 0 else (dev, y_id)

    def w_view(i, line, dev, part):
        lo, n = ((0, nf), (0, nf // 2), (nf // 2, nf // 2))[part]
        if not line:
            z, y = ids_of(i, dev)
            return wbuf.at[1 + i, pl.ds(lo, n), z, y]
        return wbuf.at[1 + i, pl.ds(lo, n), dev] if i == 0 else wbuf.at[1 + i, pl.ds(lo, n), :, dev]

    def o_view(i, line, dev, part):
        size = TPA if line else kv.shape[3]
        lo, n = ((0, size), (0, size // 2), (size // 2, size // 2))[part]
        if not line:
            z, y = ids_of(i, dev)
            return kv.at[i, z, y, pl.ds(lo, n)]
        return kv.at[i, dev, pl.ds(lo, n)] if i == 0 else kv.at[i, pl.ds(lo, n), dev]

    def kv_copies(step):
        res = []
        view = w_view if step < 4 else o_view
        for i in range(2):
            me, r, l = kv_rings[i][step // 2 % 2]
            line = step // 2 % 2 == 1
            if step % 2 == 0:
                src = (view(i, line, me, 0), view(i, line, me, 0))
            else:
                src = (view(i, line, (me + TPA - 1) % TPA, 1), view(i, line, (me + 1) % TPA, 2))
            for d_, (part, dev) in enumerate(zip(src, (r, l))):
                res.append(pltpu.make_async_remote_copy(src_ref=part, dst_ref=part, send_sem=kss.at[nf + step, 2 * i + d_], recv_sem=krs.at[nf + step, 2 * i + d_],
                                                        device_id={"tp": dev}, device_id_type=MESH))
        return res

    def kv_start(step):
        for c in kv_copies(step):
            c.start()

    def kv_finish(step):
        for c in kv_copies(step):
            c.wait_recv()
            c.wait_send()

    n_o = wo.shape[0]
    n_d = pre.shape[1] - n_o

    def pre_copies():
        res = []
        for d_, dev in ((0, f_r), (1, f_l)):
            for e, (src, lo, n) in enumerate(((wo, 0, n_o), (wd, n_o, n_d))):
                res.append(pltpu.make_async_remote_copy(src_ref=src.at[pl.ds(0, n)], dst_ref=pre.at[d_, pl.ds(lo, n)], send_sem=pss.at[d_, e], recv_sem=prs.at[d_, e],
                                                        device_id={"fsdp": dev}, device_id_type=MESH))
        return res

    def send_own(i):
        for part in range(2):
            load(i, part, wq, part * GU).wait()
        for s in range(3):
            transfer(i, s).start()

    def net_a(xi):
        i = chunk_of(xi)
        transfer(i, 0).wait_recv()
        transfer(i, 3).start()
        transfer(i, 1).wait_recv()
        transfer(i, 4).start()

        @pl.when(xi + 2 < n_x)
        def _():
            send_own(chunk_of(xi + 2))

        @pl.when(xi + 1 == n_x)
        def _():
            for c in pre_copies():
                c.start()

        transfer(i, 5).start()
        transfer(i, 6).start()

    def net_b(xi):
        i = chunk_of(xi)
        transfer(i, 3).wait_recv()
        transfer(i, 4).wait_recv()
        transfer(i, 7).start()

    def ready(i):
        for s in (2, 5, 6, 7):
            transfer(i, s).wait_recv()
        for s in range(8):
            transfer(i, s).wait_send()

    ld_g.wait()
    gcol = gbuf.at[:, pl.ds(pl.multiple_of(f * depth, depth), depth)]
    gcopies = [pltpu.make_async_remote_copy(src_ref=gcol, dst_ref=gcol, send_sem=gss.at[e], recv_sem=grs.at[e],
                                            device_id={"fsdp": (f + e) % nf}, device_id_type=MESH) for e in range(1, nf)]
    for c in gcopies:
        c.start()
    kv_x = []
    for i in range(2):
        ld_kv[i].wait()
        for e in range(1, nf):
            part = wbuf.at[1 + i, f, z_id, y_id]
            kv_x.append(pltpu.make_async_remote_copy(src_ref=part, dst_ref=part, send_sem=kss.at[e, i], recv_sem=krs.at[e, i],
                                                     device_id={"fsdp": (f + e) % nf}, device_id_type=MESH))
    for c in kv_x:
        c.start()
    send_own(0)
    send_own(3)

    lanes = pos.shape[1]
    eye = lax.broadcasted_iota(jnp.int32, (lanes, lanes), 0) == lax.broadcasted_iota(jnp.int32, (lanes, lanes), 1)

    @pl.loop(0, seq // lanes)
    def _(b):
        rows = pl.ds(pl.multiple_of(b * lanes, lanes), lanes)
        line = pos[pl.ds(b, 1), :].astype(jnp.float32)
        column = jnp.sum(jnp.where(eye, line, 0.0), axis=-1, keepdims=True)
        angle = column * inv_freq[...]
        cos_t[rows, :] = jnp.cos(angle)
        sin_t[rows, :] = jnp.sin(angle)

    for c in gcopies:
        c.wait()
    for c in kv_x:
        c.wait()
    kv_start(0)

    n_blk = seq // LN_ROWS

    def norm_blocks(lo, hi):
        @pl.loop(lo, hi)
        def _(blk):
            load_x(blk).wait()

            @pl.when(blk + X_SLOTS - 1 < n_blk)
            def _():
                load_x(blk + X_SLOTS - 1).start()

            @pl.loop(0, LN_ROWS // LN_SUB)
            def _(r):
                row = xb[blk % X_SLOTS, pl.ds(pl.multiple_of(r * LN_SUB, LN_SUB), LN_SUB), :].astype(jnp.float32)
                centered = row - jnp.sum(row, axis=-1, keepdims=True) * (1.0 / d)
                var = jnp.sum(centered * centered, axis=-1, keepdims=True) * (1.0 / d)
                out = centered * lax.rsqrt(var + NORM_EPS) * gbuf[...]
                h[pl.ds(pl.multiple_of(blk * LN_ROWS + r * LN_SUB, LN_SUB), LN_SUB), :] = out.astype(jnp.bfloat16)

    norm_blocks(0, n_blk // 4)
    kv_finish(0)
    kv_start(1)
    norm_blocks(n_blk // 4, n_blk // 2)
    net_a(0)
    kv_finish(1)
    kv_start(2)
    norm_blocks(n_blk // 2, n_blk)

    def product(i, rows):
        return jnp.dot(h[rows, :], wbuf[i].reshape(d, hd), preferred_element_type=jnp.float32)

    def rope(y, rows):
        a, b = y[:, :hd // 2].astype(jnp.bfloat16).astype(jnp.float32), y[:, hd // 2:].astype(jnp.bfloat16).astype(jnp.float32)
        c, s = cos_t[rows, :], sin_t[rows, :]
        return jnp.concatenate([a * c - b * s, b * c + a * s], axis=1).astype(jnp.bfloat16)

    def keys_values():
        n = kv.shape[3]
        rows = pl.ds(pl.multiple_of(t * n, n), n)
        kv[0, z_id, y_id] = rope(product(1, rows), rows)
        kv[1, z_id, y_id] = product(2, rows).astype(jnp.bfloat16)

    def compute(i):
        @pl.when(i == 0)
        def _():
            @pl.loop(0, seq // M1)
            def _(m):
                rows = pl.ds(pl.multiple_of(m * M1, M1), M1)
                q[rows, :] = rope(product(i, rows), rows)

        @pl.when(i >= 3)
        def _():
            for m in range(seq // M2):
                rows = pl.ds(m * M2, M2)
                y = product(i, rows)
                g = y[:, :GU].astype(jnp.bfloat16).astype(jnp.float32)
                u = y[:, GU:].astype(jnp.bfloat16).astype(jnp.float32)
                z = (g * (1.0 / (1.0 + jnp.exp(-g)))) * u
                az[rows, pl.ds(pl.multiple_of(hd + (i - 3) * GU, GU), GU)] = z.astype(jnp.bfloat16)

    scale = hd ** -0.5
    n_q = seq // QB

    keys, values = (kv.at[i].reshape(seq, hd) for i in range(2))

    def attend(b):
        rows = pl.ds(b * QB, QB)
        qb = q[rows, :]
        peak = None
        for t in range(b + 1):
            s = lax.dot_general(qb, keys[pl.ds(t * QB, QB), :], (((1,), (1,)), ((), ())), preferred_element_type=jnp.float32) * scale
            if t == b:
                keep = lax.broadcasted_iota(jnp.int32, (QB, QB), 1) <= lax.broadcasted_iota(jnp.int32, (QB, QB), 0)
                s = jnp.where(keep, s, -1e30)
            scores[:, t * QB:(t + 1) * QB] = s
            s = jnp.maximum(s[:, :128], s[:, 128:])
            peak = s if peak is None else jnp.maximum(peak, s)
        peak = jnp.max(peak, axis=-1, keepdims=True)
        total = None
        for t in range(b + 1):
            e = jnp.exp(scores[:, t * QB:(t + 1) * QB] - peak)
            scores[:, t * QB:(t + 1) * QB] = e
            e = e[:, :128] + e[:, 128:]
            total = e if total is None else total + e
        inv = 1.0 / jnp.sum(total, axis=-1, keepdims=True)
        p = (scores[:, :(b + 1) * QB] * inv).astype(jnp.bfloat16)
        out = jnp.dot(p, values[pl.ds(0, (b + 1) * QB), :], preferred_element_type=jnp.float32)
        az[rows, 0:hd] = out.astype(jnp.bfloat16)

    @pl.loop(0, n_x)
    def _(j):
        @pl.when(j + 1 < n_x)
        def _():
            net_a(j + 1)

        net_b(j)

        @pl.when(j == 1)
        def _():
            kv_finish(2)
            kv_start(3)

        @pl.when(j == 2)
        def _():
            kv_finish(3)
            keys_values()
            kv_start(4)

        for step in range(4, 7):
            @pl.when(j == step - 1)
            def _(step=step):
                kv_finish(step)
                kv_start(step + 1)

        @pl.when(j == n_x - 3)
        def _():
            kv_finish(7)

        for lo, hi, step in ((0, 5, n_x - 3), (5, 8, n_x - 2)):
            @pl.when(j == step)
            def _(lo=lo, hi=hi):
                for b in range(lo, hi):
                    attend(b)

        ready(chunk_of(j))
        compute(chunk_of(j))

    for c in pre_copies():
        c.wait()


def project_call(x, positions, norm_gain, w_query, w_key, w_value, w_gate, w_up, w_out, w_down):
    seq, d = x.shape
    depth, hd = w_query.shape
    ff = w_gate.shape[1]
    n_chunk = 3 + ff // GU
    inv_freq = jnp.asarray((10000.0 ** (-np.arange(0, hd, 2) / hd)).astype(np.float32))
    bf, f32 = jnp.bfloat16, jnp.float32
    hbm = pl.BlockSpec(memory_space=pl.ANY)
    vm = pl.BlockSpec(memory_space=pltpu.VMEM)
    flops = 2 * seq * d * (3 * hd + 2 * ff) + 2 * seq * seq * hd
    return pl.pallas_call(
        project_kernel,
        out_shape=(jax.ShapeDtypeStruct((seq, hd + ff), bf), jax.ShapeDtypeStruct((2, hd + PRE_DOWN, w_out.shape[1]), bf)),
        in_specs=[hbm, vm, vm] + [hbm] * 8,
        out_specs=(vm, hbm),
        scratch_shapes=[
            pltpu.VMEM((n_chunk, d // depth, TPA, TPA, depth // TPA // TPA, hd), bf),
            pltpu.VMEM((seq, d), bf),
            pltpu.VMEM((seq, hd), bf),
            pltpu.VMEM((2, TPA, TPA, seq // TPA // TPA, hd), bf),
            pltpu.VMEM((seq, hd // 2), f32),
            pltpu.VMEM((seq, hd // 2), f32),
            pltpu.VMEM((1, d), f32),
            pltpu.VMEM((X_SLOTS, LN_ROWS, d), bf),
            pltpu.VMEM((QB, seq), f32),
            pltpu.SemaphoreType.DMA((n_chunk, 8)),
            pltpu.SemaphoreType.DMA((n_chunk, 8)),
            pltpu.SemaphoreType.DMA((8,)),
            pltpu.SemaphoreType.DMA((8,)),
            pltpu.SemaphoreType.DMA((n_chunk, 2)),
            pltpu.SemaphoreType.DMA,
            pltpu.SemaphoreType.DMA((X_SLOTS,)),
            pltpu.SemaphoreType.DMA((16, 4)),
            pltpu.SemaphoreType.DMA((16, 4)),
            pltpu.SemaphoreType.DMA((2, 2)),
            pltpu.SemaphoreType.DMA((2, 2)),
        ],
        compiler_params=pltpu.CompilerParams(collective_id=0, has_side_effects=True, vmem_limit_bytes=63 * 1024 * 1024),
        cost_estimate=pl.CostEstimate(flops=flops, bytes_accessed=2 * seq * d, transcendentals=0),
        name="gather_project",
    )(x, positions.reshape(seq // 128, 128), inv_freq.reshape(1, hd // 2), norm_gain.reshape(1, depth),
      *(w.reshape(TPA, TPA, depth // TPA // TPA, w.shape[1]) for w in (w_query, w_key, w_value, w_gate, w_up)), w_out, w_down)


def reduce_kernel(az, pre, x_hbm, wo, wd, out, wbuf, part, r1, r2, r3, r4, xbuf,
                  ssem, rsem, wss, wrs, lsem):
    t = lax.axis_index("tp")
    f = lax.axis_index("fsdp")
    ring_y, ring_z = _ring_ids(t)
    xc, core, f_p, f_r, f_l = _fsdp_ids(f)
    seq = az.shape[0]
    cols = wbuf.shape[2]
    half = seq // 2
    big = half // TPA
    small = big // TPA
    hd = wo.shape[0]

    ld_o = pltpu.make_async_copy(wo, wbuf.at[0, pl.ds(0, hd)], lsem.at[0])
    ld_d = pltpu.make_async_copy(wd, wbuf.at[0, pl.ds(hd, wd.shape[0])], lsem.at[1])
    n_pre = pre.shape[1]
    n_rest = wbuf.shape[1] - n_pre
    ld_pre = [pltpu.make_async_copy(pre.at[e], wbuf.at[2 + 2 * e, pl.ds(0, n_pre)], lsem.at[4 + e]) for e in range(2)]
    ld_o.start()
    ld_d.start()
    for c in ld_pre:
        c.start()
    axes = ((ring_y, ring_z), (ring_z, ring_y))

    def own_rows(h):
        (i1, _, _), (i2, _, _) = axes[h]
        return pl.multiple_of(h * half + i1 * big + i2 * small, small)

    ld_x = [pltpu.make_async_copy(x_hbm.at[pl.ds(own_rows(h), small), :], xbuf.at[h], lsem.at[2 + h]) for h in range(2)]
    for c in ld_x:
        c.start()

    barrier = pltpu.get_barrier_semaphore()
    for other in (ring_y[1], ring_y[2], ring_z[1], ring_z[2]):
        pl.semaphore_signal(barrier, inc=1, device_id={"tp": other}, device_id_type=MESH)
    for other in (f_p, f_r, f_l):
        pl.semaphore_signal(barrier, inc=1, device_id={"fsdp": other}, device_id_type=MESH)
    pl.semaphore_wait(barrier, 7)

    def wcopy(k, src, dst, dev):
        return pltpu.make_async_remote_copy(src_ref=src, dst_ref=dst, send_sem=wss.at[k], recv_sem=wrs.at[k],
                                            device_id={"fsdp": dev}, device_id_type=MESH)

    kk = wbuf.shape[1]
    kh = kk // 2
    top, bot = pl.ds(0, kh), pl.ds(kh, kh)
    w_own_p = wcopy(0, wbuf.at[0], wbuf.at[1], f_p)
    rest = pl.ds(n_pre, n_rest)
    w_own_r = wcopy(1, wbuf.at[0, rest], wbuf.at[2, rest], f_r)
    w_own_l = wcopy(2, wbuf.at[0, rest], wbuf.at[4, rest], f_l)
    w_2p = wcopy(3, wbuf.at[2], wbuf.at[3], f_p)
    w_4p = wcopy(4, wbuf.at[4], wbuf.at[5], f_p)
    w_2r = wcopy(5, wbuf.at[2, top], wbuf.at[6, top], f_r)
    w_4l = wcopy(6, wbuf.at[4, bot], wbuf.at[6, bot], f_l)
    w_6p = wcopy(7, wbuf.at[6], wbuf.at[7], f_p)
    ld_o.wait()
    ld_d.wait()
    w_own_r.start()
    w_own_l.start()
    w_own_p.start()
    for c in ld_x + ld_pre:
        c.wait()

    def block_of(k):
        q = k // 2
        dx = 3 * q - 5 * (q // 2) - 2 * (q // 3)
        return ((xc + dx) % 4) * 2 + (core + k % 2) % 2

    def ring_copy(cb, h, d, step, src, dst, dev):
        return pltpu.make_async_remote_copy(src_ref=src, dst_ref=dst, send_sem=ssem.at[cb, h, d, step],
                                            recv_sem=rsem.at[cb, h, d, step], device_id={"tp": dev}, device_id_type=MESH)

    def rs_first(cb, h, step, ring, base, n, land):
        i, r, l = ring
        o = (i + 2) % TPA
        m = n // 2
        s = pl.multiple_of(base + o * n, m)
        return (ring_copy(cb, h, 0, step, part.at[cb % PART_SLOTS, pl.ds(s, m)], land.at[cb % land.shape[0], h, 0], r),
                ring_copy(cb, h, 1, step, part.at[cb % PART_SLOTS, pl.ds(s + m, m)], land.at[cb % land.shape[0], h, 1], l))

    def rs_second(cb, h, step, ring, base, n, land):
        i, r, l = ring
        s_r = pl.multiple_of(base + ((i + 1) % TPA) * n, n)
        s_l = pl.multiple_of(base + ((i + 3) % TPA) * n, n)
        return (ring_copy(cb, h, 0, step, part.at[cb % PART_SLOTS, pl.ds(s_r, n)], land.at[cb % land.shape[0], h, 0], r),
                ring_copy(cb, h, 1, step, part.at[cb % PART_SLOTS, pl.ds(s_l, n)], land.at[cb % land.shape[0], h, 1], l))

    def rs_update(cb, h, ring, base, n, land):
        i, _, _ = ring
        m = n // 2
        s_r = pl.multiple_of(base + ((i + 1) % TPA) * n, m)
        s_l = pl.multiple_of(base + ((i + 3) % TPA) * n + m, m)
        for s, d in ((s_r, 0), (s_l, 1)):
            rows = pl.ds(s, m)
            part[cb % PART_SLOTS, rows] = (part[cb % PART_SLOTS, rows].astype(jnp.float32) + land[cb % land.shape[0], h, d].astype(jnp.float32)).astype(jnp.bfloat16)

    def ag_first(cb, h, step, ring, src, base, n):
        i, r, l = ring
        g = block_of(cb)
        dst = out.at[g, pl.ds(pl.multiple_of(base + i * n, n), n)]
        if src is None:
            src = dst
        return (ring_copy(cb, h, 0, step, src, dst, r), ring_copy(cb, h, 1, step, src, dst, l))

    def ag_second(cb, h, step, ring, base, n):
        i, r, l = ring
        g = block_of(cb)
        m = n // 2
        from_l = out.at[g, pl.ds(pl.multiple_of(base + ((i + 3) % TPA) * n, m), m)]
        from_r = out.at[g, pl.ds(pl.multiple_of(base + ((i + 1) % TPA) * n + m, m), m)]
        return (ring_copy(cb, h, 0, step, from_l, from_l, r), ring_copy(cb, h, 1, step, from_r, from_r, l))

    def copies(cb, step):
        res = []
        for h in range(2):
            ring1, ring2 = axes[h]
            base1 = h * half
            base2 = pl.multiple_of(h * half + ring1[0] * big, big)
            if step == 0:
                res.extend(rs_first(cb, h, step, ring1, base1, big, r1))
            elif step == 1:
                res.extend(rs_second(cb, h, step, ring1, base1, big, r2))
            elif step == 2:
                res.extend(rs_first(cb, h, step, ring2, base2, small, r3))
            elif step == 3:
                res.extend(rs_second(cb, h, step, ring2, base2, small, r4))
            elif step == 4:
                res.extend(ag_first(cb, h, step, ring2, None, base2, small))
            elif step == 5:
                res.extend(ag_second(cb, h, step, ring2, base2, small))
            elif step == 6:
                res.extend(ag_first(cb, h, step, ring1, None, base1, big))
            else:
                res.extend(ag_second(cb, h, step, ring1, base1, big))
        return res

    def start(cb, step):
        for c in copies(cb, step):
            c.start()

    def finish(cb, step):
        for c in copies(cb, step):
            c.wait_recv()
            c.wait_send()

    def stage0(cb):
        @pl.when(cb == 1)
        def _():
            w_own_p.wait()

        @pl.when(cb == 2)
        def _():
            w_own_r.wait()
            w_own_l.wait()
            w_2r.start()
            w_4l.start()
            w_2p.start()
            w_4p.start()

        @pl.when(cb == 3)
        def _():
            w_2p.wait()

        @pl.when(cb == 5)
        def _():
            w_4p.wait()

        @pl.when(cb == 6)
        def _():
            w_2r.wait()
            w_4l.wait()
            w_6p.start()

        @pl.when(cb == 7)
        def _():
            w_6p.wait()

        @pl.loop(0, seq // MT)
        def _(i):
            rows = pl.ds(pl.multiple_of(i * MT, MT), MT)
            part[cb % PART_SLOTS, rows] = jnp.dot(az[rows, :], wbuf[cb], preferred_element_type=jnp.float32).astype(jnp.bfloat16)

        start(cb, 0)

    def stage1(cb):
        finish(cb, 0)
        for h in range(2):
            rs_update(cb, h, axes[h][0], h * half, big, r1)
        start(cb, 1)

    def stage2(cb):
        finish(cb, 1)
        for h in range(2):
            rows = pl.ds(pl.multiple_of(h * half + axes[h][0][0] * big, big), big)
            part[cb % PART_SLOTS, rows] = (part[cb % PART_SLOTS, rows].astype(jnp.float32) + r2[cb % r2.shape[0], h, 0].astype(jnp.float32)
                              + r2[cb % r2.shape[0], h, 1].astype(jnp.float32)).astype(jnp.bfloat16)
        start(cb, 2)

    def stage3(cb):
        finish(cb, 2)
        for h in range(2):
            rs_update(cb, h, axes[h][1], pl.multiple_of(h * half + axes[h][0][0] * big, big), small, r3)
        start(cb, 3)

    def stage4(cb):
        finish(cb, 3)
        g = block_of(cb)
        for h in range(2):
            branch = (part[cb % PART_SLOTS, pl.ds(own_rows(h), small)].astype(jnp.float32) + r4[cb % r4.shape[0], h, 0].astype(jnp.float32)
                      + r4[cb % r4.shape[0], h, 1].astype(jnp.float32))
            xs = xbuf[h, :, pl.ds(pl.multiple_of(g * cols, cols), cols)].astype(jnp.float32)
            out[g, pl.ds(own_rows(h), small), :] = (xs + branch).astype(jnp.bfloat16)
        start(cb, 4)

    def stage5(cb):
        finish(cb, 4)
        start(cb, 5)

    def stage6(cb):
        finish(cb, 5)
        start(cb, 6)

    def stage7(cb):
        finish(cb, 6)
        start(cb, 7)

    def stage8(cb):
        finish(cb, 7)

    stages = (stage0, stage1, stage2, stage3, stage4, stage5, stage6, stage7, stage8)

    @pl.loop(0, COL + GAP + len(stages) - 1)
    def _(n):
        for s, fn in enumerate(stages):
            turn = n - s

            @pl.when(jnp.logical_or(jnp.logical_and(turn >= 0, turn < 2), jnp.logical_and(turn >= 2 + GAP, turn < COL + GAP)))
            def _(fn=fn, turn=turn):
                fn(jnp.where(turn >= 2, turn - GAP, turn))


MT = 512
PART_SLOTS = 5
LAND_SLOTS = 4
GAP = 1


def reduce_call(az, pre, x, wo, wd):
    seq, kk = az.shape
    d = x.shape[1]
    cols = d // COL
    half = seq // 2
    big, small = half // TPA, half // TPA // TPA
    bf = jnp.bfloat16
    hbm = pl.BlockSpec(memory_space=pl.ANY)
    vm = pl.BlockSpec(memory_space=pltpu.VMEM)
    res = pl.pallas_call(
        reduce_kernel,
        out_shape=pltpu.VMEM((COL, seq, cols), bf),
        in_specs=[vm, hbm, hbm, hbm, hbm],
        out_specs=vm,
        scratch_shapes=[
            pltpu.VMEM((COL, kk, cols), bf),
            pltpu.VMEM((PART_SLOTS, seq, cols), bf),
            pltpu.VMEM((COL, 2, 2, big // 2, cols), bf),
            pltpu.VMEM((LAND_SLOTS, 2, 2, big, cols), bf),
            pltpu.VMEM((COL, 2, 2, small // 2, cols), bf),
            pltpu.VMEM((COL, 2, 2, small, cols), bf),
            pltpu.VMEM((2, small, d), bf),
            pltpu.SemaphoreType.DMA((COL, 2, 2, 8)),
            pltpu.SemaphoreType.DMA((COL, 2, 2, 8)),
            pltpu.SemaphoreType.DMA((8,)),
            pltpu.SemaphoreType.DMA((8,)),
            pltpu.SemaphoreType.DMA((6,)),
        ],
        compiler_params=pltpu.CompilerParams(collective_id=1, has_side_effects=True, vmem_limit_bytes=40 * 1024 * 1024),
        cost_estimate=pl.CostEstimate(flops=2 * seq * kk * d, bytes_accessed=4 * seq * d, transcendentals=0),
        name="down_reduce",
    )(az, pre, x, wo, wd)
    return write_out(res)[None]


def write_kernel(src, dst, sem):
    n, seq, cols = src.shape
    copies = [pltpu.make_async_copy(src.at[b], dst.at[:, pl.ds(b * cols, cols)], sem.at[b]) for b in range(n)]
    for c in copies:
        c.start()
    for c in copies:
        c.wait()


def write_out(blocks):
    n, seq, cols = blocks.shape
    return pl.pallas_call(
        write_kernel,
        out_shape=jax.ShapeDtypeStruct((seq, n * cols), blocks.dtype),
        in_specs=[pl.BlockSpec(memory_space=pltpu.VMEM)],
        out_specs=pl.BlockSpec(memory_space=pl.ANY),
        scratch_shapes=[pltpu.SemaphoreType.DMA((n,))],
        compiler_params=pltpu.CompilerParams(vmem_limit_bytes=24 * 1024 * 1024),
        name="write_out",
    )(blocks)


def solution(mesh):
    row_spec = P(("dp", "fsdp"), None, None)

    def local_layer(hidden, positions, norm_gain, w_query, w_key, w_value, w_gate, w_up, w_out, w_down):
        az, pre = project_call(hidden[0], positions, norm_gain, w_query, w_key, w_value, w_gate, w_up, w_out, w_down)
        return reduce_call(az, pre, hidden[0], w_out, w_down)

    in_specs = (row_spec, P(None), P("fsdp"), P("fsdp", "tp"), P("fsdp", None), P("fsdp", None), P("fsdp", "tp"), P("fsdp", "tp"), P("tp", "fsdp"), P("tp", "fsdp"))
    return jax.shard_map(local_layer, mesh=mesh, in_specs=in_specs, out_specs=row_spec, check_vma=False)
```

```python
import jax
import jax.numpy as jnp
import numpy as np
from jax import lax
from jax.experimental import pallas as pl
from jax.experimental.pallas import tpu as pltpu
from jax.sharding import PartitionSpec as P

NORM_EPS = 1e-6
MESH = pl.DeviceIdType.MESH
TPA = 4
COL = 8


def _ring_ids(t):
    z, y = t // TPA, t % TPA
    y_r, y_l = z * TPA + (y + 1) % TPA, z * TPA + (y + 3) % TPA
    z_r, z_l = ((z + 1) % TPA) * TPA + y, ((z + 3) % TPA) * TPA + y
    return (y, y_r, y_l), (z, z_r, z_l)


def _fsdp_ids(f):
    xc, core = f // 2, f % 2
    f_p = xc * 2 + (1 - core)
    f_r = ((xc + 1) % 4) * 2 + core
    f_l = ((xc + 3) % 4) * 2 + core
    return xc, core, f_p, f_r, f_l


QB = 256
LN_ROWS = 128
X_SLOTS = 3
LN_SUB = 64
GU = 128
M1 = 1024
M2 = 512
VMEM_LIMIT = 95 * 512 * 1024


def project_part(x_hbm, pos, inv_freq, gain, wq, wk, wv, wg, wu, az, wbuf, h, q, kv, cos_t, sin_t, gbuf, xb, scores,
                 ssem, rsem, gss, grs, lsem, gsem, xsem, kss, krs, send_late):
    f = lax.axis_index("fsdp")
    nf = lax.axis_size("fsdp")
    t = lax.axis_index("tp")
    nt = lax.axis_size("tp")
    ring_y, ring_z = _ring_ids(t)
    z_id, y_id = ring_z[0], ring_y[0]
    xc, core, f_p, f_r, f_l = _fsdp_ids(f)
    f_o = ((xc + 2) % 4) * 2 + core
    seq, d = h.shape
    depth = gain.shape[1]
    hd = wq.shape[3]
    n_chunk = wbuf.shape[0]
    n_ff = wg.shape[3] // GU
    n_x = n_ff + 1

    def half_of(i, dev, part):
        return wbuf.at[i, dev, pl.ds(part * (TPA // 2), TPA // 2)]

    def load(i, part, src, col):
        return pltpu.make_async_copy(src.at[:, :, :, pl.ds(col, GU)], wbuf.at[i, f, :, :, :, pl.ds(part * GU, GU)], lsem.at[i, part])

    ld_kv = [pltpu.make_async_copy(w.at[z_id, y_id], wbuf.at[1 + i, f, z_id, y_id], lsem.at[1 + i, 0]) for i, w in enumerate((wk, wv))]
    for c in ld_kv:
        c.start()
    for part in range(2):
        load(0, part, wq, part * GU).start()
    for j in range(n_ff):
        load(3 + j, 0, wg, j * GU).start()
        load(3 + j, 1, wu, j * GU).start()

    def load_x(blk):
        slot = blk % X_SLOTS
        return pltpu.make_async_copy(x_hbm.at[pl.ds(pl.multiple_of(blk * LN_ROWS, LN_ROWS), LN_ROWS), :], xb.at[slot], xsem.at[slot])

    for blk in range(X_SLOTS - 1):
        load_x(blk).start()
    ld_g = pltpu.make_async_copy(gain, gbuf.at[:, pl.ds(pl.multiple_of(f * depth, depth), depth)], gsem)
    ld_g.start()

    barrier = pltpu.get_barrier_semaphore()
    for e in range(1, nf):
        pl.semaphore_signal(barrier, inc=1, device_id={"fsdp": (f + e) % nf}, device_id_type=MESH)
    for other in (ring_y[1], ring_y[2], ring_z[1], ring_z[2]):
        pl.semaphore_signal(barrier, inc=1, device_id={"tp": other}, device_id_type=MESH)
    pl.semaphore_wait(barrier, nf - 1 + 4)

    def rcopy(i, s, src, dev):
        return pltpu.make_async_remote_copy(src_ref=src, dst_ref=src, send_sem=ssem.at[i, s], recv_sem=rsem.at[i, s],
                                            device_id={"fsdp": dev}, device_id_type=MESH)

    def transfer(i, s):
        src, dev = (
            (lambda: wbuf.at[i, f], f_r),
            (lambda: wbuf.at[i, f], f_l),
            (lambda: wbuf.at[i, f], f_p),
            (lambda: half_of(i, f_l, 0), f_r),
            (lambda: half_of(i, f_r, 1), f_l),
            (lambda: wbuf.at[i, f_l], f_p),
            (lambda: wbuf.at[i, f_r], f_p),
            (lambda: wbuf.at[i, f_o], f_p),
        )[s]
        return rcopy(i, s, src(), dev)

    def chunk_of(xi):
        return xi + 2 * ((xi + n_x - 1) // n_x)

    kv_rings = ((ring_y, ring_z), (ring_z, ring_y))

    def ids_of(i, dev):
        return (z_id, dev) if i == 0 else (dev, y_id)

    def w_view(i, line, dev, part):
        lo, n = ((0, nf), (0, nf // 2), (nf // 2, nf // 2))[part]
        if not line:
            z, y = ids_of(i, dev)
            return wbuf.at[1 + i, pl.ds(lo, n), z, y]
        return wbuf.at[1 + i, pl.ds(lo, n), dev] if i == 0 else wbuf.at[1 + i, pl.ds(lo, n), :, dev]

    def o_view(i, line, dev, part):
        size = TPA if line else kv.shape[3]
        lo, n = ((0, size), (0, size // 2), (size // 2, size // 2))[part]
        if not line:
            z, y = ids_of(i, dev)
            return kv.at[i, z, y, pl.ds(lo, n)]
        return kv.at[i, dev, pl.ds(lo, n)] if i == 0 else kv.at[i, pl.ds(lo, n), dev]

    def kv_copies(step):
        res = []
        view = w_view if step < 4 else o_view
        for i in range(2):
            me, r, l = kv_rings[i][step // 2 % 2]
            line = step // 2 % 2 == 1
            if step % 2 == 0:
                src = (view(i, line, me, 0), view(i, line, me, 0))
            else:
                src = (view(i, line, (me + TPA - 1) % TPA, 1), view(i, line, (me + 1) % TPA, 2))
            for d_, (part, dev) in enumerate(zip(src, (r, l))):
                res.append(pltpu.make_async_remote_copy(src_ref=part, dst_ref=part, send_sem=kss.at[nf + step, 2 * i + d_], recv_sem=krs.at[nf + step, 2 * i + d_],
                                                        device_id={"tp": dev}, device_id_type=MESH))
        return res

    def kv_start(step):
        for c in kv_copies(step):
            c.start()

    def kv_finish(step):
        for c in kv_copies(step):
            c.wait_recv()
            c.wait_send()

    def send_own(i):
        for part in range(2):
            load(i, part, wq, part * GU).wait()
        for s in range(3):
            transfer(i, s).start()

    def net_a(xi):
        i = chunk_of(xi)
        transfer(i, 0).wait_recv()
        transfer(i, 3).start()
        transfer(i, 1).wait_recv()
        transfer(i, 4).start()

        @pl.when(xi + 2 < n_x)
        def _():
            send_own(chunk_of(xi + 2))

        @pl.when(xi + 1 == n_x)
        def _():
            send_late()

        transfer(i, 5).start()
        transfer(i, 6).start()

    def net_b(xi):
        i = chunk_of(xi)
        transfer(i, 3).wait_recv()
        transfer(i, 4).wait_recv()
        transfer(i, 7).start()

    def ready(i):
        for s in (2, 5, 6, 7):
            transfer(i, s).wait_recv()
        for s in range(8):
            transfer(i, s).wait_send()

    ld_g.wait()
    gcol = gbuf.at[:, pl.ds(pl.multiple_of(f * depth, depth), depth)]
    gcopies = [pltpu.make_async_remote_copy(src_ref=gcol, dst_ref=gcol, send_sem=gss.at[e], recv_sem=grs.at[e],
                                            device_id={"fsdp": (f + e) % nf}, device_id_type=MESH) for e in range(1, nf)]
    for c in gcopies:
        c.start()
    kv_x = []
    for i in range(2):
        ld_kv[i].wait()
        for e in range(1, nf):
            part = wbuf.at[1 + i, f, z_id, y_id]
            kv_x.append(pltpu.make_async_remote_copy(src_ref=part, dst_ref=part, send_sem=kss.at[e, i], recv_sem=krs.at[e, i],
                                                     device_id={"fsdp": (f + e) % nf}, device_id_type=MESH))
    for c in kv_x:
        c.start()
    send_own(0)
    send_own(3)

    lanes = pos.shape[1]
    eye = lax.broadcasted_iota(jnp.int32, (lanes, lanes), 0) == lax.broadcasted_iota(jnp.int32, (lanes, lanes), 1)

    @pl.loop(0, seq // lanes)
    def _(b):
        rows = pl.ds(pl.multiple_of(b * lanes, lanes), lanes)
        line = pos[pl.ds(b, 1), :].astype(jnp.float32)
        column = jnp.sum(jnp.where(eye, line, 0.0), axis=-1, keepdims=True)
        angle = column * inv_freq[...]
        cos_t[rows, :] = jnp.cos(angle)
        sin_t[rows, :] = jnp.sin(angle)

    for c in gcopies:
        c.wait()
    for c in kv_x:
        c.wait()
    kv_start(0)

    n_blk = seq // LN_ROWS

    def norm_blocks(lo, hi):
        @pl.loop(lo, hi)
        def _(blk):
            load_x(blk).wait()

            @pl.when(blk + X_SLOTS - 1 < n_blk)
            def _():
                load_x(blk + X_SLOTS - 1).start()

            @pl.loop(0, LN_ROWS // LN_SUB)
            def _(r):
                row = xb[blk % X_SLOTS, pl.ds(pl.multiple_of(r * LN_SUB, LN_SUB), LN_SUB), :].astype(jnp.float32)
                centered = row - jnp.sum(row, axis=-1, keepdims=True) * (1.0 / d)
                var = jnp.sum(centered * centered, axis=-1, keepdims=True) * (1.0 / d)
                out = centered * lax.rsqrt(var + NORM_EPS) * gbuf[...]
                h[pl.ds(pl.multiple_of(blk * LN_ROWS + r * LN_SUB, LN_SUB), LN_SUB), :] = out.astype(jnp.bfloat16)

    norm_blocks(0, n_blk // 4)
    kv_finish(0)
    kv_start(1)
    norm_blocks(n_blk // 4, n_blk // 2)
    net_a(0)
    kv_finish(1)
    kv_start(2)
    norm_blocks(n_blk // 2, n_blk)

    def product(i, rows):
        return jnp.dot(h[rows, :], wbuf[i].reshape(d, hd), preferred_element_type=jnp.float32)

    def rope(y, rows):
        a, b = y[:, :hd // 2].astype(jnp.bfloat16).astype(jnp.float32), y[:, hd // 2:].astype(jnp.bfloat16).astype(jnp.float32)
        c, s = cos_t[rows, :], sin_t[rows, :]
        return jnp.concatenate([a * c - b * s, b * c + a * s], axis=1).astype(jnp.bfloat16)

    def keys_values():
        n = kv.shape[3]
        rows = pl.ds(pl.multiple_of(t * n, n), n)
        kv[0, z_id, y_id] = rope(product(1, rows), rows)
        kv[1, z_id, y_id] = product(2, rows).astype(jnp.bfloat16)

    def compute(i):
        @pl.when(i == 0)
        def _():
            @pl.loop(0, seq // M1)
            def _(m):
                rows = pl.ds(pl.multiple_of(m * M1, M1), M1)
                q[rows, :] = rope(product(i, rows), rows)

        @pl.when(i >= 3)
        def _():
            for m in range(seq // M2):
                rows = pl.ds(m * M2, M2)
                y = product(i, rows)
                g = y[:, :GU].astype(jnp.bfloat16).astype(jnp.float32)
                u = y[:, GU:].astype(jnp.bfloat16).astype(jnp.float32)
                z = (g * (1.0 / (1.0 + jnp.exp(-g)))) * u
                az[rows, pl.ds(pl.multiple_of(hd + (i - 3) * GU, GU), GU)] = z.astype(jnp.bfloat16)

    scale = hd ** -0.5
    n_q = seq // QB

    keys, values = (kv.at[i].reshape(seq, hd) for i in range(2))

    def attend(b):
        rows = pl.ds(b * QB, QB)
        qb = q[rows, :]
        peak = None
        for t in range(b + 1):
            s = lax.dot_general(qb, keys[pl.ds(t * QB, QB), :], (((1,), (1,)), ((), ())), preferred_element_type=jnp.float32) * scale
            if t == b:
                keep = lax.broadcasted_iota(jnp.int32, (QB, QB), 1) <= lax.broadcasted_iota(jnp.int32, (QB, QB), 0)
                s = jnp.where(keep, s, -1e30)
            scores[:, t * QB:(t + 1) * QB] = s
            s = jnp.maximum(s[:, :128], s[:, 128:])
            peak = s if peak is None else jnp.maximum(peak, s)
        peak = jnp.max(peak, axis=-1, keepdims=True)
        total = None
        for t in range(b + 1):
            e = jnp.exp(scores[:, t * QB:(t + 1) * QB] - peak)
            scores[:, t * QB:(t + 1) * QB] = e
            e = e[:, :128] + e[:, 128:]
            total = e if total is None else total + e
        inv = 1.0 / jnp.sum(total, axis=-1, keepdims=True)
        p = (scores[:, :(b + 1) * QB] * inv).astype(jnp.bfloat16)
        out = jnp.dot(p, values[pl.ds(0, (b + 1) * QB), :], preferred_element_type=jnp.float32)
        az[rows, 0:hd] = out.astype(jnp.bfloat16)

    @pl.loop(0, n_x)
    def _(j):
        @pl.when(j + 1 < n_x)
        def _():
            net_a(j + 1)

        net_b(j)

        @pl.when(j == 1)
        def _():
            kv_finish(2)
            kv_start(3)

        @pl.when(j == 2)
        def _():
            kv_finish(3)
            keys_values()
            kv_start(4)

        for step in range(4, 7):
            @pl.when(j == step - 1)
            def _(step=step):
                kv_finish(step)
                kv_start(step + 1)

        @pl.when(j == n_x - 3)
        def _():
            kv_finish(7)

        for lo, hi, step in ((0, 5, n_x - 3), (5, 8, n_x - 2)):
            @pl.when(j == step)
            def _(lo=lo, hi=hi):
                for b in range(lo, hi):
                    attend(b)

        ready(chunk_of(j))
        compute(chunk_of(j))


def reduce_part(az, x_hbm, wo, wd, out, w2, wbuf, wvm, xb, ssem, rsem, wss, wrs, lsem, xsem, phase):
    t = lax.axis_index("tp")
    f = lax.axis_index("fsdp")
    ring_y, ring_z = _ring_ids(t)
    xc, core, f_p, f_r, f_l = _fsdp_ids(f)
    seq = az.shape[0]
    cols = wvm.shape[2]
    part = wbuf.at[pl.ds(0, 5)].reshape(5, 2, seq, cols // 2)
    half = seq // 2
    big = half // TPA
    small = big // TPA
    r2 = wbuf.at[pl.ds(5, 2)].reshape(LAND_SLOTS, 2, 2, 2, big, cols // 2)
    r1 = wbuf.at[pl.ds(7, 2)].reshape(COL, 2, 2, 2, big // 2, cols // 2)
    r4 = wbuf.at[9].reshape(COL, 2, 2, 2, small, cols // 2)
    r3 = wbuf.at[10, pl.ds(0, 4)].reshape(COL, 2, 2, 2, small // 2, cols // 2)
    hd = wo.shape[0]

    axes = ((ring_y, ring_z), (ring_z, ring_y))

    def own_rows(h):
        (i1, _, _), (i2, _, _) = axes[h]
        return pl.multiple_of(h * half + i1 * big + i2 * small, small)

    xrow = [xb.at[0, pl.ds(hf * small, small)] for hf in range(2)]
    ld_x = [pltpu.make_async_copy(x_hbm.at[pl.ds(own_rows(hf), small), :], xrow[hf], xsem.at[hf]) for hf in range(2)]

    def wcopy(k, e, src, dst, dev):
        return pltpu.make_async_remote_copy(src_ref=src, dst_ref=dst, send_sem=wss.at[k, e], recv_sem=wrs.at[k, e],
                                            device_id={"fsdp": dev}, device_id_type=MESH)

    kk = wvm.shape[1]
    kh = kk // 2
    rows_o, rows_d = pl.ds(0, hd), pl.ds(hd, kk - hd)

    def w_own(k, slot, dev):
        return wcopy(k, 0, wo, w2.at[slot, rows_o], dev), wcopy(k, 1, wd, w2.at[slot, rows_d], dev)

    def w_whole(k, slot):
        return wcopy(k, 0, w2.at[slot], w2.at[slot + 1], f_p)

    def w_2r():
        return wcopy(5, 0, w2.at[2, pl.ds(0, kh)], w2.at[6, pl.ds(0, kh)], f_r)

    def w_4l():
        return wcopy(6, 0, w2.at[4, pl.ds(kh, kh)], w2.at[6, pl.ds(kh, kh)], f_l)

    def load_own():
        return (pltpu.make_async_copy(wo, wvm.at[0, rows_o], lsem.at[2]), pltpu.make_async_copy(wd, wvm.at[0, rows_d], lsem.at[3]))

    def load_w(cb):
        return pltpu.make_async_copy(w2.at[cb], wvm.at[cb % 2], lsem.at[cb % 2])

    def send_late():
        for c in w_own(1, 2, f_r) + w_own(2, 4, f_l) + w_own(0, 1, f_p) + load_own():
            c.start()

    def fetch(cb):
        @pl.when(cb == 1)
        def _():
            for c in w_own(0, 1, f_p):
                c.wait()

        @pl.when(cb == 2)
        def _():
            for c in w_own(1, 2, f_r) + w_own(2, 4, f_l):
                c.wait()
            w_2r().start()
            w_4l().start()
            w_whole(3, 2).start()
            w_whole(4, 4).start()

        @pl.when(cb == 3)
        def _():
            w_whole(3, 2).wait()

        @pl.when(cb == 5)
        def _():
            w_whole(4, 4).wait()

        @pl.when(cb == 6)
        def _():
            w_2r().wait()
            w_4l().wait()
            w_whole(7, 6).start()

        @pl.when(cb == 7)
        def _():
            w_whole(7, 6).wait()

        load_w(cb).start()

    def block_of(k):
        q = k // 2
        dx = 3 * q - 5 * (q // 2) - 2 * (q // 3)
        return ((xc + dx) % 4) * 2 + (core + k % 2) % 2

    def block_cols(cb):
        return pl.ds(pl.multiple_of(block_of(cb) * cols, cols), cols)

    def ring_copy(cb, h, d, step, src, dst, dev):
        return pltpu.make_async_remote_copy(src_ref=src, dst_ref=dst, send_sem=ssem.at[cb, h, d, step],
                                            recv_sem=rsem.at[cb, h, d, step], device_id={"tp": dev}, device_id_type=MESH)

    def rs_first(cb, h, step, ring, base, n, land):
        i, r, l = ring
        o = (i + 2) % TPA
        m = n // 2
        s = pl.multiple_of(base + o * n, m)
        return (ring_copy(cb, h, 0, step, part.at[cb % PART_SLOTS, :, pl.ds(s, m)], land.at[cb % land.shape[0], h, 0], r),
                ring_copy(cb, h, 1, step, part.at[cb % PART_SLOTS, :, pl.ds(s + m, m)], land.at[cb % land.shape[0], h, 1], l))

    def rs_second(cb, h, step, ring, base, n, land):
        i, r, l = ring
        s_r = pl.multiple_of(base + ((i + 1) % TPA) * n, n)
        s_l = pl.multiple_of(base + ((i + 3) % TPA) * n, n)
        return (ring_copy(cb, h, 0, step, part.at[cb % PART_SLOTS, :, pl.ds(s_r, n)], land.at[cb % land.shape[0], h, 0], r),
                ring_copy(cb, h, 1, step, part.at[cb % PART_SLOTS, :, pl.ds(s_l, n)], land.at[cb % land.shape[0], h, 1], l))

    def rs_update(cb, h, ring, base, n, land):
        i, _, _ = ring
        m = n // 2
        s_r = pl.multiple_of(base + ((i + 1) % TPA) * n, m)
        s_l = pl.multiple_of(base + ((i + 3) % TPA) * n + m, m)
        for s, d in ((s_r, 0), (s_l, 1)):
            rows = pl.ds(s, m)
            part[cb % PART_SLOTS, :, rows] = (part[cb % PART_SLOTS, :, rows].astype(jnp.float32) + land[cb % land.shape[0], h, d].astype(jnp.float32)).astype(jnp.bfloat16)

    def ag_first(cb, h, step, ring, src, base, n):
        i, r, l = ring
        dst = out.at[pl.ds(pl.multiple_of(base + i * n, n), n), block_cols(cb)]
        if src is None:
            src = dst
        return (ring_copy(cb, h, 0, step, src, dst, r), ring_copy(cb, h, 1, step, src, dst, l))

    def ag_second(cb, h, step, ring, base, n):
        i, r, l = ring
        m = n // 2
        from_l = out.at[pl.ds(pl.multiple_of(base + ((i + 3) % TPA) * n, m), m), block_cols(cb)]
        from_r = out.at[pl.ds(pl.multiple_of(base + ((i + 1) % TPA) * n + m, m), m), block_cols(cb)]
        return (ring_copy(cb, h, 0, step, from_l, from_l, r), ring_copy(cb, h, 1, step, from_r, from_r, l))

    def copies(cb, step):
        res = []
        for h in range(2):
            ring1, ring2 = axes[h]
            base1 = h * half
            base2 = pl.multiple_of(h * half + ring1[0] * big, big)
            if step == 0:
                res.extend(rs_first(cb, h, step, ring1, base1, big, r1))
            elif step == 1:
                res.extend(rs_second(cb, h, step, ring1, base1, big, r2))
            elif step == 2:
                res.extend(rs_first(cb, h, step, ring2, base2, small, r3))
            elif step == 3:
                res.extend(rs_second(cb, h, step, ring2, base2, small, r4))
            elif step == 4:
                res.extend(ag_first(cb, h, step, ring2, None, base2, small))
            elif step == 5:
                res.extend(ag_second(cb, h, step, ring2, base2, small))
            elif step == 6:
                res.extend(ag_first(cb, h, step, ring1, None, base1, big))
            else:
                res.extend(ag_second(cb, h, step, ring1, base1, big))
        return res

    def start(cb, step):
        for c in copies(cb, step):
            c.start()

    def finish(cb, step):
        for c in copies(cb, step):
            c.wait_recv()
            c.wait_send()

    def stage0(cb):
        @pl.when(cb == 0)
        def _():
            for c in load_own():
                c.wait()

        @pl.when(cb > 0)
        def _():
            load_w(cb).wait()

        @pl.loop(0, seq // MT)
        def _(i):
            rows = pl.ds(pl.multiple_of(i * MT, MT), MT)
            y = jnp.dot(az[rows, :], wvm[cb % 2], preferred_element_type=jnp.float32).astype(jnp.bfloat16)
            for hf in range(2):
                part[cb % PART_SLOTS, hf, rows] = y[:, hf * (cols // 2):(hf + 1) * (cols // 2)]

        @pl.when(cb == 0)
        def _():
            pl.semaphore_wait(phase, 4)

        start(cb, 0)

    def stage1(cb):
        finish(cb, 0)
        for h in range(2):
            rs_update(cb, h, axes[h][0], h * half, big, r1)
        start(cb, 1)

    def stage2(cb):
        finish(cb, 1)
        for h in range(2):
            rows = pl.ds(pl.multiple_of(h * half + axes[h][0][0] * big, big), big)
            part[cb % PART_SLOTS, :, rows] = (part[cb % PART_SLOTS, :, rows].astype(jnp.float32) + r2[cb % r2.shape[0], h, 0].astype(jnp.float32)
                              + r2[cb % r2.shape[0], h, 1].astype(jnp.float32)).astype(jnp.bfloat16)
        start(cb, 2)

    def stage3(cb):
        finish(cb, 2)
        for h in range(2):
            rs_update(cb, h, axes[h][1], pl.multiple_of(h * half + axes[h][0][0] * big, big), small, r3)
        start(cb, 3)

    def stage4(cb):
        finish(cb, 3)
        g = block_of(cb)
        for h in range(2):
            branch = (part[cb % PART_SLOTS, :, pl.ds(own_rows(h), small)].astype(jnp.float32) + r4[cb % r4.shape[0], h, 0].astype(jnp.float32)
                      + r4[cb % r4.shape[0], h, 1].astype(jnp.float32))
            for hf in range(2):
                lanes = pl.ds(pl.multiple_of(g * cols + hf * (cols // 2), cols // 2), cols // 2)
                xs = xb[0, pl.ds(h * small, small), lanes].astype(jnp.float32)
                out[pl.ds(own_rows(h), small), lanes] = (xs + branch[hf]).astype(jnp.bfloat16)
        start(cb, 4)

    def stage5(cb):
        finish(cb, 4)
        start(cb, 5)

    def stage6(cb):
        finish(cb, 5)
        start(cb, 6)

    def stage7(cb):
        finish(cb, 6)
        start(cb, 7)

    def stage8(cb):
        finish(cb, 7)

    stages = (stage0, stage1, stage2, stage3, stage4, stage5, stage6, stage7, stage8)

    def reduce_all():
        for c in ld_x:
            c.start()
        for other in (ring_y[1], ring_y[2], ring_z[1], ring_z[2]):
            pl.semaphore_signal(phase, inc=1, device_id={"tp": other}, device_id_type=MESH)
        for c in ld_x:
            c.wait()

        @pl.loop(0, COL + len(stages) - 1)
        def _(n):
            for s, fn in enumerate(stages):
                cb = n - s

                @pl.when(jnp.logical_and(cb >= 0, cb < COL))
                def _(fn=fn, cb=cb):
                    fn(cb)

            @pl.when(n + 1 < COL)
            def _():
                fetch(n + 1)

    return send_late, reduce_all


MT = 512
PART_SLOTS = 5
LAND_SLOTS = 4


def layer_kernel(x_hbm, pos, inv_freq, gain, wq, wk, wv, wg, wu, wo, wd, out, w2, wbuf, q, kv, cos_t, sin_t, gbuf, xb, scores, az, wvm,
                 ssem, rsem, gss, grs, lsem, gsem, xsem, kss, krs, rss, rrs, wss, wrs, wlsem, phase):
    send_late, reduce_all = reduce_part(az, x_hbm, wo, wd, out, w2, wbuf, wvm, xb, rss, rrs, wss, wrs, wlsem, xsem, phase)
    project_part(x_hbm, pos, inv_freq, gain, wq, wk, wv, wg, wu, az, wbuf, out, q, kv, cos_t, sin_t, gbuf, xb, scores,
                 ssem, rsem, gss, grs, lsem, gsem, xsem, kss, krs, send_late)
    reduce_all()


def layer_call(x, positions, norm_gain, w_query, w_key, w_value, w_gate, w_up, w_out, w_down):
    seq, d = x.shape
    depth, hd = w_query.shape
    ff = w_gate.shape[1]
    n_chunk = 3 + ff // GU
    cols = d // COL
    inv_freq = jnp.asarray((10000.0 ** (-np.arange(0, hd, 2) / hd)).astype(np.float32))
    bf, f32 = jnp.bfloat16, jnp.float32
    hbm = pl.BlockSpec(memory_space=pl.ANY)
    vm = pl.BlockSpec(memory_space=pltpu.VMEM)
    dma = pltpu.SemaphoreType.DMA
    flops = 2 * seq * d * (3 * hd + 2 * ff) + 2 * seq * seq * hd + 2 * seq * d * (hd + ff)
    return pl.pallas_call(
        layer_kernel,
        out_shape=(pltpu.VMEM((seq, d), bf), jax.ShapeDtypeStruct((COL, hd + ff, cols), bf)),
        in_specs=[hbm, vm, vm] + [hbm] * 8,
        out_specs=(vm, hbm),
        scratch_shapes=[
            pltpu.VMEM((n_chunk, d // depth, TPA, TPA, depth // TPA // TPA, hd), bf),
            pltpu.VMEM((seq, hd), bf),
            pltpu.VMEM((2, TPA, TPA, seq // TPA // TPA, hd), bf),
            pltpu.VMEM((seq, hd // 2), f32),
            pltpu.VMEM((seq, hd // 2), f32),
            pltpu.VMEM((1, d), f32),
            pltpu.VMEM((X_SLOTS, LN_ROWS, d), bf),
            pltpu.VMEM((QB, seq), f32),
            pltpu.VMEM((seq, hd + ff), bf),
            pltpu.VMEM((2, hd + ff, cols), bf),
            dma((n_chunk, 8)),
            dma((n_chunk, 8)),
            dma((8,)),
            dma((8,)),
            dma((n_chunk, 2)),
            dma,
            dma((X_SLOTS,)),
            dma((16, 4)),
            dma((16, 4)),
            dma((COL, 2, 2, 8)),
            dma((COL, 2, 2, 8)),
            dma((8, 2)),
            dma((8, 2)),
            dma((4,)),
            pltpu.SemaphoreType.REGULAR,
        ],
        compiler_params=pltpu.CompilerParams(collective_id=0, has_side_effects=True, vmem_limit_bytes=VMEM_LIMIT),
        cost_estimate=pl.CostEstimate(flops=flops, bytes_accessed=4 * seq * d, transcendentals=0),
        name="decoder_layer",
    )(x, positions.reshape(seq // 128, 128), inv_freq.reshape(1, hd // 2), norm_gain.reshape(1, depth),
      *(w.reshape(TPA, TPA, depth // TPA // TPA, w.shape[1]) for w in (w_query, w_key, w_value, w_gate, w_up)), w_out, w_down)


def write_kernel(src, dst, sem):
    parts = sem.shape[0]
    rows = src.shape[0] // parts
    copies = [pltpu.make_async_copy(src.at[pl.ds(b * rows, rows)], dst.at[pl.ds(b * rows, rows)], sem.at[b]) for b in range(parts)]
    for c in copies:
        c.start()
    for c in copies:
        c.wait()


def write_out(block):
    return pl.pallas_call(
        write_kernel,
        out_shape=jax.ShapeDtypeStruct(block.shape, block.dtype),
        in_specs=[pl.BlockSpec(memory_space=pltpu.VMEM)],
        out_specs=pl.BlockSpec(memory_space=pl.ANY),
        scratch_shapes=[pltpu.SemaphoreType.DMA((8,))],
        compiler_params=pltpu.CompilerParams(vmem_limit_bytes=24 * 1024 * 1024),
        name="write_out",
    )(block)


def solution(mesh):
    row_spec = P(("dp", "fsdp"), None, None)

    def local_layer(hidden, positions, norm_gain, w_query, w_key, w_value, w_gate, w_up, w_out, w_down):
        rows, _ = layer_call(hidden[0], positions, norm_gain, w_query, w_key, w_value, w_gate, w_up, w_out, w_down)
        return write_out(rows)[None]

    in_specs = (row_spec, P(None), P("fsdp"), P("fsdp", "tp"), P("fsdp", None), P("fsdp", None), P("fsdp", "tp"), P("fsdp", "tp"), P("tp", "fsdp"), P("tp", "fsdp"))
    return jax.shard_map(local_layer, mesh=mesh, in_specs=in_specs, out_specs=row_spec, check_vma=False)
```

```python
import jax
import jax.numpy as jnp
import numpy as np
from jax import lax
from jax.experimental import pallas as pl
from jax.experimental.pallas import tpu as pltpu
from jax.sharding import PartitionSpec as P

NORM_EPS = 1e-6
MESH = pl.DeviceIdType.MESH
TPA = 4
COL = 8


def _ring_ids(t):
    z, y = t // TPA, t % TPA
    y_r, y_l = z * TPA + (y + 1) % TPA, z * TPA + (y + 3) % TPA
    z_r, z_l = ((z + 1) % TPA) * TPA + y, ((z + 3) % TPA) * TPA + y
    return (y, y_r, y_l), (z, z_r, z_l)


def _fsdp_ids(f):
    xc, core = f // 2, f % 2
    f_p = xc * 2 + (1 - core)
    f_r = ((xc + 1) % 4) * 2 + core
    f_l = ((xc + 3) % 4) * 2 + core
    return xc, core, f_p, f_r, f_l


QB = 256
LN_ROWS = 128
X_SLOTS = 3
LN_SUB = 64
GU = 128
M1 = 1024
M2 = 512
VMEM_LIMIT = 95 * 512 * 1024


def project_part(x_hbm, pos, inv_freq, gain, wq, wk, wv, wg, wu, az, wbuf, h, q, kv, cos_t, sin_t, gbuf, xb, scores,
                 ssem, rsem, gss, grs, lsem, gsem, xsem, kss, krs, send_late):
    f = lax.axis_index("fsdp")
    nf = lax.axis_size("fsdp")
    t = lax.axis_index("tp")
    nt = lax.axis_size("tp")
    ring_y, ring_z = _ring_ids(t)
    z_id, y_id = ring_z[0], ring_y[0]
    xc, core, f_p, f_r, f_l = _fsdp_ids(f)
    f_o = ((xc + 2) % 4) * 2 + core
    seq, d = h.shape
    depth = gain.shape[1]
    hd = wq.shape[3]
    n_chunk = wbuf.shape[0]
    n_ff = wg.shape[3] // GU
    n_x = n_ff + 1

    def half_of(i, dev, part):
        return wbuf.at[i, dev, pl.ds(part * (TPA // 2), TPA // 2)]

    def load(i, part, src, col):
        return pltpu.make_async_copy(src.at[:, :, :, pl.ds(col, GU)], wbuf.at[i, f, :, :, :, pl.ds(part * GU, GU)], lsem.at[i, part])

    ld_kv = [pltpu.make_async_copy(w.at[z_id, y_id], wbuf.at[1 + i, f, z_id, y_id], lsem.at[1 + i, 0]) for i, w in enumerate((wk, wv))]
    for c in ld_kv:
        c.start()
    for part in range(2):
        load(0, part, wq, part * GU).start()
    for j in range(n_ff):
        load(3 + j, 0, wg, j * GU).start()
        load(3 + j, 1, wu, j * GU).start()

    def load_x(blk):
        slot = blk % X_SLOTS
        return pltpu.make_async_copy(x_hbm.at[pl.ds(pl.multiple_of(blk * LN_ROWS, LN_ROWS), LN_ROWS), :], xb.at[slot], xsem.at[slot])

    for blk in range(X_SLOTS - 1):
        load_x(blk).start()
    ld_g = pltpu.make_async_copy(gain, gbuf.at[:, pl.ds(pl.multiple_of(f * depth, depth), depth)], gsem)
    ld_g.start()

    barrier = pltpu.get_barrier_semaphore()
    for e in range(1, nf):
        pl.semaphore_signal(barrier, inc=1, device_id={"fsdp": (f + e) % nf}, device_id_type=MESH)
    for other in (ring_y[1], ring_y[2], ring_z[1], ring_z[2]):
        pl.semaphore_signal(barrier, inc=1, device_id={"tp": other}, device_id_type=MESH)
    pl.semaphore_wait(barrier, nf - 1 + 4)

    def rcopy(i, s, src, dev):
        return pltpu.make_async_remote_copy(src_ref=src, dst_ref=src, send_sem=ssem.at[i, s], recv_sem=rsem.at[i, s],
                                            device_id={"fsdp": dev}, device_id_type=MESH)

    def transfer(i, s):
        src, dev = (
            (lambda: wbuf.at[i, f], f_r),
            (lambda: wbuf.at[i, f], f_l),
            (lambda: wbuf.at[i, f], f_p),
            (lambda: half_of(i, f_l, 0), f_r),
            (lambda: half_of(i, f_r, 1), f_l),
            (lambda: wbuf.at[i, f_l], f_p),
            (lambda: wbuf.at[i, f_r], f_p),
            (lambda: wbuf.at[i, f_o], f_p),
        )[s]
        return rcopy(i, s, src(), dev)

    def chunk_of(xi):
        return xi + 2 * ((xi + n_x - 1) // n_x)

    kv_rings = ((ring_y, ring_z), (ring_z, ring_y))

    def ids_of(i, dev):
        return (z_id, dev) if i == 0 else (dev, y_id)

    def w_view(i, line, dev, part):
        lo, n = ((0, nf), (0, nf // 2), (nf // 2, nf // 2))[part]
        if not line:
            z, y = ids_of(i, dev)
            return wbuf.at[1 + i, pl.ds(lo, n), z, y]
        return wbuf.at[1 + i, pl.ds(lo, n), dev] if i == 0 else wbuf.at[1 + i, pl.ds(lo, n), :, dev]

    def o_view(i, line, dev, part):
        size = TPA if line else kv.shape[3]
        lo, n = ((0, size), (0, size // 2), (size // 2, size // 2))[part]
        if not line:
            z, y = ids_of(i, dev)
            return kv.at[i, z, y, pl.ds(lo, n)]
        return kv.at[i, dev, pl.ds(lo, n)] if i == 0 else kv.at[i, pl.ds(lo, n), dev]

    def kv_copies(step):
        res = []
        view = w_view if step < 4 else o_view
        for i in range(2):
            me, r, l = kv_rings[i][step // 2 % 2]
            line = step // 2 % 2 == 1
            if step % 2 == 0:
                src = (view(i, line, me, 0), view(i, line, me, 0))
            else:
                src = (view(i, line, (me + TPA - 1) % TPA, 1), view(i, line, (me + 1) % TPA, 2))
            for d_, (part, dev) in enumerate(zip(src, (r, l))):
                res.append(pltpu.make_async_remote_copy(src_ref=part, dst_ref=part, send_sem=kss.at[nf + step, 2 * i + d_], recv_sem=krs.at[nf + step, 2 * i + d_],
                                                        device_id={"tp": dev}, device_id_type=MESH))
        return res

    def kv_start(step):
        for c in kv_copies(step):
            c.start()

    def kv_finish(step):
        for c in kv_copies(step):
            c.wait_recv()
            c.wait_send()

    def send_own(i):
        for part in range(2):
            load(i, part, wq, part * GU).wait()
        for s in range(3):
            transfer(i, s).start()

    def net_a(xi):
        i = chunk_of(xi)
        transfer(i, 0).wait_recv()
        transfer(i, 3).start()
        transfer(i, 1).wait_recv()
        transfer(i, 4).start()

        @pl.when(xi + 2 < n_x)
        def _():
            send_own(chunk_of(xi + 2))

        @pl.when(xi + 1 == n_x)
        def _():
            send_late()

        transfer(i, 5).start()
        transfer(i, 6).start()

    def net_b(xi):
        i = chunk_of(xi)
        transfer(i, 3).wait_recv()
        transfer(i, 4).wait_recv()
        transfer(i, 7).start()

    def ready(i):
        for s in (2, 5, 6, 7):
            transfer(i, s).wait_recv()
        for s in range(8):
            transfer(i, s).wait_send()

    ld_g.wait()
    gcol = gbuf.at[:, pl.ds(pl.multiple_of(f * depth, depth), depth)]
    gcopies = [pltpu.make_async_remote_copy(src_ref=gcol, dst_ref=gcol, send_sem=gss.at[e], recv_sem=grs.at[e],
                                            device_id={"fsdp": (f + e) % nf}, device_id_type=MESH) for e in range(1, nf)]
    for c in gcopies:
        c.start()
    kv_x = []
    for i in range(2):
        ld_kv[i].wait()
        for e in range(1, nf):
            part = wbuf.at[1 + i, f, z_id, y_id]
            kv_x.append(pltpu.make_async_remote_copy(src_ref=part, dst_ref=part, send_sem=kss.at[e, i], recv_sem=krs.at[e, i],
                                                     device_id={"fsdp": (f + e) % nf}, device_id_type=MESH))
    for c in kv_x:
        c.start()
    send_own(0)
    send_own(3)

    lanes = pos.shape[1]
    eye = lax.broadcasted_iota(jnp.int32, (lanes, lanes), 0) == lax.broadcasted_iota(jnp.int32, (lanes, lanes), 1)

    @pl.loop(0, seq // lanes)
    def _(b):
        rows = pl.ds(pl.multiple_of(b * lanes, lanes), lanes)
        line = pos[pl.ds(b, 1), :].astype(jnp.float32)
        column = jnp.sum(jnp.where(eye, line, 0.0), axis=-1, keepdims=True)
        angle = column * inv_freq[...]
        cos_t[rows, :] = jnp.cos(angle)
        sin_t[rows, :] = jnp.sin(angle)

    for c in gcopies:
        c.wait()
    for c in kv_x:
        c.wait()
    kv_start(0)

    n_blk = seq // LN_ROWS

    def norm_blocks(lo, hi):
        @pl.loop(lo, hi)
        def _(blk):
            load_x(blk).wait()

            @pl.when(blk + X_SLOTS - 1 < n_blk)
            def _():
                load_x(blk + X_SLOTS - 1).start()

            @pl.loop(0, LN_ROWS // LN_SUB)
            def _(r):
                row = xb[blk % X_SLOTS, pl.ds(pl.multiple_of(r * LN_SUB, LN_SUB), LN_SUB), :].astype(jnp.float32)
                centered = row - jnp.sum(row, axis=-1, keepdims=True) * (1.0 / d)
                var = jnp.sum(centered * centered, axis=-1, keepdims=True) * (1.0 / d)
                out = centered * lax.rsqrt(var + NORM_EPS) * gbuf[...]
                h[pl.ds(pl.multiple_of(blk * LN_ROWS + r * LN_SUB, LN_SUB), LN_SUB), :] = out.astype(jnp.bfloat16)

    norm_blocks(0, n_blk // 4)
    kv_finish(0)
    kv_start(1)
    norm_blocks(n_blk // 4, n_blk // 2)
    net_a(0)
    kv_finish(1)
    kv_start(2)
    norm_blocks(n_blk // 2, n_blk)

    def product(i, rows):
        return jnp.dot(h[rows, :], wbuf[i].reshape(d, hd), preferred_element_type=jnp.float32)

    def rope(y, rows):
        a, b = y[:, :hd // 2].astype(jnp.bfloat16).astype(jnp.float32), y[:, hd // 2:].astype(jnp.bfloat16).astype(jnp.float32)
        c, s = cos_t[rows, :], sin_t[rows, :]
        return jnp.concatenate([a * c - b * s, b * c + a * s], axis=1).astype(jnp.bfloat16)

    def keys_values():
        n = kv.shape[3]
        rows = pl.ds(pl.multiple_of(t * n, n), n)
        kv[0, z_id, y_id] = rope(product(1, rows), rows)
        kv[1, z_id, y_id] = product(2, rows).astype(jnp.bfloat16)

    def compute(i):
        @pl.when(i == 0)
        def _():
            @pl.loop(0, seq // M1)
            def _(m):
                rows = pl.ds(pl.multiple_of(m * M1, M1), M1)
                q[rows, :] = rope(product(i, rows), rows)

        @pl.when(i >= 3)
        def _():
            for m in range(seq // M2):
                rows = pl.ds(m * M2, M2)
                y = product(i, rows)
                g = y[:, :GU].astype(jnp.bfloat16).astype(jnp.float32)
                u = y[:, GU:].astype(jnp.bfloat16).astype(jnp.float32)
                z = (g * (1.0 / (1.0 + jnp.exp(-g)))) * u
                az[rows, pl.ds(pl.multiple_of(hd + (i - 3) * GU, GU), GU)] = z.astype(jnp.bfloat16)

    scale = hd ** -0.5
    n_q = seq // QB

    keys, values = (kv.at[i].reshape(seq, hd) for i in range(2))

    def attend(b):
        rows = pl.ds(b * QB, QB)
        qb = q[rows, :]
        peak = None
        for t in range(b + 1):
            s = lax.dot_general(qb, keys[pl.ds(t * QB, QB), :], (((1,), (1,)), ((), ())), preferred_element_type=jnp.float32) * scale
            if t == b:
                keep = lax.broadcasted_iota(jnp.int32, (QB, QB), 1) <= lax.broadcasted_iota(jnp.int32, (QB, QB), 0)
                s = jnp.where(keep, s, -1e30)
            scores[:, t * QB:(t + 1) * QB] = s
            s = jnp.maximum(s[:, :128], s[:, 128:])
            peak = s if peak is None else jnp.maximum(peak, s)
        peak = jnp.max(peak, axis=-1, keepdims=True)
        total = None
        for t in range(b + 1):
            e = jnp.exp(scores[:, t * QB:(t + 1) * QB] - peak)
            scores[:, t * QB:(t + 1) * QB] = e
            e = e[:, :128] + e[:, 128:]
            total = e if total is None else total + e
        inv = 1.0 / jnp.sum(total, axis=-1, keepdims=True)
        p = (scores[:, :(b + 1) * QB] * inv).astype(jnp.bfloat16)
        out = jnp.dot(p, values[pl.ds(0, (b + 1) * QB), :], preferred_element_type=jnp.float32)
        az[rows, 0:hd] = out.astype(jnp.bfloat16)

    @pl.loop(0, n_x)
    def _(j):
        @pl.when(j + 1 < n_x)
        def _():
            net_a(j + 1)

        net_b(j)

        @pl.when(j == 1)
        def _():
            kv_finish(2)
            kv_start(3)

        @pl.when(j == 2)
        def _():
            kv_finish(3)
            keys_values()
            kv_start(4)

        @pl.when(j == 3)
        def _():
            kv_finish(5)
            kv_start(6)

        @pl.when(j == 4)
        def _():
            kv_finish(7)

        for lo, hi, step in ((0, 3, 4), (3, 5, 5), (5, 7, 6), (7, 8, 7)):
            @pl.when(j == step)
            def _(lo=lo, hi=hi):
                for b in range(lo, hi):
                    attend(b)

        ready(chunk_of(j))
        compute(chunk_of(j))

        @pl.when(j == 2)
        def _():
            kv_finish(4)
            kv_start(5)

        @pl.when(j == 3)
        def _():
            kv_finish(6)
            kv_start(7)


def reduce_part(az, x_hbm, wo, wd, out, w2, wbuf, wvm, xb, ssem, rsem, wss, wrs, lsem, xsem, phase):
    t = lax.axis_index("tp")
    f = lax.axis_index("fsdp")
    ring_y, ring_z = _ring_ids(t)
    xc, core, f_p, f_r, f_l = _fsdp_ids(f)
    seq = az.shape[0]
    cols = wvm.shape[2]
    part = wbuf.at[pl.ds(0, 5)].reshape(5, 2, seq, cols // 2)
    half = seq // 2
    big = half // TPA
    small = big // TPA
    r2 = wbuf.at[pl.ds(5, 2)].reshape(LAND_SLOTS, 2, 2, 2, big, cols // 2)
    r1 = wbuf.at[pl.ds(7, 2)].reshape(COL, 2, 2, 2, big // 2, cols // 2)
    r4 = wbuf.at[9].reshape(COL, 2, 2, 2, small, cols // 2)
    r3 = wbuf.at[10, pl.ds(0, 4)].reshape(COL, 2, 2, 2, small // 2, cols // 2)
    hd = wo.shape[0]

    axes = ((ring_y, ring_z), (ring_z, ring_y))

    def own_rows(h):
        (i1, _, _), (i2, _, _) = axes[h]
        return pl.multiple_of(h * half + i1 * big + i2 * small, small)

    xrow = [xb.at[0, pl.ds(hf * small, small)] for hf in range(2)]
    ld_x = [pltpu.make_async_copy(x_hbm.at[pl.ds(own_rows(hf), small), :], xrow[hf], xsem.at[hf]) for hf in range(2)]

    def wcopy(k, e, src, dst, dev):
        return pltpu.make_async_remote_copy(src_ref=src, dst_ref=dst, send_sem=wss.at[k, e], recv_sem=wrs.at[k, e],
                                            device_id={"fsdp": dev}, device_id_type=MESH)

    kk = wvm.shape[1]
    kh = kk // 2
    rows_o, rows_d = pl.ds(0, hd), pl.ds(hd, kk - hd)

    def w_own(k, slot, dev):
        return wcopy(k, 0, wo, w2.at[slot, rows_o], dev), wcopy(k, 1, wd, w2.at[slot, rows_d], dev)

    def w_whole(k, slot):
        return wcopy(k, 0, w2.at[slot], w2.at[slot + 1], f_p)

    def w_2r():
        return wcopy(5, 0, w2.at[2, pl.ds(0, kh)], w2.at[6, pl.ds(0, kh)], f_r)

    def w_4l():
        return wcopy(6, 0, w2.at[4, pl.ds(kh, kh)], w2.at[6, pl.ds(kh, kh)], f_l)

    def load_own():
        return (pltpu.make_async_copy(wo, wvm.at[0, rows_o], lsem.at[2]), pltpu.make_async_copy(wd, wvm.at[0, rows_d], lsem.at[3]))

    def load_w(cb):
        return pltpu.make_async_copy(w2.at[cb], wvm.at[cb % 2], lsem.at[cb % 2])

    def send_late():
        for c in w_own(1, 2, f_r) + w_own(2, 4, f_l) + w_own(0, 1, f_p) + load_own():
            c.start()

    def fetch(cb):
        @pl.when(cb == 1)
        def _():
            for c in w_own(0, 1, f_p):
                c.wait()

        @pl.when(cb == 2)
        def _():
            for c in w_own(1, 2, f_r) + w_own(2, 4, f_l):
                c.wait()
            w_2r().start()
            w_4l().start()
            w_whole(3, 2).start()
            w_whole(4, 4).start()

        @pl.when(cb == 3)
        def _():
            w_whole(3, 2).wait()

        @pl.when(cb == 5)
        def _():
            w_whole(4, 4).wait()

        @pl.when(cb == 6)
        def _():
            w_2r().wait()
            w_4l().wait()
            w_whole(7, 6).start()

        @pl.when(cb == 7)
        def _():
            w_whole(7, 6).wait()

        load_w(cb).start()

    def block_of(k):
        q = k // 2
        dx = 3 * q - 5 * (q // 2) - 2 * (q // 3)
        return ((xc + dx) % 4) * 2 + (core + k % 2) % 2

    def block_cols(cb):
        return pl.ds(pl.multiple_of(block_of(cb) * cols, cols), cols)

    def ring_copy(cb, h, d, step, src, dst, dev):
        return pltpu.make_async_remote_copy(src_ref=src, dst_ref=dst, send_sem=ssem.at[cb, h, d, step],
                                            recv_sem=rsem.at[cb, h, d, step], device_id={"tp": dev}, device_id_type=MESH)

    def rs_first(cb, h, step, ring, base, n, land):
        i, r, l = ring
        o = (i + 2) % TPA
        m = n // 2
        s = pl.multiple_of(base + o * n, m)
        return (ring_copy(cb, h, 0, step, part.at[cb % PART_SLOTS, :, pl.ds(s, m)], land.at[cb % land.shape[0], h, 0], r),
                ring_copy(cb, h, 1, step, part.at[cb % PART_SLOTS, :, pl.ds(s + m, m)], land.at[cb % land.shape[0], h, 1], l))

    def rs_second(cb, h, step, ring, base, n, land):
        i, r, l = ring
        s_r = pl.multiple_of(base + ((i + 1) % TPA) * n, n)
        s_l = pl.multiple_of(base + ((i + 3) % TPA) * n, n)
        return (ring_copy(cb, h, 0, step, part.at[cb % PART_SLOTS, :, pl.ds(s_r, n)], land.at[cb % land.shape[0], h, 0], r),
                ring_copy(cb, h, 1, step, part.at[cb % PART_SLOTS, :, pl.ds(s_l, n)], land.at[cb % land.shape[0], h, 1], l))

    def rs_update(cb, h, ring, base, n, land):
        i, _, _ = ring
        m = n // 2
        s_r = pl.multiple_of(base + ((i + 1) % TPA) * n, m)
        s_l = pl.multiple_of(base + ((i + 3) % TPA) * n + m, m)
        for s, d in ((s_r, 0), (s_l, 1)):
            rows = pl.ds(s, m)
            part[cb % PART_SLOTS, :, rows] = (part[cb % PART_SLOTS, :, rows].astype(jnp.float32) + land[cb % land.shape[0], h, d].astype(jnp.float32)).astype(jnp.bfloat16)

    def ag_first(cb, h, step, ring, src, base, n):
        i, r, l = ring
        dst = out.at[pl.ds(pl.multiple_of(base + i * n, n), n), block_cols(cb)]
        if src is None:
            src = dst
        return (ring_copy(cb, h, 0, step, src, dst, r), ring_copy(cb, h, 1, step, src, dst, l))

    def ag_second(cb, h, step, ring, base, n):
        i, r, l = ring
        m = n // 2
        from_l = out.at[pl.ds(pl.multiple_of(base + ((i + 3) % TPA) * n, m), m), block_cols(cb)]
        from_r = out.at[pl.ds(pl.multiple_of(base + ((i + 1) % TPA) * n + m, m), m), block_cols(cb)]
        return (ring_copy(cb, h, 0, step, from_l, from_l, r), ring_copy(cb, h, 1, step, from_r, from_r, l))

    def copies(cb, step):
        res = []
        for h in range(2):
            ring1, ring2 = axes[h]
            base1 = h * half
            base2 = pl.multiple_of(h * half + ring1[0] * big, big)
            if step == 0:
                res.extend(rs_first(cb, h, step, ring1, base1, big, r1))
            elif step == 1:
                res.extend(rs_second(cb, h, step, ring1, base1, big, r2))
            elif step == 2:
                res.extend(rs_first(cb, h, step, ring2, base2, small, r3))
            elif step == 3:
                res.extend(rs_second(cb, h, step, ring2, base2, small, r4))
            elif step == 4:
                res.extend(ag_first(cb, h, step, ring2, None, base2, small))
            elif step == 5:
                res.extend(ag_second(cb, h, step, ring2, base2, small))
            elif step == 6:
                res.extend(ag_first(cb, h, step, ring1, None, base1, big))
            else:
                res.extend(ag_second(cb, h, step, ring1, base1, big))
        return res

    def start(cb, step):
        for c in copies(cb, step):
            c.start()

    def finish(cb, step):
        for c in copies(cb, step):
            c.wait_recv()
            c.wait_send()

    def stage0(cb):
        @pl.when(cb == 0)
        def _():
            for c in load_own():
                c.wait()

        @pl.when(cb > 0)
        def _():
            load_w(cb).wait()

        @pl.loop(0, seq // MT)
        def _(i):
            rows = pl.ds(pl.multiple_of(i * MT, MT), MT)
            y = jnp.dot(az[rows, :], wvm[cb % 2], preferred_element_type=jnp.float32).astype(jnp.bfloat16)
            for hf in range(2):
                part[cb % PART_SLOTS, hf, rows] = y[:, hf * (cols // 2):(hf + 1) * (cols // 2)]

        @pl.when(cb == 0)
        def _():
            pl.semaphore_wait(phase, 4)

        start(cb, 0)

    def stage1(cb):
        finish(cb, 0)
        for h in range(2):
            rs_update(cb, h, axes[h][0], h * half, big, r1)
        start(cb, 1)

    def stage2(cb):
        finish(cb, 1)
        for h in range(2):
            rows = pl.ds(pl.multiple_of(h * half + axes[h][0][0] * big, big), big)
            part[cb % PART_SLOTS, :, rows] = (part[cb % PART_SLOTS, :, rows].astype(jnp.float32) + r2[cb % r2.shape[0], h, 0].astype(jnp.float32)
                              + r2[cb % r2.shape[0], h, 1].astype(jnp.float32)).astype(jnp.bfloat16)
        start(cb, 2)

    def stage3(cb):
        finish(cb, 2)
        for h in range(2):
            rs_update(cb, h, axes[h][1], pl.multiple_of(h * half + axes[h][0][0] * big, big), small, r3)
        start(cb, 3)

    def stage4(cb):
        finish(cb, 3)
        g = block_of(cb)
        for h in range(2):
            branch = (part[cb % PART_SLOTS, :, pl.ds(own_rows(h), small)].astype(jnp.float32) + r4[cb % r4.shape[0], h, 0].astype(jnp.float32)
                      + r4[cb % r4.shape[0], h, 1].astype(jnp.float32))
            for hf in range(2):
                lanes = pl.ds(pl.multiple_of(g * cols + hf * (cols // 2), cols // 2), cols // 2)
                xs = xb[0, pl.ds(h * small, small), lanes].astype(jnp.float32)
                out[pl.ds(own_rows(h), small), lanes] = (xs + branch[hf]).astype(jnp.bfloat16)
        start(cb, 4)

    def stage5(cb):
        finish(cb, 4)
        start(cb, 5)

    def stage6(cb):
        finish(cb, 5)
        start(cb, 6)

    def stage7(cb):
        finish(cb, 6)
        start(cb, 7)

    def stage8(cb):
        finish(cb, 7)

    stages = (stage0, stage1, stage2, stage3, stage4, stage5, stage6, stage7, stage8)

    def reduce_all():
        for c in ld_x:
            c.start()
        for other in (ring_y[1], ring_y[2], ring_z[1], ring_z[2]):
            pl.semaphore_signal(phase, inc=1, device_id={"tp": other}, device_id_type=MESH)
        for c in ld_x:
            c.wait()

        @pl.loop(0, COL + GAP + len(stages) - 1)
        def _(n):
            for s, fn in enumerate(stages):
                turn = n - s

                @pl.when(jnp.logical_or(jnp.logical_and(turn >= 0, turn < 2), jnp.logical_and(turn >= 2 + GAP, turn < COL + GAP)))
                def _(fn=fn, turn=turn):
                    fn(jnp.where(turn >= 2, turn - GAP, turn))

            @pl.when(jnp.logical_or(n < 1, jnp.logical_and(n >= 1 + GAP, n + 1 < COL + GAP)))
            def _():
                fetch(jnp.where(n >= 1, n - GAP, n) + 1)

    return send_late, reduce_all


MT = 512
GAP = 1
PART_SLOTS = 5
LAND_SLOTS = 4


def layer_kernel(x_hbm, pos, inv_freq, gain, wq, wk, wv, wg, wu, wo, wd, out, w2, wbuf, q, kv, cos_t, sin_t, gbuf, xb, scores, az, wvm,
                 ssem, rsem, gss, grs, lsem, gsem, xsem, kss, krs, rss, rrs, wss, wrs, wlsem, phase):
    send_late, reduce_all = reduce_part(az, x_hbm, wo, wd, out, w2, wbuf, wvm, xb, rss, rrs, wss, wrs, wlsem, xsem, phase)
    project_part(x_hbm, pos, inv_freq, gain, wq, wk, wv, wg, wu, az, wbuf, out, q, kv, cos_t, sin_t, gbuf, xb, scores,
                 ssem, rsem, gss, grs, lsem, gsem, xsem, kss, krs, send_late)
    reduce_all()


def layer_call(x, positions, norm_gain, w_query, w_key, w_value, w_gate, w_up, w_out, w_down):
    seq, d = x.shape
    depth, hd = w_query.shape
    ff = w_gate.shape[1]
    n_chunk = 3 + ff // GU
    cols = d // COL
    inv_freq = jnp.asarray((10000.0 ** (-np.arange(0, hd, 2) / hd)).astype(np.float32))
    bf, f32 = jnp.bfloat16, jnp.float32
    hbm = pl.BlockSpec(memory_space=pl.ANY)
    vm = pl.BlockSpec(memory_space=pltpu.VMEM)
    dma = pltpu.SemaphoreType.DMA
    flops = 2 * seq * d * (3 * hd + 2 * ff) + 2 * seq * seq * hd + 2 * seq * d * (hd + ff)
    return pl.pallas_call(
        layer_kernel,
        out_shape=(pltpu.VMEM((seq, d), bf), jax.ShapeDtypeStruct((COL, hd + ff, cols), bf)),
        in_specs=[hbm, vm, vm] + [hbm] * 8,
        out_specs=(vm, hbm),
        scratch_shapes=[
            pltpu.VMEM((n_chunk, d // depth, TPA, TPA, depth // TPA // TPA, hd), bf),
            pltpu.VMEM((seq, hd), bf),
            pltpu.VMEM((2, TPA, TPA, seq // TPA // TPA, hd), bf),
            pltpu.VMEM((seq, hd // 2), f32),
            pltpu.VMEM((seq, hd // 2), f32),
            pltpu.VMEM((1, d), f32),
            pltpu.VMEM((X_SLOTS, LN_ROWS, d), bf),
            pltpu.VMEM((QB, seq), f32),
            pltpu.VMEM((seq, hd + ff), bf),
            pltpu.VMEM((2, hd + ff, cols), bf),
            dma((n_chunk, 8)),
            dma((n_chunk, 8)),
            dma((8,)),
            dma((8,)),
            dma((n_chunk, 2)),
            dma,
            dma((X_SLOTS,)),
            dma((16, 4)),
            dma((16, 4)),
            dma((COL, 2, 2, 8)),
            dma((COL, 2, 2, 8)),
            dma((8, 2)),
            dma((8, 2)),
            dma((4,)),
            pltpu.SemaphoreType.REGULAR,
        ],
        compiler_params=pltpu.CompilerParams(collective_id=0, has_side_effects=True, vmem_limit_bytes=VMEM_LIMIT),
        cost_estimate=pl.CostEstimate(flops=flops, bytes_accessed=4 * seq * d, transcendentals=0),
        name="decoder_layer",
    )(x, positions.reshape(seq // 128, 128), inv_freq.reshape(1, hd // 2), norm_gain.reshape(1, depth),
      *(w.reshape(TPA, TPA, depth // TPA // TPA, w.shape[1]) for w in (w_query, w_key, w_value, w_gate, w_up)), w_out, w_down)


def write_kernel(src, dst, sem):
    parts = sem.shape[0]
    rows = src.shape[0] // parts
    copies = [pltpu.make_async_copy(src.at[pl.ds(b * rows, rows)], dst.at[pl.ds(b * rows, rows)], sem.at[b]) for b in range(parts)]
    for c in copies:
        c.start()
    for c in copies:
        c.wait()


def write_out(block):
    return pl.pallas_call(
        write_kernel,
        out_shape=jax.ShapeDtypeStruct(block.shape, block.dtype),
        in_specs=[pl.BlockSpec(memory_space=pltpu.VMEM)],
        out_specs=pl.BlockSpec(memory_space=pl.ANY),
        scratch_shapes=[pltpu.SemaphoreType.DMA((8,))],
        compiler_params=pltpu.CompilerParams(vmem_limit_bytes=24 * 1024 * 1024),
        name="write_out",
    )(block)


def solution(mesh):
    row_spec = P(("dp", "fsdp"), None, None)

    def local_layer(hidden, positions, norm_gain, w_query, w_key, w_value, w_gate, w_up, w_out, w_down):
        rows, _ = layer_call(hidden[0], positions, norm_gain, w_query, w_key, w_value, w_gate, w_up, w_out, w_down)
        return write_out(rows)[None]

    in_specs = (row_spec, P(None), P("fsdp"), P("fsdp", "tp"), P("fsdp", None), P("fsdp", None), P("fsdp", "tp"), P("fsdp", "tp"), P("tp", "fsdp"), P("tp", "fsdp"))
    return jax.shard_map(local_layer, mesh=mesh, in_specs=in_specs, out_specs=row_spec, check_vma=False)
```

```python
import jax
import jax.numpy as jnp
import numpy as np
from jax import lax
from jax.experimental import pallas as pl
from jax.experimental.pallas import tpu as pltpu
from jax.sharding import PartitionSpec as P

NORM_EPS = 1e-6
MESH = pl.DeviceIdType.MESH
TPA = 4
COL = 8


def _ring_ids(t):
    z, y = t // TPA, t % TPA
    y_r, y_l = z * TPA + (y + 1) % TPA, z * TPA + (y + 3) % TPA
    z_r, z_l = ((z + 1) % TPA) * TPA + y, ((z + 3) % TPA) * TPA + y
    return (y, y_r, y_l), (z, z_r, z_l)


def _fsdp_ids(f):
    xc, core = f // 2, f % 2
    f_p = xc * 2 + (1 - core)
    f_r = ((xc + 1) % 4) * 2 + core
    f_l = ((xc + 3) % 4) * 2 + core
    return xc, core, f_p, f_r, f_l


QB = 256
LN_ROWS = 128
X_SLOTS = 3
LN_SUB = 64
GU = 128
M1 = 1024
M2 = 512
VMEM_LIMIT = 95 * 512 * 1024


def project_part(x_hbm, pos, inv_freq, gain, wq, wk, wv, wg, wu, az, wbuf, h, q, kv, cos_t, sin_t, gbuf, xb, scores,
                 ssem, rsem, gss, grs, lsem, gsem, xsem, kss, krs, send_late):
    f = lax.axis_index("fsdp")
    nf = lax.axis_size("fsdp")
    t = lax.axis_index("tp")
    nt = lax.axis_size("tp")
    ring_y, ring_z = _ring_ids(t)
    z_id, y_id = ring_z[0], ring_y[0]
    xc, core, f_p, f_r, f_l = _fsdp_ids(f)
    f_o = ((xc + 2) % 4) * 2 + core
    seq, d = h.shape
    depth = gain.shape[1]
    hd = wq.shape[3]
    n_chunk = wbuf.shape[0]
    n_ff = wg.shape[3] // GU
    n_x = n_ff + 1

    def half_of(i, dev, part):
        return wbuf.at[i, dev, pl.ds(part * (TPA // 2), TPA // 2)]

    def load(i, part, src, col):
        return pltpu.make_async_copy(src.at[:, :, :, pl.ds(col, GU)], wbuf.at[i, f, :, :, :, pl.ds(part * GU, GU)], lsem.at[i, part])

    ld_kv = [pltpu.make_async_copy(w.at[z_id, y_id], wbuf.at[1 + i, f, z_id, y_id], lsem.at[1 + i, 0]) for i, w in enumerate((wk, wv))]
    for c in ld_kv:
        c.start()
    for part in range(2):
        load(0, part, wq, part * GU).start()
    for j in range(n_ff):
        load(3 + j, 0, wg, j * GU).start()
        load(3 + j, 1, wu, j * GU).start()

    def load_x(blk):
        slot = blk % X_SLOTS
        return pltpu.make_async_copy(x_hbm.at[pl.ds(pl.multiple_of(blk * LN_ROWS, LN_ROWS), LN_ROWS), :], xb.at[slot], xsem.at[slot])

    for blk in range(X_SLOTS - 1):
        load_x(blk).start()
    ld_g = pltpu.make_async_copy(gain, gbuf.at[:, pl.ds(pl.multiple_of(f * depth, depth), depth)], gsem)
    ld_g.start()

    barrier = pltpu.get_barrier_semaphore()
    for e in range(1, nf):
        pl.semaphore_signal(barrier, inc=1, device_id={"fsdp": (f + e) % nf}, device_id_type=MESH)
    for other in (ring_y[1], ring_y[2], ring_z[1], ring_z[2]):
        pl.semaphore_signal(barrier, inc=1, device_id={"tp": other}, device_id_type=MESH)
    pl.semaphore_wait(barrier, nf - 1 + 4)

    def rcopy(i, s, src, dev):
        return pltpu.make_async_remote_copy(src_ref=src, dst_ref=src, send_sem=ssem.at[i, s], recv_sem=rsem.at[i, s],
                                            device_id={"fsdp": dev}, device_id_type=MESH)

    def transfer(i, s):
        src, dev = (
            (lambda: wbuf.at[i, f], f_r),
            (lambda: wbuf.at[i, f], f_l),
            (lambda: wbuf.at[i, f], f_p),
            (lambda: half_of(i, f_l, 0), f_r),
            (lambda: half_of(i, f_r, 1), f_l),
            (lambda: wbuf.at[i, f_l], f_p),
            (lambda: wbuf.at[i, f_r], f_p),
            (lambda: wbuf.at[i, f_o], f_p),
        )[s]
        return rcopy(i, s, src(), dev)

    def chunk_of(xi):
        return xi + 2 * ((xi + n_x - 1) // n_x)

    kv_rings = ((ring_y, ring_z), (ring_z, ring_y))

    def ids_of(i, dev):
        return (z_id, dev) if i == 0 else (dev, y_id)

    def w_view(i, line, dev, part):
        lo, n = ((0, nf), (0, nf // 2), (nf // 2, nf // 2))[part]
        if not line:
            z, y = ids_of(i, dev)
            return wbuf.at[1 + i, pl.ds(lo, n), z, y]
        return wbuf.at[1 + i, pl.ds(lo, n), dev] if i == 0 else wbuf.at[1 + i, pl.ds(lo, n), :, dev]

    def o_view(i, line, dev, part):
        size = TPA if line else kv.shape[3]
        lo, n = ((0, size), (0, size // 2), (size // 2, size // 2))[part]
        if not line:
            z, y = ids_of(i, dev)
            return kv.at[i, z, y, pl.ds(lo, n)]
        return kv.at[i, dev, pl.ds(lo, n)] if i == 0 else kv.at[i, pl.ds(lo, n), dev]

    def kv_copies(step):
        res = []
        view = w_view if step < 4 else o_view
        for i in range(2):
            me, r, l = kv_rings[i][step // 2 % 2]
            line = step // 2 % 2 == 1
            if step % 2 == 0:
                src = (view(i, line, me, 0), view(i, line, me, 0))
            else:
                src = (view(i, line, (me + TPA - 1) % TPA, 1), view(i, line, (me + 1) % TPA, 2))
            for d_, (part, dev) in enumerate(zip(src, (r, l))):
                res.append(pltpu.make_async_remote_copy(src_ref=part, dst_ref=part, send_sem=kss.at[nf + step, 2 * i + d_], recv_sem=krs.at[nf + step, 2 * i + d_],
                                                        device_id={"tp": dev}, device_id_type=MESH))
        return res

    def kv_start(step):
        for c in kv_copies(step):
            c.start()

    def kv_finish(step):
        for c in kv_copies(step):
            c.wait_recv()
            c.wait_send()

    def send_own(i):
        for part in range(2):
            load(i, part, wq, part * GU).wait()
        for s in range(3):
            transfer(i, s).start()

    def net_a(xi):
        i = chunk_of(xi)
        transfer(i, 0).wait_recv()
        transfer(i, 3).start()
        transfer(i, 1).wait_recv()
        transfer(i, 4).start()

        @pl.when(xi + 2 < n_x)
        def _():
            send_own(chunk_of(xi + 2))

        @pl.when(xi + 1 == n_x)
        def _():
            send_late()

        transfer(i, 5).start()
        transfer(i, 6).start()

    def net_b(xi):
        i = chunk_of(xi)
        transfer(i, 3).wait_recv()
        transfer(i, 4).wait_recv()
        transfer(i, 7).start()

    def ready(i):
        for s in (2, 5, 6, 7):
            transfer(i, s).wait_recv()
        for s in range(8):
            transfer(i, s).wait_send()

    ld_g.wait()
    gcol = gbuf.at[:, pl.ds(pl.multiple_of(f * depth, depth), depth)]
    gcopies = [pltpu.make_async_remote_copy(src_ref=gcol, dst_ref=gcol, send_sem=gss.at[e], recv_sem=grs.at[e],
                                            device_id={"fsdp": (f + e) % nf}, device_id_type=MESH) for e in range(1, nf)]
    for c in gcopies:
        c.start()
    kv_x = []
    for i in range(2):
        ld_kv[i].wait()
        for e in range(1, nf):
            part = wbuf.at[1 + i, f, z_id, y_id]
            kv_x.append(pltpu.make_async_remote_copy(src_ref=part, dst_ref=part, send_sem=kss.at[e, i], recv_sem=krs.at[e, i],
                                                     device_id={"fsdp": (f + e) % nf}, device_id_type=MESH))
    for c in kv_x:
        c.start()
    send_own(0)
    send_own(3)

    lanes = pos.shape[1]
    eye = lax.broadcasted_iota(jnp.int32, (lanes, lanes), 0) == lax.broadcasted_iota(jnp.int32, (lanes, lanes), 1)

    @pl.loop(0, seq // lanes)
    def _(b):
        rows = pl.ds(pl.multiple_of(b * lanes, lanes), lanes)
        line = pos[pl.ds(b, 1), :].astype(jnp.float32)
        column = jnp.sum(jnp.where(eye, line, 0.0), axis=-1, keepdims=True)
        angle = column * inv_freq[...]
        cos_t[rows, :] = jnp.cos(angle)
        sin_t[rows, :] = jnp.sin(angle)

    for c in gcopies:
        c.wait()
    for c in kv_x:
        c.wait()
    kv_start(0)

    n_blk = seq // LN_ROWS

    def norm_blocks(lo, hi):
        @pl.loop(lo, hi)
        def _(blk):
            load_x(blk).wait()

            @pl.when(blk + X_SLOTS - 1 < n_blk)
            def _():
                load_x(blk + X_SLOTS - 1).start()

            @pl.loop(0, LN_ROWS // LN_SUB)
            def _(r):
                row = xb[blk % X_SLOTS, pl.ds(pl.multiple_of(r * LN_SUB, LN_SUB), LN_SUB), :].astype(jnp.float32)
                centered = row - jnp.sum(row, axis=-1, keepdims=True) * (1.0 / d)
                var = jnp.sum(centered * centered, axis=-1, keepdims=True) * (1.0 / d)
                out = centered * lax.rsqrt(var + NORM_EPS) * gbuf[...]
                h[pl.ds(pl.multiple_of(blk * LN_ROWS + r * LN_SUB, LN_SUB), LN_SUB), :] = out.astype(jnp.bfloat16)

    norm_blocks(0, n_blk // 4)
    kv_finish(0)
    kv_start(1)
    norm_blocks(n_blk // 4, n_blk // 2)
    net_a(0)
    kv_finish(1)
    kv_start(2)
    norm_blocks(n_blk // 2, n_blk)

    def product(i, rows):
        return jnp.dot(h[rows, :], wbuf[i].reshape(d, hd), preferred_element_type=jnp.float32)

    def rope(y, rows):
        a, b = y[:, :hd // 2].astype(jnp.bfloat16).astype(jnp.float32), y[:, hd // 2:].astype(jnp.bfloat16).astype(jnp.float32)
        c, s = cos_t[rows, :], sin_t[rows, :]
        return jnp.concatenate([a * c - b * s, b * c + a * s], axis=1).astype(jnp.bfloat16)

    def keys_values():
        n = kv.shape[3]
        rows = pl.ds(pl.multiple_of(t * n, n), n)
        kv[0, z_id, y_id] = rope(product(1, rows), rows)
        kv[1, z_id, y_id] = product(2, rows).astype(jnp.bfloat16)

    def compute(i):
        @pl.when(i == 0)
        def _():
            @pl.loop(0, seq // M1)
            def _(m):
                rows = pl.ds(pl.multiple_of(m * M1, M1), M1)
                q[rows, :] = rope(product(i, rows), rows)

    def gate_up(i, lo, hi):
        @pl.when(i >= 3)
        def _():
            for m in range(lo, hi):
                rows = pl.ds(m * M2, M2)
                y = product(i, rows)
                g = y[:, :GU].astype(jnp.bfloat16).astype(jnp.float32)
                u = y[:, GU:].astype(jnp.bfloat16).astype(jnp.float32)
                z = (g * (1.0 / (1.0 + jnp.exp(-g)))) * u
                az[rows, pl.ds(pl.multiple_of(hd + (i - 3) * GU, GU), GU)] = z.astype(jnp.bfloat16)

    scale = hd ** -0.5
    n_q = seq // QB

    keys, values = (kv.at[i].reshape(seq, hd) for i in range(2))

    def attend(b):
        rows = pl.ds(b * QB, QB)
        qb = q[rows, :]
        peak = None
        for t in range(b + 1):
            s = lax.dot_general(qb, keys[pl.ds(t * QB, QB), :], (((1,), (1,)), ((), ())), preferred_element_type=jnp.float32) * scale
            if t == b:
                keep = lax.broadcasted_iota(jnp.int32, (QB, QB), 1) <= lax.broadcasted_iota(jnp.int32, (QB, QB), 0)
                s = jnp.where(keep, s, -1e30)
            scores[:, t * QB:(t + 1) * QB] = s
            s = jnp.maximum(s[:, :128], s[:, 128:])
            peak = s if peak is None else jnp.maximum(peak, s)
        peak = jnp.max(peak, axis=-1, keepdims=True)
        total = None
        for t in range(b + 1):
            e = jnp.exp(scores[:, t * QB:(t + 1) * QB] - peak)
            scores[:, t * QB:(t + 1) * QB] = e
            e = e[:, :128] + e[:, 128:]
            total = e if total is None else total + e
        inv = 1.0 / jnp.sum(total, axis=-1, keepdims=True)
        p = (scores[:, :(b + 1) * QB] * inv).astype(jnp.bfloat16)
        out = jnp.dot(p, values[pl.ds(0, (b + 1) * QB), :], preferred_element_type=jnp.float32)
        az[rows, 0:hd] = out.astype(jnp.bfloat16)

    @pl.loop(0, n_x)
    def _(j):
        @pl.when(j + 1 < n_x)
        def _():
            net_a(j + 1)

        @pl.when(j < n_x - 1)
        def _():
            net_b(j)

        @pl.when(j == 1)
        def _():
            kv_finish(2)
            kv_start(3)

        @pl.when(j == 2)
        def _():
            kv_finish(3)
            keys_values()
            kv_start(4)

        @pl.when(j == 3)
        def _():
            kv_finish(5)
            kv_start(6)

        @pl.when(j == 4)
        def _():
            kv_finish(7)

        for lo, hi, step in ((0, 3, 4), (3, 5, 5), (5, 7, 6), (7, 8, 7)):
            @pl.when(j == step)
            def _(lo=lo, hi=hi):
                for b in range(lo, hi):
                    attend(b)

        ready(chunk_of(j))
        compute(chunk_of(j))
        n_tile = seq // M2
        gate_up(chunk_of(j), 0, n_tile - 1)

        @pl.when(j == n_x - 2)
        def _():
            net_b(n_x - 1)

        gate_up(chunk_of(j), n_tile - 1, n_tile)

        @pl.when(j == 2)
        def _():
            kv_finish(4)
            kv_start(5)

        @pl.when(j == 3)
        def _():
            kv_finish(6)
            kv_start(7)


def reduce_part(az, x_hbm, wo, wd, out, w2, wbuf, wvm, xb, ssem, rsem, wss, wrs, lsem, xsem, phase):
    t = lax.axis_index("tp")
    f = lax.axis_index("fsdp")
    ring_y, ring_z = _ring_ids(t)
    xc, core, f_p, f_r, f_l = _fsdp_ids(f)
    seq = az.shape[0]
    cols = wvm.shape[2]
    part = wbuf.at[pl.ds(0, 5)].reshape(5, 2, seq, cols // 2)
    half = seq // 2
    big = half // TPA
    small = big // TPA
    r2 = wbuf.at[pl.ds(5, 2)].reshape(LAND_SLOTS, 2, 2, 2, big, cols // 2)
    r1 = wbuf.at[pl.ds(7, 2)].reshape(COL, 2, 2, 2, big // 2, cols // 2)
    r4 = wbuf.at[9].reshape(COL, 2, 2, 2, small, cols // 2)
    r3 = wbuf.at[10, pl.ds(0, 4)].reshape(COL, 2, 2, 2, small // 2, cols // 2)
    hd = wo.shape[0]

    axes = ((ring_y, ring_z), (ring_z, ring_y))

    def own_rows(h):
        (i1, _, _), (i2, _, _) = axes[h]
        return pl.multiple_of(h * half + i1 * big + i2 * small, small)

    xrow = [xb.at[0, pl.ds(hf * small, small)] for hf in range(2)]
    ld_x = [pltpu.make_async_copy(x_hbm.at[pl.ds(own_rows(hf), small), :], xrow[hf], xsem.at[hf]) for hf in range(2)]

    def wcopy(k, e, src, dst, dev):
        return pltpu.make_async_remote_copy(src_ref=src, dst_ref=dst, send_sem=wss.at[k, e], recv_sem=wrs.at[k, e],
                                            device_id={"fsdp": dev}, device_id_type=MESH)

    kk = wvm.shape[1]
    kh = kk // 2
    rows_o, rows_d = pl.ds(0, hd), pl.ds(hd, kk - hd)

    def w_own(k, slot, dev):
        return wcopy(k, 0, wo, w2.at[slot, rows_o], dev), wcopy(k, 1, wd, w2.at[slot, rows_d], dev)

    def w_whole(k, slot):
        return wcopy(k, 0, w2.at[slot], w2.at[slot + 1], f_p)

    def w_2r():
        return wcopy(5, 0, w2.at[2, pl.ds(0, kh)], w2.at[6, pl.ds(0, kh)], f_r)

    def w_4l():
        return wcopy(6, 0, w2.at[4, pl.ds(kh, kh)], w2.at[6, pl.ds(kh, kh)], f_l)

    def load_own():
        return (pltpu.make_async_copy(wo, wvm.at[0, rows_o], lsem.at[2]), pltpu.make_async_copy(wd, wvm.at[0, rows_d], lsem.at[3]))

    def load_w(cb):
        return pltpu.make_async_copy(w2.at[cb], wvm.at[cb % 2], lsem.at[cb % 2])

    def send_late():
        for c in w_own(1, 2, f_r) + w_own(2, 4, f_l) + w_own(0, 1, f_p) + load_own():
            c.start()

    def fetch(cb):
        @pl.when(cb == 1)
        def _():
            for c in w_own(0, 1, f_p):
                c.wait()

        @pl.when(cb == 2)
        def _():
            for c in w_own(1, 2, f_r) + w_own(2, 4, f_l):
                c.wait()
            w_2r().start()
            w_4l().start()
            w_whole(3, 2).start()
            w_whole(4, 4).start()

        @pl.when(cb == 3)
        def _():
            w_whole(3, 2).wait()

        @pl.when(cb == 5)
        def _():
            w_whole(4, 4).wait()

        @pl.when(cb == 6)
        def _():
            w_2r().wait()
            w_4l().wait()
            w_whole(7, 6).start()

        @pl.when(cb == 7)
        def _():
            w_whole(7, 6).wait()

        load_w(cb).start()

    def block_of(k):
        q = k // 2
        dx = 3 * q - 5 * (q // 2) - 2 * (q // 3)
        return ((xc + dx) % 4) * 2 + (core + k % 2) % 2

    def block_cols(cb):
        return pl.ds(pl.multiple_of(block_of(cb) * cols, cols), cols)

    def ring_copy(cb, h, d, step, src, dst, dev):
        return pltpu.make_async_remote_copy(src_ref=src, dst_ref=dst, send_sem=ssem.at[cb, h, d, step],
                                            recv_sem=rsem.at[cb, h, d, step], device_id={"tp": dev}, device_id_type=MESH)

    def rs_first(cb, h, step, ring, base, n, land):
        i, r, l = ring
        o = (i + 2) % TPA
        m = n // 2
        s = pl.multiple_of(base + o * n, m)
        return (ring_copy(cb, h, 0, step, part.at[cb % PART_SLOTS, :, pl.ds(s, m)], land.at[cb % land.shape[0], h, 0], r),
                ring_copy(cb, h, 1, step, part.at[cb % PART_SLOTS, :, pl.ds(s + m, m)], land.at[cb % land.shape[0], h, 1], l))

    def rs_second(cb, h, step, ring, base, n, land):
        i, r, l = ring
        s_r = pl.multiple_of(base + ((i + 1) % TPA) * n, n)
        s_l = pl.multiple_of(base + ((i + 3) % TPA) * n, n)
        return (ring_copy(cb, h, 0, step, part.at[cb % PART_SLOTS, :, pl.ds(s_r, n)], land.at[cb % land.shape[0], h, 0], r),
                ring_copy(cb, h, 1, step, part.at[cb % PART_SLOTS, :, pl.ds(s_l, n)], land.at[cb % land.shape[0], h, 1], l))

    def rs_update(cb, h, ring, base, n, land):
        i, _, _ = ring
        m = n // 2
        s_r = pl.multiple_of(base + ((i + 1) % TPA) * n, m)
        s_l = pl.multiple_of(base + ((i + 3) % TPA) * n + m, m)
        for s, d in ((s_r, 0), (s_l, 1)):
            rows = pl.ds(s, m)
            part[cb % PART_SLOTS, :, rows] = (part[cb % PART_SLOTS, :, rows].astype(jnp.float32) + land[cb % land.shape[0], h, d].astype(jnp.float32)).astype(jnp.bfloat16)

    def ag_first(cb, h, step, ring, src, base, n):
        i, r, l = ring
        dst = out.at[pl.ds(pl.multiple_of(base + i * n, n), n), block_cols(cb)]
        if src is None:
            src = dst
        return (ring_copy(cb, h, 0, step, src, dst, r), ring_copy(cb, h, 1, step, src, dst, l))

    def ag_second(cb, h, step, ring, base, n):
        i, r, l = ring
        m = n // 2
        from_l = out.at[pl.ds(pl.multiple_of(base + ((i + 3) % TPA) * n, m), m), block_cols(cb)]
        from_r = out.at[pl.ds(pl.multiple_of(base + ((i + 1) % TPA) * n + m, m), m), block_cols(cb)]
        return (ring_copy(cb, h, 0, step, from_l, from_l, r), ring_copy(cb, h, 1, step, from_r, from_r, l))

    def copies(cb, step):
        res = []
        for h in range(2):
            ring1, ring2 = axes[h]
            base1 = h * half
            base2 = pl.multiple_of(h * half + ring1[0] * big, big)
            if step == 0:
                res.extend(rs_first(cb, h, step, ring1, base1, big, r1))
            elif step == 1:
                res.extend(rs_second(cb, h, step, ring1, base1, big, r2))
            elif step == 2:
                res.extend(rs_first(cb, h, step, ring2, base2, small, r3))
            elif step == 3:
                res.extend(rs_second(cb, h, step, ring2, base2, small, r4))
            elif step == 4:
                res.extend(ag_first(cb, h, step, ring2, None, base2, small))
            elif step == 5:
                res.extend(ag_second(cb, h, step, ring2, base2, small))
            elif step == 6:
                res.extend(ag_first(cb, h, step, ring1, None, base1, big))
            else:
                res.extend(ag_second(cb, h, step, ring1, base1, big))
        return res

    def start(cb, step):
        for c in copies(cb, step):
            c.start()

    def finish(cb, step):
        for c in copies(cb, step):
            c.wait_recv()
            c.wait_send()

    def stage0(cb):
        @pl.when(cb == 0)
        def _():
            for c in load_own():
                c.wait()

        @pl.when(cb > 0)
        def _():
            load_w(cb).wait()

        @pl.loop(0, seq // MT)
        def _(i):
            rows = pl.ds(pl.multiple_of(i * MT, MT), MT)
            y = jnp.dot(az[rows, :], wvm[cb % 2], preferred_element_type=jnp.float32).astype(jnp.bfloat16)
            for hf in range(2):
                part[cb % PART_SLOTS, hf, rows] = y[:, hf * (cols // 2):(hf + 1) * (cols // 2)]

        @pl.when(cb == 0)
        def _():
            pl.semaphore_wait(phase, 4)

        start(cb, 0)

    def stage1(cb):
        finish(cb, 0)
        for h in range(2):
            rs_update(cb, h, axes[h][0], h * half, big, r1)
        start(cb, 1)

    def stage2(cb):
        finish(cb, 1)
        for h in range(2):
            rows = pl.ds(pl.multiple_of(h * half + axes[h][0][0] * big, big), big)
            part[cb % PART_SLOTS, :, rows] = (part[cb % PART_SLOTS, :, rows].astype(jnp.float32) + r2[cb % r2.shape[0], h, 0].astype(jnp.float32)
                              + r2[cb % r2.shape[0], h, 1].astype(jnp.float32)).astype(jnp.bfloat16)
        start(cb, 2)

    def stage3(cb):
        finish(cb, 2)
        for h in range(2):
            rs_update(cb, h, axes[h][1], pl.multiple_of(h * half + axes[h][0][0] * big, big), small, r3)
        start(cb, 3)

    def stage4(cb):
        finish(cb, 3)
        g = block_of(cb)
        for h in range(2):
            branch = (part[cb % PART_SLOTS, :, pl.ds(own_rows(h), small)].astype(jnp.float32) + r4[cb % r4.shape[0], h, 0].astype(jnp.float32)
                      + r4[cb % r4.shape[0], h, 1].astype(jnp.float32))
            for hf in range(2):
                lanes = pl.ds(pl.multiple_of(g * cols + hf * (cols // 2), cols // 2), cols // 2)
                xs = xb[0, pl.ds(h * small, small), lanes].astype(jnp.float32)
                out[pl.ds(own_rows(h), small), lanes] = (xs + branch[hf]).astype(jnp.bfloat16)
        start(cb, 4)

    def stage5(cb):
        finish(cb, 4)
        start(cb, 5)

    def stage6(cb):
        finish(cb, 5)
        start(cb, 6)

    def stage7(cb):
        finish(cb, 6)
        start(cb, 7)

    def stage8(cb):
        finish(cb, 7)

    stages = (stage0, stage1, stage2, stage3, stage4, stage5, stage6, stage7, stage8)

    def reduce_all():
        for c in ld_x:
            c.start()
        for other in (ring_y[1], ring_y[2], ring_z[1], ring_z[2]):
            pl.semaphore_signal(phase, inc=1, device_id={"tp": other}, device_id_type=MESH)
        for c in ld_x:
            c.wait()

        @pl.loop(0, COL + GAP + len(stages) - 1)
        def _(n):
            for s, fn in enumerate(stages):
                turn = n - s

                @pl.when(jnp.logical_or(jnp.logical_and(turn >= 0, turn < 2), jnp.logical_and(turn >= 2 + GAP, turn < COL + GAP)))
                def _(fn=fn, turn=turn):
                    fn(jnp.where(turn >= 2, turn - GAP, turn))

            @pl.when(jnp.logical_or(n < 1, jnp.logical_and(n >= 1 + GAP, n + 1 < COL + GAP)))
            def _():
                fetch(jnp.where(n >= 1, n - GAP, n) + 1)

    return send_late, reduce_all


MT = 512
GAP = 1
PART_SLOTS = 5
LAND_SLOTS = 4


def layer_kernel(x_hbm, pos, inv_freq, gain, wq, wk, wv, wg, wu, wo, wd, out, w2, wbuf, q, kv, cos_t, sin_t, gbuf, xb, scores, az, wvm,
                 ssem, rsem, gss, grs, lsem, gsem, xsem, kss, krs, rss, rrs, wss, wrs, wlsem, phase):
    send_late, reduce_all = reduce_part(az, x_hbm, wo, wd, out, w2, wbuf, wvm, xb, rss, rrs, wss, wrs, wlsem, xsem, phase)
    project_part(x_hbm, pos, inv_freq, gain, wq, wk, wv, wg, wu, az, wbuf, out, q, kv, cos_t, sin_t, gbuf, xb, scores,
                 ssem, rsem, gss, grs, lsem, gsem, xsem, kss, krs, send_late)
    reduce_all()


def layer_call(x, positions, norm_gain, w_query, w_key, w_value, w_gate, w_up, w_out, w_down):
    seq, d = x.shape
    depth, hd = w_query.shape
    ff = w_gate.shape[1]
    n_chunk = 3 + ff // GU
    cols = d // COL
    inv_freq = jnp.asarray((10000.0 ** (-np.arange(0, hd, 2) / hd)).astype(np.float32))
    bf, f32 = jnp.bfloat16, jnp.float32
    hbm = pl.BlockSpec(memory_space=pl.ANY)
    vm = pl.BlockSpec(memory_space=pltpu.VMEM)
    dma = pltpu.SemaphoreType.DMA
    flops = 2 * seq * d * (3 * hd + 2 * ff) + 2 * seq * seq * hd + 2 * seq * d * (hd + ff)
    return pl.pallas_call(
        layer_kernel,
        out_shape=(pltpu.VMEM((seq, d), bf), jax.ShapeDtypeStruct((COL, hd + ff, cols), bf)),
        in_specs=[hbm, vm, vm] + [hbm] * 8,
        out_specs=(vm, hbm),
        scratch_shapes=[
            pltpu.VMEM((n_chunk, d // depth, TPA, TPA, depth // TPA // TPA, hd), bf),
            pltpu.VMEM((seq, hd), bf),
            pltpu.VMEM((2, TPA, TPA, seq // TPA // TPA, hd), bf),
            pltpu.VMEM((seq, hd // 2), f32),
            pltpu.VMEM((seq, hd // 2), f32),
            pltpu.VMEM((1, d), f32),
            pltpu.VMEM((X_SLOTS, LN_ROWS, d), bf),
            pltpu.VMEM((QB, seq), f32),
            pltpu.VMEM((seq, hd + ff), bf),
            pltpu.VMEM((2, hd + ff, cols), bf),
            dma((n_chunk, 8)),
            dma((n_chunk, 8)),
            dma((8,)),
            dma((8,)),
            dma((n_chunk, 2)),
            dma,
            dma((X_SLOTS,)),
            dma((16, 4)),
            dma((16, 4)),
            dma((COL, 2, 2, 8)),
            dma((COL, 2, 2, 8)),
            dma((8, 2)),
            dma((8, 2)),
            dma((4,)),
            pltpu.SemaphoreType.REGULAR,
        ],
        compiler_params=pltpu.CompilerParams(collective_id=0, has_side_effects=True, vmem_limit_bytes=VMEM_LIMIT),
        cost_estimate=pl.CostEstimate(flops=flops, bytes_accessed=4 * seq * d, transcendentals=0),
        name="decoder_layer",
    )(x, positions.reshape(seq // 128, 128), inv_freq.reshape(1, hd // 2), norm_gain.reshape(1, depth),
      *(w.reshape(TPA, TPA, depth // TPA // TPA, w.shape[1]) for w in (w_query, w_key, w_value, w_gate, w_up)), w_out, w_down)


def write_kernel(src, dst, sem):
    parts = sem.shape[0]
    rows = src.shape[0] // parts
    copies = [pltpu.make_async_copy(src.at[pl.ds(b * rows, rows)], dst.at[pl.ds(b * rows, rows)], sem.at[b]) for b in range(parts)]
    for c in copies:
        c.start()
    for c in copies:
        c.wait()


def write_out(block):
    return pl.pallas_call(
        write_kernel,
        out_shape=jax.ShapeDtypeStruct(block.shape, block.dtype),
        in_specs=[pl.BlockSpec(memory_space=pltpu.VMEM)],
        out_specs=pl.BlockSpec(memory_space=pl.ANY),
        scratch_shapes=[pltpu.SemaphoreType.DMA((8,))],
        compiler_params=pltpu.CompilerParams(vmem_limit_bytes=24 * 1024 * 1024),
        name="write_out",
    )(block)


def solution(mesh):
    row_spec = P(("dp", "fsdp"), None, None)

    def local_layer(hidden, positions, norm_gain, w_query, w_key, w_value, w_gate, w_up, w_out, w_down):
        rows, _ = layer_call(hidden[0], positions, norm_gain, w_query, w_key, w_value, w_gate, w_up, w_out, w_down)
        return write_out(rows)[None]

    in_specs = (row_spec, P(None), P("fsdp"), P("fsdp", "tp"), P("fsdp", None), P("fsdp", None), P("fsdp", "tp"), P("fsdp", "tp"), P("tp", "fsdp"), P("tp", "fsdp"))
    return jax.shard_map(local_layer, mesh=mesh, in_specs=in_specs, out_specs=row_spec, check_vma=False)
```
